8 devices in a mesh: data: 8 (over z, y, x, core).
Axes of the slice: x: 2, y: 2, z: 1, core: 2. Of those that a mesh axis runs over, the one named last changes fastest.
Arguments:
- x_now: bfloat16 [128, 256, 128], P('data')
- labels_now: int32 [128], P('data')
- x_next: bfloat16 [128, 256, 128], P('data')
- up_one: float32 [2, 128, 512], replicated
- down_one: float32 [2, 512, 128], replicated
- merge_proj: float32 [512, 512], replicated
- up_two: float32 [2, 512, 2048], replicated
- down_two: float32 [2, 2048, 512], replicated
- head_proj: float32 [512, 1000], replicated
- vel_up_one: float32 [2, 128, 512], replicated
- vel_down_one: float32 [2, 512, 128], replicated
- vel_merge_proj: float32 [512, 512], replicated
- vel_up_two: float32 [2, 512, 2048], replicated
- vel_down_two: float32 [2, 2048, 512], replicated
- vel_head_proj: float32 [512, 1000], replicated
Outputs:
- output 1: float32 [128, 1000], P('data')
- output 2: float32 [2, 128, 512], replicated
- output 3: float32 [2, 512, 128], replicated
- output 4: float32 [512, 512], replicated
- output 5: float32 [2, 512, 2048], replicated
- output 6: float32 [2, 2048, 512], replicated
- output 7: float32 [512, 1000], replicated
- output 8: float32 [2, 128, 512], replicated
- output 9: float32 [2, 512, 128], replicated
- output 10: float32 [512, 512], replicated
- output 11: float32 [2, 512, 2048], replicated
- output 12: float32 [2, 2048, 512], replicated
- output 13: float32 [512, 1000], replicated
All inputs are finite; a program needn't handle non-finite values.
Results may differ from the reference program's by a relative error of at most 0.0114749.
Values are sent between devices in bfloat16 or wider.
A program may use at most 1 GiB of HBM per device.

```python
import jax
import jax.numpy as jnp
from jax import lax

DATA_DEVS = 8
IMAGES_DEV = 16
TOKENS = 256
WIDTH = 128
DEPTH_ONE = 2
DEPTH_TWO = 2
CLASSES = 1000
BATCH = DATA_DEVS * IMAGES_DEV
MERGED = TOKENS // 4
WIDTH_TWO = 4 * WIDTH
HIDDEN_ONE = 4 * WIDTH
HIDDEN_TWO = 4 * WIDTH_TWO
MOMENTUM = 0.9
TRUST = 0.1
LN_EPS = 1e-6
SHIFT_SCALE = 1.5


def draw_weight(key_w, shape_w, fan_in, scale):
    return jax.random.normal(key_w, shape_w, jnp.float32) * (scale * fan_in ** -0.5)


def draw_images(key_img, key_shift):
    img_shift = jax.random.normal(key_shift, (BATCH, 1, WIDTH), jnp.float32) * SHIFT_SCALE
    raw_vals = jax.random.normal(key_img, (BATCH, TOKENS, WIDTH), jnp.float32)
    return (raw_vals + img_shift).astype(jnp.bfloat16)


def setup_inputs(seed: int = 0) -> dict:
    key_list = jax.random.split(jax.random.key(seed), 17)
    draw_specs = [
        ('up_one', (DEPTH_ONE, WIDTH, HIDDEN_ONE), WIDTH),
        ('down_one', (DEPTH_ONE, HIDDEN_ONE, WIDTH), HIDDEN_ONE),
        ('merge_proj', (4 * WIDTH, WIDTH_TWO), 4 * WIDTH),
        ('up_two', (DEPTH_TWO, WIDTH_TWO, HIDDEN_TWO), WIDTH_TWO),
        ('down_two', (DEPTH_TWO, HIDDEN_TWO, WIDTH_TWO), HIDDEN_TWO),
        ('head_proj', (WIDTH_TWO, CLASSES), WIDTH_TWO),
    ]
    drawn = {}
    drawn['x_now'] = draw_images(key_list[0], key_list[15])
    drawn['labels_now'] = jax.random.randint(key_list[1], (BATCH,), 0, CLASSES, jnp.int32)
    drawn['x_next'] = draw_images(key_list[2], key_list[16])
    for slot_num, spec_w in enumerate(draw_specs):
        drawn[spec_w[0]] = draw_weight(key_list[3 + slot_num], spec_w[1], spec_w[2], 1.0)
    for slot_num, spec_w in enumerate(draw_specs):
        drawn['vel_' + spec_w[0]] = draw_weight(key_list[9 + slot_num], spec_w[1], spec_w[2], TRUST)
    return drawn


def layer_norm(values):
    row_mean = jnp.mean(values, axis=-1, keepdims=True)
    centered = values - row_mean
    variance = jnp.mean(centered * centered, axis=-1, keepdims=True)
    return centered * lax.rsqrt(variance + LN_EPS)


def stage_block(residual, layer_weights):
    w_up, w_down = layer_weights
    normed = layer_norm(residual.astype(jnp.float32)).astype(jnp.bfloat16)
    pre_act = jnp.dot(normed, w_up.astype(jnp.bfloat16), preferred_element_type=jnp.float32)
    activated = jax.nn.gelu(pre_act, approximate=True).astype(jnp.bfloat16)
    block_out = jnp.dot(activated, w_down.astype(jnp.bfloat16), preferred_element_type=jnp.float32)
    return (residual.astype(jnp.float32) + block_out).astype(jnp.bfloat16), None


def model_logits(params, images):
    up_one, down_one, merge_proj, up_two, down_two, head_proj = params
    img_count = images.shape[0]
    residual = images.reshape(img_count * TOKENS, WIDTH)
    residual = lax.scan(stage_block, residual, (up_one, down_one))[0]
    merged = residual.reshape(img_count * MERGED, 4 * WIDTH)
    residual = jnp.dot(merged, merge_proj.astype(jnp.bfloat16), preferred_element_type=jnp.float32).astype(jnp.bfloat16)
    residual = lax.scan(stage_block, residual, (up_two, down_two))[0]
    pooled = jnp.mean(residual.reshape(img_count, MERGED, WIDTH_TWO).astype(jnp.float32), axis=1)
    normed = layer_norm(pooled).astype(jnp.bfloat16)
    return jnp.dot(normed, head_proj.astype(jnp.bfloat16), preferred_element_type=jnp.float32)


def shard_loss(params, images, labels):
    logits = model_logits(params, images)
    log_norm = jax.nn.logsumexp(logits, axis=-1)
    picked = jnp.sum(logits * jax.nn.one_hot(labels, CLASSES, dtype=jnp.float32), axis=-1)
    return jnp.sum(log_norm - picked) / BATCH


def lars_step(weight, velocity, grad_sum):
    red_axes = (weight.ndim - 2, weight.ndim - 1)
    w_norm = jnp.sqrt(jnp.sum(weight * weight, axis=red_axes, keepdims=True))
    g_norm = jnp.sqrt(jnp.sum(grad_sum * grad_sum, axis=red_axes, keepdims=True))
    new_vel = MOMENTUM * velocity + TRUST * (w_norm / g_norm) * grad_sum
    return weight - new_vel, new_vel


def reference(x_now, labels_now, x_next, up_one, down_one, merge_proj, up_two, down_two, head_proj, vel_up_one, vel_down_one, vel_merge_proj, vel_up_two, vel_down_two, vel_head_proj):
    params = (up_one, down_one, merge_proj, up_two, down_two, head_proj)
    grad_fn = jax.grad(shard_loss)

    def add_shard(running, shard_pair):
        grads = grad_fn(params, shard_pair[0], shard_pair[1])
        summed = jax.tree.map(lambda run_sum, shard_grad: run_sum + shard_grad.astype(jnp.bfloat16).astype(jnp.float32), running, grads)
        return summed, None

    zero_sums = jax.tree.map(jnp.zeros_like, params)
    img_shards = x_now.reshape(DATA_DEVS, IMAGES_DEV, TOKENS, WIDTH)
    label_shards = labels_now.reshape(DATA_DEVS, IMAGES_DEV)
    grad_sums = lax.scan(add_shard, zero_sums, (img_shards, label_shards))[0]
    new_up_one, new_vel_up_one = lars_step(up_one, vel_up_one, grad_sums[0])
    new_down_one, new_vel_down_one = lars_step(down_one, vel_down_one, grad_sums[1])
    new_merge_proj, new_vel_merge_proj = lars_step(merge_proj, vel_merge_proj, grad_sums[2])
    new_up_two, new_vel_up_two = lars_step(up_two, vel_up_two, grad_sums[3])
    new_down_two, new_vel_down_two = lars_step(down_two, vel_down_two, grad_sums[4])
    new_head_proj, new_vel_head_proj = lars_step(head_proj, vel_head_proj, grad_sums[5])
    new_params = (new_up_one, new_down_one, new_merge_proj, new_up_two, new_down_two, new_head_proj)
    next_shards = x_next.reshape(DATA_DEVS, IMAGES_DEV, TOKENS, WIDTH)
    logits_next = lax.map(lambda images: model_logits(new_params, images), next_shards).reshape(BATCH, CLASSES)
    return (logits_next, new_up_one, new_down_one, new_merge_proj, new_up_two, new_down_two, new_head_proj, new_vel_up_one, new_vel_down_one, new_vel_merge_proj, new_vel_up_two, new_vel_down_two, new_vel_head_proj)
```

```python
import jax
import jax.numpy as jnp
from jax import lax
from jax.experimental import pallas as pl
from jax.experimental.pallas import tpu as pltpu
from jax.sharding import PartitionSpec as P

MOMENTUM = 0.9
TRUST = 0.1
LN_EPS = 1e-6
GELU_C = 0.7978845608028654
GELU_K = 0.044715
MESH = pl.DeviceIdType.MESH
F32 = jnp.float32
BF16 = jnp.bfloat16
VMEM_LIMIT = 67043328

IMAGES = 16
TOKENS = 256
D1 = 128
H1 = 512
D2 = 512
H2 = 2048
ROWS1 = IMAGES * TOKENS
ROWS2 = ROWS1 // 4
CLASSES = 1000
CPAD = 1024
TILE = 256
NTILE = ROWS2 // TILE
WIDE = 512
CH = 7
LETTERS = 'abcdefg'
LRW = 3584
LRG = 2560
NDEV = 8
MT = 64
SUB = 8
PAIR = range(2)
QUADS = range(4)
CHUNK = 32768


def nn(a, b):
    return lax.dot_general(a, b, (((1,), (0,)), ((), ())), preferred_element_type=F32)


def nt(a, b):
    return lax.dot_general(a, b, (((1,), (1,)), ((), ())), preferred_element_type=F32)


def tn(a, b):
    return lax.dot_general(a, b, (((0,), (0,)), ((), ())), preferred_element_type=F32)


def gelu_only(x):
    inner = x * (GELU_C + (GELU_C * GELU_K) * (x * x))
    half = 0.5 + 0.5 * jnp.tanh(inner)
    return x * half


def gelu_pair(x):
    x2 = x * x
    t = jnp.tanh(x * (GELU_C + (GELU_C * GELU_K) * x2))
    half = 0.5 + 0.5 * t
    act = x * half
    slope = half + act * ((1.0 - t) * (GELU_C + (3.0 * GELU_C * GELU_K) * x2))
    return act, slope


def ln_parts(r):
    mean = jnp.mean(r, axis=-1, keepdims=True)
    cen = r - mean
    var = jnp.mean(cen * cen, axis=-1, keepdims=True)
    rstd = lax.rsqrt(var + LN_EPS)
    return cen * rstd, rstd


def ln_back(dy, xhat, rstd):
    m1 = jnp.mean(dy, axis=-1, keepdims=True)
    m2 = jnp.mean(dy * xhat, axis=-1, keepdims=True)
    return rstd * (dy - m1 - xhat * m2)


def fold_sq(v):
    rows, cols = v.shape
    s = jnp.sum((v * v).reshape(rows // SUB, SUB, cols), axis=0)
    out = s[:, 0:D1]
    for q in range(1, cols // D1):
        out = out + s[:, D1 * q:D1 * (q + 1)]
    return out


def total(acc):
    return jnp.sum(jnp.sum(acc, axis=1, keepdims=True), axis=0, keepdims=True)


def ds(start, size, mult=None):
    if isinstance(start, int):
        return pl.ds(start, size)
    return pl.ds(pl.multiple_of(start, mult or size), size)


def onehot_rows(t):
    row = lax.broadcasted_iota(jnp.int32, (IMAGES, WIDE), 0)
    col = lax.broadcasted_iota(jnp.int32, (IMAGES, WIDE), 1)
    return jnp.where(row == t * (WIDE // MT) + col // MT, 1.0, 0.0).astype(BF16)


class Ring:
    def __init__(self, num, g, r1, r2, r3, ssem, rsem, csem, pos):
        self.num = num
        self.g, self.r1, self.r2, self.r3 = (ref.at[num] for ref in (g, r1, r2, r3))
        self.ssem, self.rsem, self.csem = ssem, rsem, csem
        self.pos = pos
        self.rb = g.shape[1] // NDEV
        c, f, s = pos['c'], pos['f'], pos['s']
        self.f, self.s, self.nf, self.ns = f, s, 1 - f, 1 - s
        self.mine, self.other = 4 * c, 4 - 4 * c
        self.keep = self.mine + 2 * f
        self.give = self.mine + 2 * self.nf
        self.own_b, self.s_b = self.keep + s, self.keep + self.ns
        self.f_b, self.d_b = self.give + s, self.give + self.ns

    def blk(self, b, n=1):
        return self.g.at[ds(b * self.rb, n * self.rb, self.rb)]

    def rc(self, k, src, dst, dev):
        return pltpu.make_async_remote_copy(src_ref=src, dst_ref=dst, send_sem=self.ssem.at[self.num, k], recv_sem=self.rsem.at[self.num, k], device_id=(self.pos[dev],), device_id_type=MESH)

    def add(self, b, recv, i, n):
        rows, width = n * self.rb, self.g.shape[1]
        step = min(rows, CHUNK // width)
        b0, i0 = b * self.rb, i * self.rb

        def body(j, carry):
            dst = ds(b0 + j * step, step)
            src = ds(i0 + j * step, step)
            self.g[dst, :] = (self.g[dst, :].astype(F32) + recv[src, :].astype(F32)).astype(BF16)
            return carry

        lax.fori_loop(0, rows // step, body, 0)

    def to_core(self):
        return self.rc(0, self.blk(self.other, 4), self.r1, 'core')

    def to_f(self):
        return self.rc(1, self.blk(self.give, 2), self.r2, 'fn')

    def to_s(self):
        return self.rc(2, self.blk(self.s_b), self.r3, 'sn')

    def back(self, k, b, dev):
        return self.rc(k, self.blk(b), self.blk(b), dev)

    def own_to_s(self):
        return self.back(3, self.own_b, 'sn')

    def own_to_f(self):
        return self.back(4, self.own_b, 'fn')

    def own_to_core(self):
        return self.back(5, self.own_b, 'core')

    def s_to_f(self):
        return self.back(6, self.s_b, 'fn')

    def s_to_core(self):
        return self.back(7, self.s_b, 'core')

    def f_to_core(self):
        return self.back(8, self.f_b, 'core')

    def d_to_core(self):
        return self.back(9, self.d_b, 'core')

    def half(self):
        self.to_core().start()

    def link_f(self):
        self.to_core().wait_recv()
        self.add(self.give, self.r1, 2 * self.nf, 2)
        self.to_f().start()
        self.add(self.keep, self.r1, 2 * self.f, 2)

    def link_s(self):
        self.to_f().wait_recv()
        self.add(self.s_b, self.r2, self.ns, 1)
        self.to_s().start()
        self.add(self.own_b, self.r2, self.s, 1)
        self.to_core().wait_send()
        self.free(0, 'core')
        self.to_f().wait_send()
        self.free(1, 'fn')

    def own(self):
        self.to_s().wait_recv()
        self.to_s().wait_send()
        self.free(2, 'sn')
        self.add(self.own_b, self.r3, 0, 1)
        self.held(1)
        self.own_to_f().start()
        self.held(0)
        self.own_to_core().start()

    def own_s(self):
        self.held(2)
        self.own_to_s().start()

    def pass_s(self):
        self.own_to_s().wait_recv()
        self.s_to_f().start()
        self.s_to_core().start()

    def pass_f(self):
        self.own_to_f().wait_recv()
        self.f_to_core().start()

    def pass_d(self):
        self.s_to_f().wait_recv()
        self.d_to_core().start()

    def done(self):
        for cp in (self.own_to_core(), self.s_to_core(), self.f_to_core(), self.d_to_core()):
            cp.wait()
        for cp in (self.own_to_s(), self.own_to_f(), self.s_to_f()):
            cp.wait_send()

    def free(self, i, who):
        pl.semaphore_signal(self.csem.at[self.num, i], inc=1, device_id=(self.pos[who],), device_id_type=MESH)

    def held(self, i):
        pl.semaphore_wait(self.csem.at[self.num, i], 1)


class Share:
    def __init__(self, buf, ssem, rsem, pos):
        self.buf, self.ssem, self.rsem, self.pos = buf, ssem, rsem, pos

    def rc(self, k):
        p = self.pos
        own, fblk, sblk, dblk = p['me'], p['fn'], p['sn'], p['diag']
        b, dev = {0: (own, 'fn'), 1: (own, 'sn'), 2: (own, 'core'), 3: (fblk, 'sn'), 4: (fblk, 'core'), 5: (sblk, 'core'), 6: (dblk, 'core')}[k]
        return pltpu.make_async_remote_copy(src_ref=self.buf.at[b], dst_ref=self.buf.at[b], send_sem=self.ssem.at[k], recv_sem=self.rsem.at[k], device_id=(p[dev],), device_id_type=MESH)


    def send(self):
        for k in (0, 1, 2):
            self.rc(k).start()

    def relay(self):
        self.rc(0).wait_recv()
        self.rc(3).start()
        self.rc(4).start()
        self.rc(1).wait_recv()
        self.rc(5).start()

    def done(self):
        self.rc(3).wait_recv()
        self.rc(6).start()
        for k in (2, 4, 5, 6):
            self.rc(k).wait_recv()
        for k in range(7):
            self.rc(k).wait_send()


def position():
    me = lax.axis_index('data')
    c = lax.rem(me, 2)
    x = lax.rem(me // 2, 2)
    y = me // 4
    f = c * y + (1 - c) * x
    s = c * x + (1 - c) * y
    xn = me + 2 - 4 * x
    yn = me + 4 - SUB * y
    fn = c * yn + (1 - c) * xn
    sn = c * xn + (1 - c) * yn
    diag = xn + yn - me
    core = me + 1 - 2 * c
    return dict(me=me, c=c, f=f, s=s, fn=fn, sn=sn, diag=diag, core=core)


STEPS = ('half', 'link_f', 'link_s', 'own', 'own_s', 'pass_s', 'pass_f', 'pass_d', 'done')
SHARE_STEPS = ('send', 'relay', 'done')
PLAN = dict(
    up1=('', 'a0', '', 'b0 a1'),
    in1=('', 's1', 'b1', 'a2'),
    dn0=('', 'c0', 'b2', 'd0 a3'),
    pre0=('c1 a4', '', 'd1', 'a5 b3'),
    up0=('b4', 'e0 c2', '', 'f0 d2'),
    in0=('e1 s2', 'a6', 'f1 a7', 'c3 b5'),
    mrg=('e2 c4 d3',),
    back=('d4 f2 c5 b6', 'e3 b7 c6 a8', 'e4 f3 d5 c7', 'g0 f4 d6 b8'),
    rank=('g1 e5', 'd7', 'g2 e6 c8', 'f5 e7'),
    rankh=('g3 f6', 'g4', 'f7', 'g5'),
    tail=('d8 g6', 'e8 g7', 'f8', 'g8'),
)


def grad_kernel(x_hbm, lab, uo_hbm, do_hbm, m_hbm, ut_hbm, dt_hbm, h_hbm,
                g_out, gv1_out, gh_out, scal,
                g_all, r1_all, r2_all, r3_all, lr,
                wuo, wdo, wm, wut, wdt, wh,
                merged, n1, rst1, r2, n2, rst2, a2, sl2, pooled, asum, accv, accu, sq, gsq,
                in_sem, st_sem, out_sem, ssem, rsem, csem, lssem, lrsem):
    pos = position()
    barrier = pltpu.get_barrier_semaphore()
    for who in ('core', 'fn', 'sn'):
        pl.semaphore_signal(barrier, inc=1, device_id=(pos[who],), device_id_type=MESH)

    gv1, gh, grad = wdt.at[1], wh, r2

    share = Share(lr, lssem, lrsem, pos)
    rings = {letter: Ring(i, g_all, r1_all, r2_all, r3_all, ssem, rsem, csem, pos) for i, letter in enumerate(LETTERS)}
    outs = {letter: pltpu.make_async_copy(g_all.at[i], g_out.at[i], out_sem.at[i]) for i, letter in enumerate(LETTERS)}

    def act(word):
        letter, num = word[0], int(word[1])
        if letter == 's':
            getattr(share, SHARE_STEPS[num])()
        else:
            getattr(rings[letter], STEPS[num])()
            if STEPS[num] == 'done':
                outs[letter].start()

    def run(name, body):
        plan = PLAN[name]

        def wrapped(t, carry):
            body(t)
            for i, words in enumerate(plan):
                if words:
                    @pl.when(t == i)
                    def _():
                        for word in words.split():
                            act(word)
            return carry

        lax.fori_loop(0, len(plan), wrapped, 0)

    def forward(xb, xf, suo, sdo, sm, sut, sdt, abuf):
        loads = [pltpu.make_async_copy(src, dst, in_sem.at[i]) for i, (src, dst) in enumerate(((x_hbm, xb), (uo_hbm, suo), (do_hbm, sdo), (m_hbm, sm), (h_hbm, sdt.at[0:CLASSES])))]

        def stage_up(i):
            return pltpu.make_async_copy(ut_hbm.at[i // 2, ds((i % 2) * TILE, TILE)], sut, st_sem.at[0])

        def stage_down(i):
            return pltpu.make_async_copy(dt_hbm.at[i // 2, ds((i % 2) * ROWS2, ROWS2)], sdt, st_sem.at[1])

        for cp in loads[:3]:
            cp.start()
        stage_up(0).start()
        stage_down(0).start()
        loads[3].start()
        sq[...] = jnp.zeros_like(sq)
        for cp in loads[:3]:
            cp.wait()
        for b in PAIR:
            v = suo[b]
            sq[b] = fold_sq(v)
            wuo[b] = v.astype(BF16)
            v = sdo[b]
            sq[2 + b] = fold_sq(v)
            wdo[b] = v.astype(BF16)

        def stage_one(t, carry):
            xf[...] = xb[ds(t * ROWS2, ROWS2), :].astype(F32)
            r = jnp.concatenate([xf[pl.ds(j, TILE, stride=4), :] for j in QUADS], axis=0)
            rows = ds(t * ROWS2, ROWS2)
            for b in PAIR:
                xhat, rstd = ln_parts(r)
                n = xhat.astype(BF16)
                n1[b, rows, :] = n
                if b == 1:
                    rst1[rows, :] = rstd
                a = gelu_only(nn(n, wuo[b])).astype(BF16)
                rb = (r + nn(a, wdo[b])).astype(BF16)
                r = rb.astype(F32)
            for j in QUADS:
                merged[ds(t * TILE, TILE), D1 * j:D1 * (j + 1)] = rb[TILE * j:TILE * (j + 1), :]
            stage_up(t).wait()
            layer = t // 2

            def cast_up(i, acc):
                v = sut[ds(i * IMAGES, IMAGES), :]
                wut[layer, ds((t % 2) * TILE + i * IMAGES, IMAGES), :] = v.astype(BF16)
                return acc + fold_sq(v)

            sq[4 + layer] += lax.fori_loop(0, IMAGES, cast_up, jnp.zeros((SUB, D1), F32))
            stage_down(t).wait()

            def cast_down(i, acc):
                v = sdt[ds(i * MT, MT), :]
                wdt[layer, ds((t % 2) * ROWS2 + i * MT, MT), :] = v.astype(BF16)
                return acc + fold_sq(v)

            sq[6 + layer] += lax.fori_loop(0, IMAGES, cast_down, jnp.zeros((SUB, D1), F32))

            @pl.when(t < 3)
            def _():
                stage_up(t + 1).start()
                stage_down(t + 1).start()

            return carry

        lax.fori_loop(0, NTILE, stage_one, 0)

        loads[4].start()
        loads[3].wait()

        def cast_m(i, acc):
            v = sm[ds(i * MT, MT), :]
            wm[ds(i * MT, MT), :] = v.astype(BF16)
            return acc + fold_sq(v)

        sq[SUB] = lax.fori_loop(0, SUB, cast_m, jnp.zeros((SUB, D1), F32))

        def merge_tile(t, carry):
            rows = ds(t * WIDE, WIDE)
            r2[rows, :] = nn(merged[rows, :], wm[...]).astype(BF16)
            return carry

        lax.fori_loop(0, ROWS2 // WIDE, merge_tile, 0)
        asum[...] = jnp.zeros_like(asum)
        pooled[...] = jnp.zeros_like(pooled)

        for layer in PAIR:
            def stage_two(t, carry):
                rows = ds(t * WIDE, WIDE)
                r = r2[rows, :].astype(F32)
                xhat, rstd = ln_parts(r)
                n = xhat.astype(BF16)
                n2[layer, rows, :] = n
                rst2[layer, rows, :] = rstd
                for q in QUADS:
                    cols = slice(D2 * q, D2 * (q + 1))
                    acts, slope = gelu_pair(nn(n, wut[layer, :, cols]))
                    if layer == 0:
                        a2[rows, cols] = acts.astype(BF16)
                    else:
                        abuf[:, cols] = acts.astype(BF16)
                    sl2[layer, rows, cols] = slope.astype(BF16)
                if layer == 0:
                    r2[rows, :] = (r + nn(a2[rows, :], wdt[layer])).astype(BF16)
                else:
                    rb = (r + nn(abuf[...], wdt[layer])).astype(BF16)
                    pick = onehot_rows(t)
                    asum[...] += nn(pick, abuf[...])
                    pooled[...] += nn(pick, rb)
                return carry

            lax.fori_loop(0, ROWS2 // WIDE, stage_two, 0)
        wh[CLASSES:, :] = jnp.zeros((CPAD - CLASSES, D2), BF16)
        loads[4].wait()
        for k in QUADS:
            rows = slice(TILE * k, min(TILE * (k + 1), CLASSES))
            v = sdt[rows, :]
            wh[rows, :] = v.astype(BF16)
            sq[9] += fold_sq(v)

    pl.run_scoped(
        forward,
        pltpu.VMEM((ROWS1, D1), BF16),
        pltpu.VMEM((ROWS2, D1), F32),
        pltpu.VMEM((2, D1, H1), F32),
        pltpu.VMEM((2, H1, D1), F32),
        pltpu.VMEM((D2, D2), F32),
        pltpu.VMEM((TILE, H2), F32),
        pltpu.VMEM((ROWS2, D2), F32),
        pltpu.VMEM((WIDE, H2), BF16),
    )

    xhat, rstd = ln_parts(pooled[...] * (1.0 / MT))
    hb = xhat.astype(BF16)
    logits = nt(hb, wh[...])
    col = lax.broadcasted_iota(jnp.int32, (IMAGES, CPAD), 1)
    row = lax.broadcasted_iota(jnp.int32, (IMAGES, CPAD), 0)
    logits = jnp.where(col < CLASSES, logits, -jnp.inf)
    ex = jnp.exp(logits - jnp.max(logits, axis=-1, keepdims=True))
    prob = ex / jnp.sum(ex, axis=-1, keepdims=True)
    lab_row = jnp.zeros((IMAGES, CPAD), jnp.int32)
    for i in range(IMAGES):
        lab_row = jnp.where(row == i, lab[i], lab_row)
    gl = ((prob - jnp.where(col == lab_row, 1.0, 0.0)) * (1.0 / (IMAGES * NDEV))).astype(BF16)
    g16 = (ln_back(nn(gl, wh[...]), xhat, rstd) * (1.0 / MT)).astype(BF16)
    hi = asum[...].astype(BF16)
    lo = (asum[...] - hi.astype(F32)).astype(BF16)
    me = pos['me']
    lr[me, 0:IMAGES, 0:H2] = hi
    lr[me, IMAGES:32, 0:H2] = lo
    lr[me, 0:IMAGES, H2:LRG] = g16
    lr[me, IMAGES:32, H2:LRG] = g16
    lr[me, 0:IMAGES, LRG:LRW] = gl
    lr[me, IMAGES:32, LRG:LRG + D2] = hb
    pl.semaphore_wait(barrier, 3)
    share.send()

    asum[...] = nt(g16, wdt[1])
    pooled[...] = g16.astype(F32)

    def slope_one(i, carry):
        rows = ds(i * MT, MT)
        grad[rows, :] = jnp.broadcast_to(pooled[pl.ds(i, 1), :], (MT, D2)).astype(BF16)
        for q in QUADS:
            cols = slice(D2 * q, D2 * (q + 1))
            sl2[1, rows, cols] = (asum[pl.ds(i, 1), cols] * sl2[1, rows, cols].astype(F32)).astype(BF16)
        return carry

    lax.fori_loop(0, IMAGES, slope_one, 0)

    def up_grad(layer, first):
        def body(q):
            g_all[first + q // 2, ds((q % 2) * D2, D2), :] = tn(n2[layer], sl2[layer, :, ds(q * D2, D2)]).astype(BF16)

        return body

    def down_grad(q):
        g_all[2 + q // 2, ds((q % 2) * D2, D2), :] = tn(a2[:, ds(q * D2, D2)], grad[...]).astype(BF16)

    def input_grad(layer):
        def body(t):
            rows = ds(t * TILE, TILE)
            dy = nt(sl2[layer, rows, :], wut[layer])
            dx = ln_back(dy, n2[layer, rows, :].astype(F32), rst2[layer, rows, :])
            grad[rows, :] = (dx + grad[rows, :].astype(F32)).astype(BF16)

        return body

    def pre_grad(t):
        rows = ds(t * TILE, TILE)
        for q in QUADS:
            cols = slice(D2 * q, D2 * (q + 1))
            ga = nt(grad[rows, :], wdt[0, cols, :])
            sl2[0, rows, cols] = (ga * sl2[0, rows, cols].astype(F32)).astype(BF16)

    gsm = g_all.at[CH - 1]

    def merge_grad(t):
        gsm[D2:ROWS2, :] = tn(merged[...], grad[...]).astype(BF16)

    def stage_one_back(t):
        gm = nt(grad[ds(t * TILE, TILE), :], wm[...]).astype(BF16)
        rows = ds(t * ROWS2, ROWS2)
        g = jnp.concatenate([gm[:, D1 * j:D1 * (j + 1)] for j in QUADS], axis=0)
        for b in (1, 0):
            n = n1[b, rows, :]
            acts, slope = gelu_pair(nn(n, wuo[b]))
            accv[b] += tn(acts.astype(BF16), g)
            gp = (nt(g, wdo[b]) * slope).astype(BF16)
            accu[b] += tn(n, gp)
            if b == 1:
                dx = ln_back(nt(gp, wuo[b]), n.astype(F32), rst1[rows, :])
                g = (dx + g.astype(F32)).astype(BF16)

        @pl.when(t == 3)
        def _():
            for b in PAIR:
                gsm[D1 * b:D1 * (b + 1), :] = accu[b].astype(BF16)
                for q in PAIR:
                    gsm[TILE:D2, TILE * b + D1 * q:TILE * b + D1 * (q + 1)] = accv[b, TILE * q:TILE * (q + 1), :].astype(BF16)

    run('up1', up_grad(1, 0))
    run('in1', input_grad(1))
    run('dn0', down_grad)
    run('pre0', pre_grad)
    run('up0', up_grad(0, 4))
    run('in0', input_grad(0))
    accv[...] = jnp.zeros_like(accv)
    accu[...] = jnp.zeros_like(accu)
    gsq[...] = jnp.zeros_like(gsq)
    run('mrg', merge_grad)
    run('back', stage_one_back)

    def v1_rows(i):
        cols = ds(i * D2, D2)
        out = jnp.zeros((D2, D2), F32)
        for d in range(NDEV):
            out = out + tn(lr[d, :, cols], lr[d, :, H2:LRG]).astype(BF16).astype(F32)
        ob = out.astype(BF16)
        gv1[cols, :] = ob
        gsq[7] += fold_sq(ob.astype(F32))

    def head_rows(i):
        rows = ds(i * TILE, TILE)
        out = jnp.zeros((TILE, D2), F32)
        for d in range(NDEV):
            out = out + tn(lr[d, 0:IMAGES, ds(LRG + i * TILE, TILE, TILE)], lr[d, IMAGES:32, LRG:LRG + D2]).astype(BF16).astype(F32)
        ob = out.astype(BF16)
        gh[rows, :] = ob
        gsq[9] += fold_sq(ob.astype(F32))

    def norm_of(letter, row):
        ref = g_all.at[LETTERS.index(letter)]

        def body(i, acc):
            return acc + fold_sq(ref[ds(i * MT, MT), :].astype(F32))

        gsq[row] += lax.fori_loop(0, ROWS2 // MT, body, jnp.zeros((SUB, D1), F32))

    gv1_cp = pltpu.make_async_copy(gv1, gv1_out, out_sem.at[CH])
    gh_cp = pltpu.make_async_copy(gh, gh_out, out_sem.at[CH + 1])
    run('rank', v1_rows)
    gv1_cp.start()
    run('rankh', head_rows)
    gh_cp.start()
    norm_of('a', 5)
    norm_of('b', 5)
    norm_of('c', 6)
    for i, words in enumerate(PLAN['tail']):
        for word in words.split():
            act(word)
        if i == 0:
            norm_of('d', 6)
        if i == 1:
            norm_of('e', 4)
        if i == 2:
            norm_of('f', 4)
    for b in PAIR:
        gsq[b] = fold_sq(gsm[D1 * b:D1 * (b + 1), :].astype(F32))
        gsq[2 + b] = fold_sq(gsm[TILE:D2, TILE * b:TILE * (b + 1)].astype(F32))
    gsq[SUB] = fold_sq(gsm[D2:ROWS2, :].astype(F32))
    for i in range(10):
        ratio = jnp.sqrt(total(sq[i])) / jnp.sqrt(total(gsq[i]))
        scal[i:i + 1, :] = jnp.broadcast_to(TRUST * ratio, (1, D1))
    scal[10:IMAGES, :] = jnp.zeros((6, D1), F32)
    for letter in LETTERS:
        outs[letter].wait()
    gv1_cp.wait()
    gh_cp.wait()


def step_kernel(x_hbm, uo_hbm, do_hbm, m_hbm, ut_hbm, dt_hbm, h_hbm, vuo_hbm, vdo_hbm, vm_hbm, vut_hbm, vdt_hbm, vh_hbm,
                g_hbm, gv1_hbm, gh_hbm, scal,
                logits_out, uo_out, do_out, m_out, ut_out, dt_out, h_out, vuo_out, vdo_out, vm_out, vut_out, vdt_out, vh_out,
                xb, xf, g_all, gv1, gh, suo, sdo, sm, sh, sut, sdt, tuo, tdo, tm, th, tut, tdt,
                wuo, wdo, wm, wut, wdt, wh, r2, pooled,
                s_in, s_out, q_in, q_out, g_sem):
    small = [(uo_hbm, suo, uo_out), (vuo_hbm, tuo, vuo_out), (do_hbm, sdo, do_out), (vdo_hbm, tdo, vdo_out), (m_hbm, sm, m_out), (vm_hbm, tm, vm_out), (h_hbm, sh, h_out), (vh_hbm, th, vh_out)]
    ins = [pltpu.make_async_copy(src, buf, s_in.at[i]) for i, (src, buf, _) in enumerate(small)]
    louts = [pltpu.make_async_copy(buf, dst, s_out.at[i]) for i, (_, buf, dst) in enumerate(small)]
    big = [(ut_hbm, sut, ut_out, D1), (vut_hbm, tut, vut_out, D1), (dt_hbm, sdt, dt_out, D2), (vdt_hbm, tdt, vdt_out, D2)]
    gsm = g_all.at[CH - 1]

    def qin(layer, t, k):
        src, buf, _, n = big[k]
        return pltpu.make_async_copy(src.at[layer, ds(t * n, n)], buf.at[ds(t * n, n)], q_in.at[k, t])

    def qout(layer, t, k):
        _, buf, dst, n = big[k]
        return pltpu.make_async_copy(buf.at[ds(t * n, n)], dst.at[layer, ds(t * n, n)], q_out.at[k, t])

    x_cp = pltpu.make_async_copy(x_hbm, xb, g_sem.at[CH])
    g_cps = [pltpu.make_async_copy(g_hbm.at[i], g_all.at[i], g_sem.at[i]) for i in range(CH)]
    gv1_cp = pltpu.make_async_copy(gv1_hbm, gv1, g_sem.at[CH + 1])
    gh_cp = pltpu.make_async_copy(gh_hbm, gh, g_sem.at[CH + 2])
    x_cp.start()
    g_cps[CH - 1].start()
    for cp in ins[:4]:
        cp.start()

    def update(w, v, g, scale):
        nv = MOMENTUM * v + scale * g.astype(F32)
        nw = w - nv
        return nw, nv

    x_cp.wait()
    g_cps[CH - 1].wait()
    for cp in ins[:4]:
        cp.wait()
    for i in (4, 5, 2, 3):
        g_cps[i].start()
    for t in QUADS:
        for k in QUADS:
            qin(0, t, k).start()
    ins[4].start()
    ins[5].start()
    g_cps[0].start()
    g_cps[1].start()
    gv1_cp.start()
    gh_cp.start()
    ins[6].start()
    ins[7].start()
    for b in PAIR:
        nw, nv = update(suo[b], tuo[b], gsm[D1 * b:D1 * (b + 1), :], scal[b:b + 1, 0:1])
        suo[b] = nw
        tuo[b] = nv
        wuo[b] = nw.astype(BF16)
        for q in PAIR:
            rows = slice(TILE * q, TILE * (q + 1))
            nw, nv = update(sdo[b, rows, :], tdo[b, rows, :], gsm[TILE:D2, TILE * b + D1 * q:TILE * b + D1 * (q + 1)], scal[2 + b:3 + b, 0:1])
            sdo[b, rows, :] = nw
            tdo[b, rows, :] = nv
            wdo[b, rows, :] = nw.astype(BF16)
    for cp in louts[:4]:
        cp.start()

    def loop_update(wbuf, vbuf, gref, wdst, base, count, scale, gbase):
        def body(i, carry):
            rows = ds(base + i * MT, MT)
            nw, nv = update(wbuf[rows, :], vbuf[rows, :], gref[ds(gbase + i * MT, MT), :], scale)
            wbuf[rows, :] = nw
            vbuf[rows, :] = nv
            wdst[rows, :] = nw.astype(BF16)
            return carry

        lax.fori_loop(0, count // MT, body, 0)

    def big_update(layer, t):
        for k in QUADS:
            qin(layer, t, k).wait()
        up_scale, down_scale = scal[4 + layer:5 + layer, 0:1], scal[6 + layer:7 + layer, 0:1]

        def up_body(i, carry):
            rows = ds(t * D1 + i * IMAGES, IMAGES)
            for q in QUADS:
                cols = slice(D2 * q, D2 * (q + 1))
                g = g_all[4 - 4 * layer + q // 2, ds((q % 2) * D2 + t * D1 + i * IMAGES, IMAGES), :]
                nw, nv = update(sut[rows, cols], tut[rows, cols], g, up_scale)
                sut[rows, cols] = nw
                tut[rows, cols] = nv
                wut[layer, rows, cols] = nw.astype(BF16)
            return carry

        lax.fori_loop(0, D1 // IMAGES, up_body, 0)
        if layer == 0:
            loop_update(sdt, tdt, g_all.at[2 + t // 2], wdt.at[0], t * D2, D2, down_scale, (t % 2) * D2)
        else:
            loop_update(sdt, tdt, gv1, wdt.at[1], t * D2, D2, down_scale, t * D2)
        for k in QUADS:
            qout(layer, t, k).start()

    def refill(t):
        for k in QUADS:
            qout(0, t, k).wait()
        for k in QUADS:
            qin(1, t, k).start()

    def stage_one(t, carry):
        xf[...] = xb[ds(t * ROWS2, ROWS2), :].astype(F32)
        r = jnp.concatenate([xf[pl.ds(j, TILE, stride=4), :] for j in QUADS], axis=0)
        for b in PAIR:
            xhat, _ = ln_parts(r)
            a = gelu_only(nn(xhat.astype(BF16), wuo[b])).astype(BF16)
            rb = (r + nn(a, wdo[b])).astype(BF16)
            r = rb.astype(F32)
        for j in QUADS:
            r2[ds(t * TILE, TILE), D1 * j:D1 * (j + 1)] = rb[TILE * j:TILE * (j + 1), :]

        @pl.when(t == 0)
        def _():
            for i in (4, 5, 2, 3):
                g_cps[i].wait()

        big_update(0, t)

        @pl.when(t > 0)
        def _():
            refill(t - 1)

        return carry

    lax.fori_loop(0, NTILE, stage_one, 0)
    for cp in ins[4:6]:
        cp.wait()
    loop_update(sm, tm, gsm.at[D2:ROWS2], wm, 0, D2, scal[SUB:9, 0:1], 0)
    for cp in louts[4:6]:
        cp.start()
    refill(3)
    g_cps[0].wait()
    g_cps[1].wait()
    gv1_cp.wait()
    pooled[...] = jnp.zeros_like(pooled)

    def stage_two(layer, r):
        xhat, _ = ln_parts(r)
        n = xhat.astype(BF16)
        acc = r
        for q in QUADS:
            cols = slice(D2 * q, D2 * (q + 1))
            a = gelu_only(nn(n, wut[layer, :, cols])).astype(BF16)
            acc = acc + nn(a, wdt[layer, cols, :])
        return acc.astype(BF16)

    def first(t, carry):
        rows = ds(t * WIDE, WIDE)
        r = nn(r2[rows, :], wm[...]).astype(BF16).astype(F32)
        r2[rows, :] = stage_two(0, r)

        def both(i, inner):
            big_update(1, 2 * t + i)
            return inner

        lax.fori_loop(0, 2, both, 0)
        return carry

    lax.fori_loop(0, ROWS2 // WIDE, first, 0)

    wh[CLASSES:, :] = jnp.zeros((CPAD - CLASSES, D2), BF16)
    ins[6].wait()
    ins[7].wait()
    gh_cp.wait()
    for k in QUADS:
        rows = slice(TILE * k, min(TILE * (k + 1), CLASSES))
        nw, nv = update(sh[rows, :], th[rows, :], gh[rows, :], scal[9:10, 0:1])
        sh[rows, :] = nw
        th[rows, :] = nv
        wh[rows, :] = nw.astype(BF16)
    for cp in louts[6:]:
        cp.start()

    def second(t, carry):
        rows = ds(t * WIDE, WIDE)
        rb = stage_two(1, r2[rows, :].astype(F32))
        pooled[...] += nn(onehot_rows(t), rb)
        return carry

    lax.fori_loop(0, ROWS2 // WIDE, second, 0)
    xhat, _ = ln_parts(pooled[...] * (1.0 / MT))
    logits = nt(xhat.astype(BF16), wh[...])
    logits_out[...] = logits[:, 0:CLASSES]
    for cp in louts:
        cp.wait()
    for t in QUADS:
        for k in QUADS:
            qout(1, t, k).wait()


def weight_scratch():
    return [pltpu.VMEM((2, D1, H1), BF16), pltpu.VMEM((2, H1, D1), BF16), pltpu.VMEM((D2, D2), BF16), pltpu.VMEM((2, D2, H2), BF16), pltpu.VMEM((2, H2, D2), BF16), pltpu.VMEM((CPAD, D2), BF16)]


def master_scratch():
    return [pltpu.VMEM((2, D1, H1), F32), pltpu.VMEM((2, H1, D1), F32), pltpu.VMEM((D2, D2), F32), pltpu.VMEM((CLASSES, D2), F32), pltpu.VMEM((D2, H2), F32), pltpu.VMEM((H2, D2), F32)]


def solution(mesh):
    hbm = pl.BlockSpec(memory_space=pl.ANY)
    vmem = pl.BlockSpec(memory_space=pltpu.VMEM)
    smem = pl.BlockSpec(memory_space=pltpu.SMEM)
    shape = jax.ShapeDtypeStruct
    dma = pltpu.SemaphoreType.DMA
    wide_g = [shape((CH, ROWS2, D2), BF16), shape((H2, D2), BF16), shape((CPAD, D2), BF16)]
    masters = [shape((2, D1, H1), F32), shape((2, H1, D1), F32), shape((D2, D2), F32), shape((2, D2, H2), F32), shape((2, H2, D2), F32), shape((CLASSES, D2), F32)]

    grads_call = pl.pallas_call(
        grad_kernel,
        out_shape=wide_g + [shape((IMAGES, D1), F32)],
        in_specs=[hbm, smem] + [hbm] * 6,
        out_specs=[hbm] * 3 + [vmem],
        scratch_shapes=[pltpu.VMEM((CH, ROWS2 // k, D2), BF16) for k in (1, 2, 4, NDEV)]
        + [pltpu.VMEM((NDEV, 32, LRW), BF16)]
        + weight_scratch()
        + [pltpu.VMEM((ROWS2, D2), BF16), pltpu.VMEM((2, ROWS1, D1), BF16), pltpu.VMEM((ROWS1, 1), F32), pltpu.VMEM((ROWS2, D2), BF16), pltpu.VMEM((2, ROWS2, D2), BF16), pltpu.VMEM((2, ROWS2, 1), F32), pltpu.VMEM((ROWS2, H2), BF16), pltpu.VMEM((2, ROWS2, H2), BF16), pltpu.VMEM((IMAGES, D2), F32), pltpu.VMEM((IMAGES, H2), F32), pltpu.VMEM((2, H1, D1), F32), pltpu.VMEM((2, D1, H1), F32), pltpu.VMEM((10, SUB, D1), F32), pltpu.VMEM((10, SUB, D1), F32)]
        + [dma((5,)), dma((2,)), dma((CH + 2,)), dma((CH, 10)), dma((CH, 10)), pltpu.SemaphoreType.REGULAR((CH, 3)), dma((CH,)), dma((CH,))],
        compiler_params=pltpu.CompilerParams(collective_id=0, has_side_effects=True, vmem_limit_bytes=VMEM_LIMIT),
        name="grads",
    )

    step_call = pl.pallas_call(
        step_kernel,
        out_shape=[shape((IMAGES, CLASSES), F32)] + masters * 2,
        in_specs=[hbm] * 16 + [vmem],
        out_specs=[vmem] + [hbm] * 12,
        scratch_shapes=[pltpu.VMEM((ROWS1, D1), BF16), pltpu.VMEM((ROWS2, D1), F32)]
        + [pltpu.VMEM(g.shape, BF16) for g in wide_g]
        + master_scratch() * 2
        + weight_scratch()
        + [pltpu.VMEM((ROWS2, D2), BF16), pltpu.VMEM((IMAGES, D2), F32)]
        + [dma((SUB,)), dma((SUB,)), dma((4, 4)), dma((4, 4)), dma((CH + 3,))],
        compiler_params=pltpu.CompilerParams(vmem_limit_bytes=VMEM_LIMIT),
        name="step",
    )

    def local_step(x_now, labels_now, x_next, up_one, down_one, merge_proj, up_two, down_two, head_proj, vel_up_one, vel_down_one, vel_merge_proj, vel_up_two, vel_down_two, vel_head_proj):
        params = (up_one, down_one, merge_proj, up_two, down_two, head_proj.T)
        vels = (vel_up_one, vel_down_one, vel_merge_proj, vel_up_two, vel_down_two, vel_head_proj.T)
        got = grads_call(x_now.reshape(ROWS1, D1), labels_now, *params)
        outs = list(step_call(x_next.reshape(ROWS1, D1), *params, *vels, *got))
        outs[6], outs[12] = outs[6].T, outs[12].T
        return tuple(outs)

    replicated = P()
    batch_split = P('data')
    in_specs = (batch_split, batch_split, batch_split) + (replicated,) * 12
    out_specs = (batch_split,) + (replicated,) * 12
    return jax.shard_map(local_step, mesh=mesh, in_specs=in_specs, out_specs=out_specs, check_vma=False)
```

```python
import jax
import jax.numpy as jnp
from jax import lax
from jax.experimental import pallas as pl
from jax.experimental.pallas import tpu as pltpu
from jax.sharding import PartitionSpec as P

MOMENTUM = 0.9
TRUST = 0.1
LN_EPS = 1e-6
GELU_C = 0.7978845608028654
GELU_K = 0.044715
MESH = pl.DeviceIdType.MESH
F32 = jnp.float32
BF16 = jnp.bfloat16
VMEM_LIMIT = 67043328

IMAGES = 16
TOKENS = 256
D1 = 128
H1 = 512
D2 = 512
H2 = 2048
ROWS1 = IMAGES * TOKENS
ROWS2 = ROWS1 // 4
CLASSES = 1000
CPAD = 1024
TILE = 256
NTILE = ROWS2 // TILE
WIDE = 512
HEAD_STEP = 192
CH = 7
LETTERS = 'abcdefg'
NORM_ROW = dict(a=5, b=5, c=6, d=6, e=4, f=4)
LRW = 3072
LRG = 2560
NDEV = 8
MT = 64
SUB = 8
PAIR = range(2)
QUADS = range(4)
DOWNS = (2, 3)
CHUNK = 32768


def nn(a, b):
    return lax.dot_general(a, b, (((1,), (0,)), ((), ())), preferred_element_type=F32)


def nt(a, b):
    return lax.dot_general(a, b, (((1,), (1,)), ((), ())), preferred_element_type=F32)


def tn(a, b):
    return lax.dot_general(a, b, (((0,), (0,)), ((), ())), preferred_element_type=F32)


def gelu_only(x):
    inner = x * (GELU_C + (GELU_C * GELU_K) * (x * x))
    half = 0.5 + 0.5 * jnp.tanh(inner)
    return x * half


def gelu_pair(x):
    x2 = x * x
    t = jnp.tanh(x * (GELU_C + (GELU_C * GELU_K) * x2))
    half = 0.5 + 0.5 * t
    act = x * half
    slope = half + act * ((1.0 - t) * (GELU_C + (3.0 * GELU_C * GELU_K) * x2))
    return act, slope


def ln_parts(r):
    mean = jnp.mean(r, axis=-1, keepdims=True)
    cen = r - mean
    var = jnp.mean(cen * cen, axis=-1, keepdims=True)
    rstd = lax.rsqrt(var + LN_EPS)
    return cen * rstd, rstd


def ln_back(dy, xhat, rstd):
    m1 = jnp.mean(dy, axis=-1, keepdims=True)
    m2 = jnp.mean(dy * xhat, axis=-1, keepdims=True)
    return rstd * (dy - m1 - xhat * m2)


def fold_sq(v):
    rows, cols = v.shape
    s = jnp.sum((v * v).reshape(rows // SUB, SUB, cols), axis=0)
    out = s[:, 0:D1]
    for q in range(1, cols // D1):
        out = out + s[:, D1 * q:D1 * (q + 1)]
    return out


def total(acc):
    return jnp.sum(jnp.sum(acc, axis=1, keepdims=True), axis=0, keepdims=True)


def ds(start, size, mult=None):
    if isinstance(start, int):
        return pl.ds(start, size)
    return pl.ds(pl.multiple_of(start, mult or size), size)


def onehot_rows(t):
    row = lax.broadcasted_iota(jnp.int32, (IMAGES, WIDE), 0)
    col = lax.broadcasted_iota(jnp.int32, (IMAGES, WIDE), 1)
    return jnp.where(row == t * (WIDE // MT) + col // MT, 1.0, 0.0).astype(BF16)


def stage_one_tile(t, xb, xf, wuo, wdo, dst):
    xf[...] = xb[ds(t * ROWS2, ROWS2), :].astype(F32)
    r = jnp.concatenate([xf[pl.ds(j, TILE, stride=4), :] for j in QUADS], axis=0)
    for b in PAIR:
        xhat, _ = ln_parts(r)
        a = gelu_only(nn(xhat.astype(BF16), wuo[b])).astype(BF16)
        rb = (r + nn(a, wdo[b])).astype(BF16)
        r = rb.astype(F32)
    for j in QUADS:
        dst[ds(t * TILE, TILE), D1 * j:D1 * (j + 1)] = rb[TILE * j:TILE * (j + 1), :]


def update(w, v, g, scale):
    nv = MOMENTUM * v + scale * g.astype(F32)
    nw = w - nv
    return nw, nv


class Ring:
    def __init__(self, num, g, r1, r2, r3, ssem, rsem, csem, pos):
        self.num = num
        self.g, self.r1, self.r2, self.r3 = (ref.at[num] for ref in (g, r1, r2, r3))
        self.ssem, self.rsem, self.csem = ssem, rsem, csem
        self.pos = pos
        self.rb = g.shape[1] // NDEV
        c, f, s = pos['c'], pos['f'], pos['s']
        self.f, self.s, self.nf, self.ns = f, s, 1 - f, 1 - s
        self.mine, self.other = 4 * c, 4 - 4 * c
        self.keep = self.mine + 2 * f
        self.give = self.mine + 2 * self.nf
        self.own_b, self.s_b = self.keep + s, self.keep + self.ns
        self.f_b, self.d_b = self.give + s, self.give + self.ns

    def blk(self, b, n=1):
        return self.g.at[ds(b * self.rb, n * self.rb, self.rb)]

    def rc(self, k, src, dst, dev):
        return pltpu.make_async_remote_copy(src_ref=src, dst_ref=dst, send_sem=self.ssem.at[self.num, k], recv_sem=self.rsem.at[self.num, k], device_id=(self.pos[dev],), device_id_type=MESH)

    def add(self, b, recv, i, n):
        rows, width = n * self.rb, self.g.shape[1]
        step = min(rows, CHUNK // width)
        b0, i0 = b * self.rb, i * self.rb

        def body(j, carry):
            dst = ds(b0 + j * step, step)
            src = ds(i0 + j * step, step)
            self.g[dst, :] = (self.g[dst, :].astype(F32) + recv[src, :].astype(F32)).astype(BF16)
            return carry

        lax.fori_loop(0, rows // step, body, 0)

    def to_core(self):
        return self.rc(0, self.blk(self.other, 4), self.r1, 'core')

    def to_f(self):
        return self.rc(1, self.blk(self.give, 2), self.r2, 'fn')

    def to_s(self):
        return self.rc(2, self.blk(self.s_b), self.r3, 'sn')

    def back(self, k, b, dev):
        return self.rc(k, self.blk(b), self.blk(b), dev)

    def own_to_s(self):
        return self.back(3, self.own_b, 'sn')

    def own_to_f(self):
        return self.back(4, self.own_b, 'fn')

    def own_to_core(self):
        return self.back(5, self.own_b, 'core')

    def s_to_f(self):
        return self.back(6, self.s_b, 'fn')

    def s_to_core(self):
        return self.back(7, self.s_b, 'core')

    def f_to_core(self):
        return self.back(8, self.f_b, 'core')

    def d_to_core(self):
        return self.back(9, self.d_b, 'core')

    def half(self):
        self.to_core().start()

    def link_f(self):
        self.to_core().wait_recv()
        self.add(self.give, self.r1, 2 * self.nf, 2)
        self.to_f().start()
        self.add(self.keep, self.r1, 2 * self.f, 2)

    def link_s(self):
        self.to_f().wait_recv()
        self.add(self.s_b, self.r2, self.ns, 1)
        self.to_s().start()
        self.add(self.own_b, self.r2, self.s, 1)
        self.to_core().wait_send()
        self.free(0, 'core')
        self.to_f().wait_send()
        self.free(1, 'fn')

    def own(self):
        self.to_s().wait_recv()
        self.to_s().wait_send()
        self.free(2, 'sn')
        self.add(self.own_b, self.r3, 0, 1)
        self.held(1)
        self.own_to_f().start()
        self.held(0)
        self.own_to_core().start()

    def own_s(self):
        self.held(2)
        self.own_to_s().start()

    def pass_s(self):
        self.own_to_s().wait_recv()
        self.s_to_f().start()
        self.s_to_core().start()

    def pass_f(self):
        self.own_to_f().wait_recv()
        self.f_to_core().start()

    def pass_d(self):
        self.s_to_f().wait_recv()
        self.d_to_core().start()

    def done(self):
        for cp in (self.own_to_core(), self.s_to_core(), self.f_to_core(), self.d_to_core()):
            cp.wait()
        for cp in (self.own_to_s(), self.own_to_f(), self.s_to_f()):
            cp.wait_send()

    def free(self, i, who):
        pl.semaphore_signal(self.csem.at[self.num, i], inc=1, device_id=(self.pos[who],), device_id_type=MESH)

    def held(self, i):
        pl.semaphore_wait(self.csem.at[self.num, i], 1)


class Share:
    def __init__(self, buf, ssem, rsem, pos):
        self.buf, self.ssem, self.rsem, self.pos = buf, ssem, rsem, pos

    def rc(self, k):
        p = self.pos
        own, fblk, sblk, dblk = p['me'], p['fn'], p['sn'], p['diag']
        b, dev = {0: (own, 'fn'), 1: (own, 'sn'), 2: (own, 'core'), 3: (fblk, 'sn'), 4: (fblk, 'core'), 5: (sblk, 'core'), 6: (dblk, 'core')}[k]
        return pltpu.make_async_remote_copy(src_ref=self.buf.at[b], dst_ref=self.buf.at[b], send_sem=self.ssem.at[k], recv_sem=self.rsem.at[k], device_id=(p[dev],), device_id_type=MESH)


    def send(self):
        for k in (0, 1, 2):
            self.rc(k).start()

    def relay(self):
        self.rc(0).wait_recv()
        self.rc(3).start()
        self.rc(4).start()
        self.rc(1).wait_recv()
        self.rc(5).start()

    def done(self):
        self.rc(3).wait_recv()
        self.rc(6).start()
        for k in (2, 4, 5, 6):
            self.rc(k).wait_recv()
        for k in range(7):
            self.rc(k).wait_send()


def position():
    me = lax.axis_index('data')
    c = lax.rem(me, 2)
    x = lax.rem(me // 2, 2)
    y = me // 4
    f = c * y + (1 - c) * x
    s = c * x + (1 - c) * y
    xn = me + 2 - 4 * x
    yn = me + 4 - SUB * y
    fn = c * yn + (1 - c) * xn
    sn = c * xn + (1 - c) * yn
    diag = xn + yn - me
    core = me + 1 - 2 * c
    return dict(me=me, c=c, f=f, s=s, fn=fn, sn=sn, diag=diag, core=core)


STEPS = ('half', 'link_f', 'link_s', 'own', 'own_s', 'pass_s', 'pass_f', 'pass_d', 'done')
SHARE_STEPS = ('send', 'relay', 'done')
PLAN = dict(
    up1=((), ('a0',), (), ('b0',),),
    in1=(('a1',), ('s1',), ('b1',), (),),
    dn0=((), ('c0',), (), ('d0',),),
    pre0=(('a2', 'c1', 's2',), ('d1',), (), ('b2',),),
    up0=((), ('a3', 'e0',), (), ('a4', 'f0',),),
    in0=(('e1', 'c2', 'b3',), ('f1', 'b4',), (), ('a5',),),
    mrg=((),),
    back=(('a6', 'c3', 'd2',), ('b5', 'c4', 'e2',), ('b6', 'd3',), ('c5', 'd4', 'e3', 'a7', 'f2', 'g0',),),
    rank=(('c6', 'a8', 'e4',), ('g1', 'b7',), ('d5',), ('b8', 'd6',),),
    rankh=((), ('f3',), (), ('c7', 'f4',),),
    tail=('e5', 'e6', 'c8', 'f5', 'g2', 'd7', 'd8', 'f6', 'g3', 'e7', 'g4', 'f7', 'e8', 'f8', 'g5', 'g6', 'g7', 'g8', ),
)


def grad_kernel(x_hbm, lab, uo_hbm, do_hbm, m_hbm, ut_hbm, dt_hbm, h_hbm,
                g_out, gv1_out, gh_out, scal,
                g_all, r1_all, r2_all, r3_all, lr, gdup,
                wuo, wdo, wm, wut, wdt, wh,
                merged, n1, rst1, r2, n2, rst2, a2, sl2, pooled, asum, accv, accu, sq, gsq,
                in_sem, st_sem, out_sem, ssem, rsem, csem, lssem, lrsem):
    pos = position()
    barrier = pltpu.get_barrier_semaphore()
    for who in ('core', 'fn', 'sn'):
        pl.semaphore_signal(barrier, inc=1, device_id=(pos[who],), device_id_type=MESH)

    gv1, gh, grad = wdt.at[1], wh, r2

    share = Share(lr, lssem, lrsem, pos)
    rings = {letter: Ring(i, g_all, r1_all, r2_all, r3_all, ssem, rsem, csem, pos) for i, letter in enumerate(LETTERS)}
    outs = {letter: pltpu.make_async_copy(g_all.at[i], g_out.at[i], out_sem.at[i]) for i, letter in enumerate(LETTERS)}

    def norm_of(letter):
        ref = g_all.at[LETTERS.index(letter)]

        def body(i, acc):
            return acc + fold_sq(ref[ds(i * MT, MT), :].astype(F32))

        gsq[NORM_ROW[letter]] += lax.fori_loop(0, ROWS2 // MT, body, jnp.zeros((SUB, D1), F32))

    def act(word):
        letter, num = word[0], int(word[1])
        if letter == 's':
            getattr(share, SHARE_STEPS[num])()
        else:
            getattr(rings[letter], STEPS[num])()
            if STEPS[num] == 'done':
                outs[letter].start()
                if letter in NORM_ROW:
                    norm_of(letter)

    def run(name, body):
        plan = PLAN[name]

        def wrapped(t, carry):
            body(t)
            for i, words in enumerate(plan):
                if words:
                    @pl.when(t == i)
                    def _():
                        for word in words:
                            act(word)
            return carry

        lax.fori_loop(0, len(plan), wrapped, 0)

    def forward(xb, xf, suo, sdo, sm, sut, sdt, abuf):
        loads = [pltpu.make_async_copy(src, dst, in_sem.at[i]) for i, (src, dst) in enumerate(((x_hbm, xb), (uo_hbm, suo), (do_hbm, sdo), (m_hbm, sm), (h_hbm, sdt.at[0:CLASSES])))]

        def stage_up(i):
            return pltpu.make_async_copy(ut_hbm.at[i // 2, ds((i % 2) * TILE, TILE)], sut, st_sem.at[0])

        def stage_down(i):
            return pltpu.make_async_copy(dt_hbm.at[i // 2, ds((i % 2) * ROWS2, ROWS2)], sdt, st_sem.at[1])

        for cp in loads[:3]:
            cp.start()
        stage_up(0).start()
        stage_down(0).start()
        loads[3].start()
        sq[...] = jnp.zeros_like(sq)
        for cp in loads[:3]:
            cp.wait()
        for b in PAIR:
            v = suo[b]
            sq[b] = fold_sq(v)
            wuo[b] = v.astype(BF16)
            v = sdo[b]
            sq[2 + b] = fold_sq(v)
            wdo[b] = v.astype(BF16)

        def stage_one(t, carry):
            xf[...] = xb[ds(t * ROWS2, ROWS2), :].astype(F32)
            r = jnp.concatenate([xf[pl.ds(j, TILE, stride=4), :] for j in QUADS], axis=0)
            rows = ds(t * ROWS2, ROWS2)
            for b in PAIR:
                xhat, rstd = ln_parts(r)
                n = xhat.astype(BF16)
                n1[b, rows, :] = n
                if b == 1:
                    rst1[rows, :] = rstd
                a = gelu_only(nn(n, wuo[b])).astype(BF16)
                rb = (r + nn(a, wdo[b])).astype(BF16)
                r = rb.astype(F32)
            for j in QUADS:
                merged[ds(t * TILE, TILE), D1 * j:D1 * (j + 1)] = rb[TILE * j:TILE * (j + 1), :]
            layer = t // 2
            stage_up(t).wait()

            def cast_up(i, acc):
                v = sut[ds(i * 32, 32), :]
                wut[layer, ds((t % 2) * TILE + i * 32, 32), :] = v.astype(BF16)
                return acc + fold_sq(v)

            sq[4 + layer] += lax.fori_loop(0, SUB, cast_up, jnp.zeros((SUB, D1), F32))
            stage_down(t).wait()

            def cast_down(i, acc):
                v = sdt[ds(i * D1, D1), :]
                wdt[layer, ds((t % 2) * ROWS2 + i * D1, D1), :] = v.astype(BF16)
                return acc + fold_sq(v)

            sq[6 + layer] += lax.fori_loop(0, SUB, cast_down, jnp.zeros((SUB, D1), F32))

            @pl.when(t < 3)
            def _():
                stage_up(t + 1).start()
                stage_down(t + 1).start()

            return carry

        lax.fori_loop(0, NTILE, stage_one, 0)

        loads[4].start()
        loads[3].wait()

        def cast_m(i, acc):
            v = sm[ds(i * MT, MT), :]
            wm[ds(i * MT, MT), :] = v.astype(BF16)
            return acc + fold_sq(v)

        sq[SUB] = lax.fori_loop(0, SUB, cast_m, jnp.zeros((SUB, D1), F32))

        def merge_tile(t, carry):
            rows = ds(t * WIDE, WIDE)
            r2[rows, :] = nn(merged[rows, :], wm[...]).astype(BF16)
            return carry

        lax.fori_loop(0, ROWS2 // WIDE, merge_tile, 0)
        asum[...] = jnp.zeros_like(asum)
        pooled[...] = jnp.zeros_like(pooled)

        for layer in PAIR:
            def stage_two(t, carry):
                rows = ds(t * WIDE, WIDE)
                r = r2[rows, :].astype(F32)
                xhat, rstd = ln_parts(r)
                n = xhat.astype(BF16)
                n2[layer, rows, :] = n
                rst2[layer, rows, :] = rstd
                for q in QUADS:
                    cols = slice(D2 * q, D2 * (q + 1))
                    acts, slope = gelu_pair(nn(n, wut[layer, :, cols]))
                    if layer == 0:
                        a2[rows, cols] = acts.astype(BF16)
                    else:
                        abuf[:, cols] = acts.astype(BF16)
                    sl2[layer, rows, cols] = slope.astype(BF16)
                if layer == 0:
                    r2[rows, :] = (r + nn(a2[rows, :], wdt[layer])).astype(BF16)
                else:
                    rb = (r + nn(abuf[...], wdt[layer])).astype(BF16)
                    pick = onehot_rows(t)
                    asum[...] += nn(pick, abuf[...])
                    pooled[...] += nn(pick, rb)
                return carry

            lax.fori_loop(0, ROWS2 // WIDE, stage_two, 0)
        wh[CLASSES:, :] = jnp.zeros((CPAD - CLASSES, D2), BF16)
        loads[4].wait()
        for k in QUADS:
            rows = slice(TILE * k, min(TILE * (k + 1), CLASSES))
            v = sdt[rows, :]
            wh[rows, :] = v.astype(BF16)
            sq[9] += fold_sq(v)

    pl.run_scoped(
        forward,
        pltpu.VMEM((ROWS1, D1), BF16),
        pltpu.VMEM((ROWS2, D1), F32),
        pltpu.VMEM((2, D1, H1), F32),
        pltpu.VMEM((2, H1, D1), F32),
        pltpu.VMEM((D2, D2), F32),
        pltpu.VMEM((TILE, H2), F32),
        pltpu.VMEM((ROWS2, D2), F32),
        pltpu.VMEM((WIDE, H2), BF16),
    )

    xhat, rstd = ln_parts(pooled[...] * (1.0 / MT))
    hb = xhat.astype(BF16)
    logits = nt(hb, wh[...])
    col = lax.broadcasted_iota(jnp.int32, (IMAGES, CPAD), 1)
    row = lax.broadcasted_iota(jnp.int32, (IMAGES, CPAD), 0)
    logits = jnp.where(col < CLASSES, logits, -jnp.inf)
    ex = jnp.exp(logits - jnp.max(logits, axis=-1, keepdims=True))
    prob = ex / jnp.sum(ex, axis=-1, keepdims=True)
    lab_row = jnp.zeros((IMAGES, CPAD), jnp.int32)
    for i in range(IMAGES):
        lab_row = jnp.where(row == i, lab[i], lab_row)
    gl = ((prob - jnp.where(col == lab_row, 1.0, 0.0)) * (1.0 / (IMAGES * NDEV))).astype(BF16)
    g16 = (ln_back(nn(gl, wh[...]), xhat, rstd) * (1.0 / MT)).astype(BF16)
    hi = asum[...].astype(BF16)
    lo = (asum[...] - hi.astype(F32)).astype(BF16)
    me = pos['me']
    lr[me, 0:IMAGES, 0:H2] = hi
    lr[me, IMAGES:32, 0:H2] = lo
    lr[me, 0:IMAGES, H2:LRG] = g16
    lr[me, IMAGES:32, H2:LRG] = hb
    lr[me, 0:IMAGES, LRG:LRW] = gl[:, 0:D2]
    lr[me, IMAGES:32, LRG:LRW] = gl[:, D2:CPAD]
    pl.semaphore_wait(barrier, 3)
    share.send()

    asum[...] = nt(g16, wdt[1])
    pooled[...] = g16.astype(F32)

    def slope_one(i, carry):
        rows = ds(i * MT, MT)
        grad[rows, :] = jnp.broadcast_to(pooled[pl.ds(i, 1), :], (MT, D2)).astype(BF16)
        for q in QUADS:
            cols = slice(D2 * q, D2 * (q + 1))
            sl2[1, rows, cols] = (asum[pl.ds(i, 1), cols] * sl2[1, rows, cols].astype(F32)).astype(BF16)
        return carry

    lax.fori_loop(0, IMAGES, slope_one, 0)

    def up_grad(layer, first):
        def body(q):
            g_all[first + q // 2, ds((q % 2) * D2, D2), :] = tn(n2[layer], sl2[layer, :, ds(q * D2, D2)]).astype(BF16)

        return body

    def down_grad(q):
        g_all[2 + q // 2, ds((q % 2) * D2, D2), :] = tn(a2[:, ds(q * D2, D2)], grad[...]).astype(BF16)

    def input_grad(layer):
        def body(t):
            rows = ds(t * TILE, TILE)
            dy = nt(sl2[layer, rows, :], wut[layer])
            dx = ln_back(dy, n2[layer, rows, :].astype(F32), rst2[layer, rows, :])
            grad[rows, :] = (dx + grad[rows, :].astype(F32)).astype(BF16)

        return body

    def pre_grad(t):
        rows = ds(t * TILE, TILE)
        for q in QUADS:
            cols = slice(D2 * q, D2 * (q + 1))
            ga = nt(grad[rows, :], wdt[0, cols, :])
            sl2[0, rows, cols] = (ga * sl2[0, rows, cols].astype(F32)).astype(BF16)

    gsm = g_all.at[CH - 1]

    def merge_grad(t):
        gsm[D2:ROWS2, :] = tn(merged[...], grad[...]).astype(BF16)

    def stage_one_back(t):
        gm = nt(grad[ds(t * TILE, TILE), :], wm[...]).astype(BF16)
        rows = ds(t * ROWS2, ROWS2)
        g = jnp.concatenate([gm[:, D1 * j:D1 * (j + 1)] for j in QUADS], axis=0)
        for b in (1, 0):
            n = n1[b, rows, :]
            acts, slope = gelu_pair(nn(n, wuo[b]))
            accv[b] += tn(acts.astype(BF16), g)
            gp = (nt(g, wdo[b]) * slope).astype(BF16)
            accu[b] += tn(n, gp)
            if b == 1:
                dx = ln_back(nt(gp, wuo[b]), n.astype(F32), rst1[rows, :])
                g = (dx + g.astype(F32)).astype(BF16)

        @pl.when(t == 3)
        def _():
            for b in PAIR:
                gsm[D1 * b:D1 * (b + 1), :] = accu[b].astype(BF16)
                for q in PAIR:
                    gsm[TILE:D2, TILE * b + D1 * q:TILE * b + D1 * (q + 1)] = accv[b, TILE * q:TILE * (q + 1), :].astype(BF16)

    run('up1', up_grad(1, 0))
    run('in1', input_grad(1))
    run('dn0', down_grad)
    run('pre0', pre_grad)
    run('up0', up_grad(0, 4))
    run('in0', input_grad(0))
    accv[...] = jnp.zeros_like(accv)
    accu[...] = jnp.zeros_like(accu)
    gsq[...] = jnp.zeros_like(gsq)
    run('mrg', merge_grad)
    run('back', stage_one_back)

    def v1_rows(i):
        cols = ds(i * D2, D2)
        out = jnp.zeros((D2, D2), F32)
        for d in range(NDEV):
            out = out + tn(lr[d, :, cols], gdup[d]).astype(BF16).astype(F32)
        ob = out.astype(BF16)
        gv1[cols, :] = ob
        gsq[7] += fold_sq(ob.astype(F32))

    def head_rows(i):
        rows = ds(i * TILE, TILE)
        out = jnp.zeros((TILE, D2), F32)
        for d in range(NDEV):
            gl_d = lr[d, ds((i // 2) * IMAGES, IMAGES), ds(LRG + (i % 2) * TILE, TILE)]
            out = out + tn(gl_d, lr[d, IMAGES:32, H2:LRG]).astype(BF16).astype(F32)
        ob = out.astype(BF16)
        gh[rows, :] = ob
        gsq[9] += fold_sq(ob.astype(F32))

    gv1_cp = pltpu.make_async_copy(gv1, gv1_out, out_sem.at[CH])
    gh_cp = pltpu.make_async_copy(gh, gh_out, out_sem.at[CH + 1])
    for d in range(NDEV):
        gdup[d, 0:IMAGES, :] = lr[d, 0:IMAGES, H2:LRG]
        gdup[d, IMAGES:32, :] = lr[d, 0:IMAGES, H2:LRG]
    run('rank', v1_rows)
    gv1_cp.start()
    run('rankh', head_rows)
    gh_cp.start()
    for word in PLAN['tail']:
        act(word)
    for b in PAIR:
        gsq[b] = fold_sq(gsm[D1 * b:D1 * (b + 1), :].astype(F32))
        gsq[2 + b] = fold_sq(gsm[TILE:D2, TILE * b:TILE * (b + 1)].astype(F32))
    gsq[SUB] = fold_sq(gsm[D2:ROWS2, :].astype(F32))
    for i in range(10):
        ratio = jnp.sqrt(total(sq[i])) / jnp.sqrt(total(gsq[i]))
        scal[i:i + 1, :] = jnp.broadcast_to(TRUST * ratio, (1, D1))
    scal[10:IMAGES, :] = jnp.zeros((6, D1), F32)
    for letter in LETTERS:
        outs[letter].wait()
    gv1_cp.wait()
    gh_cp.wait()


def step_kernel(x_hbm, uo_hbm, do_hbm, m_hbm, ut_hbm, dt_hbm, h_hbm, vuo_hbm, vdo_hbm, vm_hbm, vut_hbm, vdt_hbm, vh_hbm,
                g_hbm, gv1_hbm, gh_hbm, scal,
                logits_out, uo_out, do_out, m_out, ut_out, dt_out, h_out, vuo_out, vdo_out, vm_out, vut_out, vdt_out, vh_out,
                xb, xf, g_all, gv1, gh, suo, sdo, sm, sh, sut, sdt, tuo, tdo, tm, th, tut, tdt,
                wuo, wdo, wm, wut, wdt, wh, r2, pooled,
                s_in, s_out, q_in, q_out, g_sem):
    small = [(uo_hbm, suo, uo_out), (vuo_hbm, tuo, vuo_out), (do_hbm, sdo, do_out), (vdo_hbm, tdo, vdo_out), (m_hbm, sm, m_out), (vm_hbm, tm, vm_out), (h_hbm, sh, h_out), (vh_hbm, th, vh_out)]
    ins = [pltpu.make_async_copy(src, buf, s_in.at[i]) for i, (src, buf, _) in enumerate(small)]
    louts = [pltpu.make_async_copy(buf, dst, s_out.at[i]) for i, (_, buf, dst) in enumerate(small)]
    up_big = [(ut_hbm, sut, ut_out), (vut_hbm, tut, vut_out)]
    down_big = [(dt_hbm, sdt, dt_out), (vdt_hbm, tdt, vdt_out)]
    gsm = g_all.at[CH - 1]

    def copies(layer, t, into, which=QUADS):
        out = []
        for k in which:
            src, buf, dst = (up_big + down_big)[k]
            n = D1 if k in PAIR else D2
            rows = ds(t * n, n)
            here = buf.at[rows] if k in PAIR else buf.at[layer, rows]
            if into:
                out.append(pltpu.make_async_copy(src.at[layer, rows], here, q_in.at[layer, k, t]))
            else:
                out.append(pltpu.make_async_copy(here, dst.at[layer, rows], q_out.at[layer, k, t]))
        return out

    def start(cps):
        for cp in cps:
            cp.start()

    def wait(cps):
        for cp in cps:
            cp.wait()

    x_cp = pltpu.make_async_copy(x_hbm, xb, g_sem.at[CH])
    g_cps = [pltpu.make_async_copy(g_hbm.at[i], g_all.at[i], g_sem.at[i]) for i in range(CH)]
    gv1_cp = pltpu.make_async_copy(gv1_hbm, gv1, g_sem.at[CH + 1])
    gh_cp = pltpu.make_async_copy(gh_hbm, gh, g_sem.at[CH + 2])

    def up_part(layer, t):
        scale = scal[4 + layer:5 + layer, 0:1]
        rows = ds(t * D1, D1)
        for q in QUADS:
            cols = slice(D2 * q, D2 * (q + 1))
            g = g_all[4 - 4 * layer + q // 2, ds((q % 2) * D2 + t * D1, D1), :]
            nw, nv = update(sut[rows, cols], tut[rows, cols], g, scale)
            sut[rows, cols] = nw
            tut[rows, cols] = nv
            wut[layer, rows, cols] = nw.astype(BF16)

    def down_part(layer, t):
        rows = ds(t * D2, D2)
        g = g_all[2 + t // 2, ds((t % 2) * D2, D2), :] if layer == 0 else gv1[rows, :]
        nw, nv = update(sdt[layer, rows, :], tdt[layer, rows, :], g, scal[6 + layer:7 + layer, 0:1])
        sdt[layer, rows, :] = nw
        tdt[layer, rows, :] = nv
        wdt[layer, rows, :] = nw.astype(BF16)

    def stage_two(layer, r):
        xhat, _ = ln_parts(r)
        n = xhat.astype(BF16)
        acc = r
        for q in QUADS:
            cols = slice(D2 * q, D2 * (q + 1))
            a = gelu_only(nn(n, wut[layer, :, cols])).astype(BF16)
            acc = acc + nn(a, wdt[layer, cols, :])
        return acc.astype(BF16)

    first_in = [x_cp, g_cps[CH - 1]] + ins[:4]
    early = [g_cps[i] for i in (4, 5, 2)]
    later = [g_cps[0], g_cps[1], gv1_cp]
    start(first_in)
    start(early)
    start(copies(0, 0, True))
    wait(first_in)
    for b in PAIR:
        nw, tuo[b] = update(suo[b], tuo[b], gsm[D1 * b:D1 * (b + 1), :], scal[b:b + 1, 0:1])
        suo[b] = nw
        wuo[b] = nw.astype(BF16)
        for q in PAIR:
            rows = slice(TILE * q, TILE * (q + 1))
            nw, tdo[b, rows, :] = update(sdo[b, rows, :], tdo[b, rows, :], gsm[TILE:D2, TILE * b + D1 * q:TILE * b + D1 * (q + 1)], scal[2 + b:3 + b, 0:1])
            sdo[b, rows, :] = nw
            wdo[b, rows, :] = nw.astype(BF16)
    wait(early)

    def stage_one_update(t, carry):
        wait(copies(0, t, True))

        @pl.when(t < 3)
        def _():
            start(copies(0, t + 1, True))

        @pl.when(t == 0)
        def _():
            start([g_cps[3]])

        @pl.when(t == 1)
        def _():
            start(ins[4:6])

        @pl.when(t == 2)
        def _():
            wait([g_cps[3]])
            start(later)

        @pl.when(t == 3)
        def _():
            start(copies(1, 0, True, DOWNS))
            start(copies(1, 1, True, DOWNS))
            start([gh_cp] + ins[6:])

        stage_one_tile(t, xb, xf, wuo, wdo, r2)
        up_part(0, t)
        down_part(0, t)
        start(copies(0, t, False, PAIR))
        return carry

    lax.fori_loop(0, NTILE, stage_one_update, 0)
    start(copies(1, 2, True, DOWNS))
    start(copies(1, 3, True, DOWNS))
    wait(ins[4:6])
    nw, tm[...] = update(sm[...], tm[...], gsm[D2:ROWS2, :], scal[SUB:9, 0:1])
    sm[...] = nw
    wm[...] = nw.astype(BF16)

    def merge_tile(t, carry):
        rows = ds(t * WIDE, WIDE)
        r2[rows, :] = nn(r2[rows, :], wm[...]).astype(BF16)
        return carry

    lax.fori_loop(0, ROWS2 // WIDE, merge_tile, 0)
    wait(later)
    pooled[...] = jnp.zeros_like(pooled)

    def first(t, carry):
        rows = ds(t * WIDE, WIDE)
        for i in PAIR:
            wait(copies(0, 2 * t + i, False, PAIR))
            start(copies(1, 2 * t + i, True, PAIR))
        for i in PAIR:
            wait(copies(1, 2 * t + i, True, DOWNS))
            start(copies(0, 2 * t + i, False, DOWNS))
        r2[rows, :] = stage_two(0, r2[rows, :].astype(F32))
        for i in PAIR:
            down_part(1, 2 * t + i)
        return carry

    lax.fori_loop(0, ROWS2 // WIDE, first, 0)
    def second_up(t, carry):
        wait(copies(1, t, True, PAIR))
        up_part(1, t)
        start(copies(1, t, False))
        return carry

    lax.fori_loop(0, NTILE, second_up, 0)
    start(louts[:6])
    wh[CLASSES:, :] = jnp.zeros((CPAD - CLASSES, D2), BF16)
    wait(ins[6:] + [gh_cp])

    def head_update(rows):
        nw, th[rows, :] = update(sh[rows, :], th[rows, :], gh[rows, :], scal[9:10, 0:1])
        sh[rows, :] = nw
        wh[rows, :] = nw.astype(BF16)

    def head_part(i, carry):
        head_update(ds(i * HEAD_STEP, HEAD_STEP))
        return carry

    lax.fori_loop(0, CLASSES // HEAD_STEP, head_part, 0)
    head_update(slice(CLASSES - CLASSES % HEAD_STEP, CLASSES))
    start(louts[6:])

    def second(t, carry):
        rows = ds(t * WIDE, WIDE)
        rb = stage_two(1, r2[rows, :].astype(F32))
        pooled[...] += nn(onehot_rows(t), rb)
        return carry

    lax.fori_loop(0, ROWS2 // WIDE, second, 0)
    xhat, _ = ln_parts(pooled[...] * (1.0 / MT))
    logits = nt(xhat.astype(BF16), wh[...])
    logits_out[...] = logits[:, 0:CLASSES]
    wait(louts)
    for t in QUADS:
        wait(copies(0, t, False, DOWNS))
        wait(copies(1, t, False))


def weight_scratch():
    return [pltpu.VMEM((2, D1, H1), BF16), pltpu.VMEM((2, H1, D1), BF16), pltpu.VMEM((D2, D2), BF16), pltpu.VMEM((2, D2, H2), BF16), pltpu.VMEM((2, H2, D2), BF16), pltpu.VMEM((CPAD, D2), BF16)]


def master_scratch():
    return [pltpu.VMEM((2, D1, H1), F32), pltpu.VMEM((2, H1, D1), F32), pltpu.VMEM((D2, D2), F32), pltpu.VMEM((CLASSES, D2), F32), pltpu.VMEM((D2, H2), F32), pltpu.VMEM((2, H2, D2), F32)]


def solution(mesh):
    hbm = pl.BlockSpec(memory_space=pl.ANY)
    vmem = pl.BlockSpec(memory_space=pltpu.VMEM)
    smem = pl.BlockSpec(memory_space=pltpu.SMEM)
    shape = jax.ShapeDtypeStruct
    dma = pltpu.SemaphoreType.DMA
    wide_g = [shape((CH, ROWS2, D2), BF16), shape((H2, D2), BF16), shape((CPAD, D2), BF16)]
    masters = [shape((2, D1, H1), F32), shape((2, H1, D1), F32), shape((D2, D2), F32), shape((2, D2, H2), F32), shape((2, H2, D2), F32), shape((CLASSES, D2), F32)]

    grads_call = pl.pallas_call(
        grad_kernel,
        out_shape=wide_g + [shape((IMAGES, D1), F32)],
        in_specs=[hbm, smem] + [hbm] * 6,
        out_specs=[hbm] * 3 + [vmem],
        scratch_shapes=[pltpu.VMEM((CH, ROWS2 // k, D2), BF16) for k in (1, 2, 4, NDEV)]
        + [pltpu.VMEM((NDEV, 32, LRW), BF16), pltpu.VMEM((NDEV, 32, D2), BF16)]
        + weight_scratch()
        + [pltpu.VMEM((ROWS2, D2), BF16), pltpu.VMEM((2, ROWS1, D1), BF16), pltpu.VMEM((ROWS1, 1), F32), pltpu.VMEM((ROWS2, D2), BF16), pltpu.VMEM((2, ROWS2, D2), BF16), pltpu.VMEM((2, ROWS2, 1), F32), pltpu.VMEM((ROWS2, H2), BF16), pltpu.VMEM((2, ROWS2, H2), BF16), pltpu.VMEM((IMAGES, D2), F32), pltpu.VMEM((IMAGES, H2), F32), pltpu.VMEM((2, H1, D1), F32), pltpu.VMEM((2, D1, H1), F32), pltpu.VMEM((10, SUB, D1), F32), pltpu.VMEM((10, SUB, D1), F32)]
        + [dma((5,)), dma((2,)), dma((CH + 2,)), dma((CH, 10)), dma((CH, 10)), pltpu.SemaphoreType.REGULAR((CH, 3)), dma((CH,)), dma((CH,))],
        compiler_params=pltpu.CompilerParams(collective_id=0, has_side_effects=True, vmem_limit_bytes=VMEM_LIMIT),
        name="grads",
    )

    step_call = pl.pallas_call(
        step_kernel,
        out_shape=[shape((IMAGES, CLASSES), F32)] + masters * 2,
        in_specs=[hbm] * 16 + [vmem],
        out_specs=[vmem] + [hbm] * 12,
        scratch_shapes=[pltpu.VMEM((ROWS1, D1), BF16), pltpu.VMEM((ROWS2, D1), F32)]
        + [pltpu.VMEM(g.shape, BF16) for g in wide_g]
        + master_scratch() * 2
        + weight_scratch()
        + [pltpu.VMEM((ROWS2, D2), BF16), pltpu.VMEM((IMAGES, D2), F32)]
        + [dma((SUB,)), dma((SUB,)), dma((2, 4, 4)), dma((2, 4, 4)), dma((CH + 3,))],
        compiler_params=pltpu.CompilerParams(vmem_limit_bytes=VMEM_LIMIT),
        name="step",
    )

    def local_step(x_now, labels_now, x_next, up_one, down_one, merge_proj, up_two, down_two, head_proj, vel_up_one, vel_down_one, vel_merge_proj, vel_up_two, vel_down_two, vel_head_proj):
        params = (up_one, down_one, merge_proj, up_two, down_two, head_proj.T)
        vels = (vel_up_one, vel_down_one, vel_merge_proj, vel_up_two, vel_down_two, vel_head_proj.T)
        got = grads_call(x_now.reshape(ROWS1, D1), labels_now, *params)
        outs = list(step_call(x_next.reshape(ROWS1, D1), *params, *vels, *got))
        outs[6], outs[12] = outs[6].T, outs[12].T
        return tuple(outs)

    replicated = P()
    batch_split = P('data')
    in_specs = (batch_split, batch_split, batch_split) + (replicated,) * 12
    out_specs = (batch_split,) + (replicated,) * 12
    return jax.shard_map(local_step, mesh=mesh, in_specs=in_specs, out_specs=out_specs, check_vma=False)
```

```python
import jax
import jax.numpy as jnp
from jax import lax
from jax.experimental import pallas as pl
from jax.experimental.pallas import tpu as pltpu
from jax.sharding import PartitionSpec as P

MOMENTUM = 0.9
TRUST = 0.1
LN_EPS = 1e-6
GELU_C = 0.7978845608028654
GELU_K = 0.044715
MESH = pl.DeviceIdType.MESH
F32 = jnp.float32
BF16 = jnp.bfloat16
VMEM_LIMIT = 67043328

IMAGES = 16
TOKENS = 256
D1 = 128
H1 = 512
D2 = 512
H2 = 2048
ROWS1 = IMAGES * TOKENS
ROWS2 = ROWS1 // 4
CLASSES = 1000
CPAD = 1024
TILE = 256
NTILE = ROWS2 // TILE
WIDE = 512
HEAD_STEP = 192
CH = 7
LETTERS = 'abcdefgh'
NORM_ROW = dict(a=5, b=5, c=6, d=6, e=4, f=4)
LRW = 3072
LRG = 2560
NDEV = 8
MT = 64
SUB = 8
PAIR = range(2)
QUADS = range(4)
DOWNS = (2, 3)
CHUNK = 32768


def nn(a, b):
    return lax.dot_general(a, b, (((1,), (0,)), ((), ())), preferred_element_type=F32)


def nt(a, b):
    return lax.dot_general(a, b, (((1,), (1,)), ((), ())), preferred_element_type=F32)


def tn(a, b):
    return lax.dot_general(a, b, (((0,), (0,)), ((), ())), preferred_element_type=F32)


def gelu_only(x):
    inner = x * (GELU_C + (GELU_C * GELU_K) * (x * x))
    half = 0.5 + 0.5 * jnp.tanh(inner)
    return x * half


def gelu_pair(x):
    x2 = x * x
    t = jnp.tanh(x * (GELU_C + (GELU_C * GELU_K) * x2))
    half = 0.5 + 0.5 * t
    act = x * half
    slope = half + act * ((1.0 - t) * (GELU_C + (3.0 * GELU_C * GELU_K) * x2))
    return act, slope


def ln_parts(r):
    mean = jnp.mean(r, axis=-1, keepdims=True)
    cen = r - mean
    var = jnp.mean(cen * cen, axis=-1, keepdims=True)
    rstd = lax.rsqrt(var + LN_EPS)
    return cen * rstd, rstd


def ln_back(dy, xhat, rstd):
    m1 = jnp.mean(dy, axis=-1, keepdims=True)
    m2 = jnp.mean(dy * xhat, axis=-1, keepdims=True)
    return rstd * (dy - m1 - xhat * m2)


def fold_sq(v):
    rows, cols = v.shape
    s = jnp.sum((v * v).reshape(rows // SUB, SUB, cols), axis=0)
    out = s[:, 0:D1]
    for q in range(1, cols // D1):
        out = out + s[:, D1 * q:D1 * (q + 1)]
    return out


def total(acc):
    return jnp.sum(jnp.sum(acc, axis=1, keepdims=True), axis=0, keepdims=True)


def ds(start, size, mult=None):
    if isinstance(start, int):
        return pl.ds(start, size)
    return pl.ds(pl.multiple_of(start, mult or size), size)


def onehot_rows(t):
    row = lax.broadcasted_iota(jnp.int32, (IMAGES, WIDE), 0)
    col = lax.broadcasted_iota(jnp.int32, (IMAGES, WIDE), 1)
    return jnp.where(row == t * (WIDE // MT) + col // MT, 1.0, 0.0).astype(BF16)


def stage_one_tile(t, xb, xf, wuo, wdo, dst):
    xf[...] = xb[ds(t * ROWS2, ROWS2), :].astype(F32)
    r = jnp.concatenate([xf[pl.ds(j, TILE, stride=4), :] for j in QUADS], axis=0)
    for b in PAIR:
        xhat, _ = ln_parts(r)
        a = gelu_only(nn(xhat.astype(BF16), wuo[b])).astype(BF16)
        rb = (r + nn(a, wdo[b])).astype(BF16)
        r = rb.astype(F32)
    for j in QUADS:
        dst[ds(t * TILE, TILE), D1 * j:D1 * (j + 1)] = rb[TILE * j:TILE * (j + 1), :]


def update(w, v, g, scale):
    nv = MOMENTUM * v + scale * g.astype(F32)
    nw = w - nv
    return nw, nv


def chunk_of(num, ref):
    if num < CH - 1:
        return ref.at[num]
    half = ref.shape[1] // 2
    return ref.at[CH - 1, pl.ds((num - CH + 1) * half, half)]


class Ring:
    def __init__(self, num, stacks, ssem, rsem, csem, pos):
        self.num = num
        self.g, self.r1, self.r2, self.r3 = (chunk_of(num, ref) for ref in stacks)
        g = self.g
        self.ssem, self.rsem, self.csem = ssem, rsem, csem
        self.pos = pos
        self.rb = g.shape[0] // NDEV
        c, f, s = pos['c'], pos['f'], pos['s']
        self.f, self.s, self.nf, self.ns = f, s, 1 - f, 1 - s
        self.mine, self.other = 4 * c, 4 - 4 * c
        self.keep = self.mine + 2 * f
        self.give = self.mine + 2 * self.nf
        self.own_b, self.s_b = self.keep + s, self.keep + self.ns
        self.f_b, self.d_b = self.give + s, self.give + self.ns

    def blk(self, b, n=1):
        return self.g.at[ds(b * self.rb, n * self.rb, self.rb)]

    def rc(self, k, src, dst, dev):
        return pltpu.make_async_remote_copy(src_ref=src, dst_ref=dst, send_sem=self.ssem.at[self.num, k], recv_sem=self.rsem.at[self.num, k], device_id=(self.pos[dev],), device_id_type=MESH)

    def add(self, b, recv, i, n):
        rows, width = n * self.rb, self.g.shape[1]
        step = min(rows, CHUNK // width)
        b0, i0 = b * self.rb, i * self.rb

        def body(j, carry):
            dst = ds(b0 + j * step, step)
            src = ds(i0 + j * step, step)
            self.g[dst, :] = (self.g[dst, :].astype(F32) + recv[src, :].astype(F32)).astype(BF16)
            return carry

        lax.fori_loop(0, rows // step, body, 0)

    def to_core(self):
        return self.rc(0, self.blk(self.other, 4), self.r1, 'core')

    def to_f(self):
        return self.rc(1, self.blk(self.give, 2), self.r2, 'fn')

    def to_s(self):
        return self.rc(2, self.blk(self.s_b), self.r3, 'sn')

    def back(self, k, b, dev):
        return self.rc(k, self.blk(b), self.blk(b), dev)

    def own_to_s(self):
        return self.back(3, self.own_b, 'sn')

    def own_to_f(self):
        return self.back(4, self.own_b, 'fn')

    def own_to_core(self):
        return self.back(5, self.own_b, 'core')

    def s_to_f(self):
        return self.back(6, self.s_b, 'fn')

    def s_to_core(self):
        return self.back(7, self.s_b, 'core')

    def f_to_core(self):
        return self.back(8, self.f_b, 'core')

    def d_to_core(self):
        return self.back(9, self.d_b, 'core')

    def half(self):
        self.to_core().start()

    def link_f(self):
        self.to_core().wait_recv()
        self.add(self.give, self.r1, 2 * self.nf, 2)
        self.to_f().start()
        self.add(self.keep, self.r1, 2 * self.f, 2)

    def link_s(self):
        self.to_f().wait_recv()
        self.add(self.s_b, self.r2, self.ns, 1)
        self.to_s().start()
        self.add(self.own_b, self.r2, self.s, 1)
        self.to_core().wait_send()
        self.free(0, 'core')
        self.to_f().wait_send()
        self.free(1, 'fn')

    def own(self):
        self.to_s().wait_recv()
        self.to_s().wait_send()
        self.free(2, 'sn')
        self.add(self.own_b, self.r3, 0, 1)
        self.held(1)
        self.own_to_f().start()
        self.held(0)
        self.own_to_core().start()

    def own_s(self):
        self.held(2)
        self.own_to_s().start()

    def pass_s(self):
        self.own_to_s().wait_recv()
        self.s_to_f().start()
        self.s_to_core().start()

    def pass_f(self):
        self.own_to_f().wait_recv()
        self.f_to_core().start()

    def pass_d(self):
        self.s_to_f().wait_recv()
        self.d_to_core().start()

    def done(self):
        for cp in (self.own_to_core(), self.s_to_core(), self.f_to_core(), self.d_to_core()):
            cp.wait()
        for cp in (self.own_to_s(), self.own_to_f(), self.s_to_f()):
            cp.wait_send()

    def free(self, i, who):
        pl.semaphore_signal(self.csem.at[self.num, i], inc=1, device_id=(self.pos[who],), device_id_type=MESH)

    def held(self, i):
        pl.semaphore_wait(self.csem.at[self.num, i], 1)


class Share:
    def __init__(self, buf, ssem, rsem, pos):
        self.buf, self.ssem, self.rsem, self.pos = buf, ssem, rsem, pos

    def rc(self, k):
        p = self.pos
        own, fblk, sblk, dblk = p['me'], p['fn'], p['sn'], p['diag']
        b, dev = {0: (own, 'fn'), 1: (own, 'sn'), 2: (own, 'core'), 3: (fblk, 'sn'), 4: (fblk, 'core'), 5: (sblk, 'core'), 6: (dblk, 'core')}[k]
        return pltpu.make_async_remote_copy(src_ref=self.buf.at[b], dst_ref=self.buf.at[b], send_sem=self.ssem.at[k], recv_sem=self.rsem.at[k], device_id=(p[dev],), device_id_type=MESH)


    def send(self):
        for k in (0, 1, 2):
            self.rc(k).start()

    def relay(self):
        self.rc(0).wait_recv()
        self.rc(3).start()
        self.rc(4).start()
        self.rc(1).wait_recv()
        self.rc(5).start()

    def done(self):
        self.rc(3).wait_recv()
        self.rc(6).start()
        for k in (2, 4, 5, 6):
            self.rc(k).wait_recv()
        for k in range(7):
            self.rc(k).wait_send()


def position():
    me = lax.axis_index('data')
    c = lax.rem(me, 2)
    x = lax.rem(me // 2, 2)
    y = me // 4
    f = c * y + (1 - c) * x
    s = c * x + (1 - c) * y
    xn = me + 2 - 4 * x
    yn = me + 4 - SUB * y
    fn = c * yn + (1 - c) * xn
    sn = c * xn + (1 - c) * yn
    diag = xn + yn - me
    core = me + 1 - 2 * c
    return dict(me=me, c=c, f=f, s=s, fn=fn, sn=sn, diag=diag, core=core)


STEPS = ('half', 'link_f', 'link_s', 'own', 'own_s', 'pass_s', 'pass_f', 'pass_d', 'done')
SHARE_STEPS = ('send', 'relay', 'done')
PLAN = dict(
    up1=((), ('a0',), (), ('b0',),),
    in1=((), ('a1',), ('s1', 'b1',), (),),
    dn0=((), ('c0',), (), ('d0',),),
    pre0=((), ('c1', 'a2',), ('s2', 'd1',), (),),
    up0=((), ('b2', 'e0',), (), ('f0',),),
    in0=(('a3', 'e1',), ('a4', 'c2', 'f1',), ('b3',), (),),
    mrg=(('b4', 'h0',),),
    back=(('a5', 'a6', 'd2', 'h1',), ('b5', 'c3',), ('c4', 'd3', 'e2', 'f2',), ('a7', 'b6', 'd4', 'g0',),),
    rank=(('c5', 'h2',), ('a8', 'g1',), ('b7', 'e3',), ('e4',),),
    rankh=(('b8', 'c6', 'f3',), (), ('f4',), ('d5',),),
    tail=('d6', 'h3', 'h4', 'c7', 'e5', 'c8', 'g2', 'f5', 'h5', 'e6', 'g3', 'f6', 'g4', 'd7', 'h6', 'd8', 'e7', 'g5', 'f7', 'e8', 'h7', 'g6', 'f8', 'g7', 'h8', 'g8', ),
)


def grad_kernel(x_hbm, lab, uo_hbm, do_hbm, m_hbm, ut_hbm, dt_hbm, h_hbm,
                g_out, gv1_out, gh_out, scal,
                g_all, r1_all, r2_all, r3_all, lr, gdup,
                wuo, wdo, wm, wut, wdt, wh,
                merged, n1, rst1, r2, n2, rst2, a2, sl2, pooled, asum, accv, accu, sq, gsq,
                in_sem, st_sem, out_sem, ssem, rsem, csem, lssem, lrsem):
    pos = position()
    barrier = pltpu.get_barrier_semaphore()
    for who in ('core', 'fn', 'sn'):
        pl.semaphore_signal(barrier, inc=1, device_id=(pos[who],), device_id_type=MESH)

    gv1, gh, grad = wdt.at[1], wh, r2

    share = Share(lr, lssem, lrsem, pos)
    rings = {letter: Ring(i, (g_all, r1_all, r2_all, r3_all), ssem, rsem, csem, pos) for i, letter in enumerate(LETTERS)}
    outs = {letter: pltpu.make_async_copy(chunk_of(i, g_all), chunk_of(i, g_out), out_sem.at[i]) for i, letter in enumerate(LETTERS)}

    def norm_of(letter):
        ref = g_all.at[LETTERS.index(letter)]

        def body(i, acc):
            return acc + fold_sq(ref[ds(i * MT, MT), :].astype(F32))

        gsq[NORM_ROW[letter]] += lax.fori_loop(0, ROWS2 // MT, body, jnp.zeros((SUB, D1), F32))

    def act(word):
        letter, num = word[0], int(word[1])
        if letter == 's':
            getattr(share, SHARE_STEPS[num])()
        else:
            getattr(rings[letter], STEPS[num])()
            if STEPS[num] == 'done':
                outs[letter].start()
                if letter in NORM_ROW:
                    norm_of(letter)

    def run(name, body):
        plan = PLAN[name]

        def wrapped(t, carry):
            body(t)
            for i, words in enumerate(plan):
                if words:
                    @pl.when(t == i)
                    def _():
                        for word in words:
                            act(word)
            return carry

        lax.fori_loop(0, len(plan), wrapped, 0)

    def forward(xb, xf, suo, sdo, sm, sut, sdt, abuf):
        loads = [pltpu.make_async_copy(src, dst, in_sem.at[i]) for i, (src, dst) in enumerate(((x_hbm, xb), (uo_hbm, suo), (do_hbm, sdo), (m_hbm, sm), (h_hbm, sdt.at[0:CLASSES])))]

        def stage_up(i):
            return pltpu.make_async_copy(ut_hbm.at[i // 2, ds((i % 2) * TILE, TILE)], sut, st_sem.at[0])

        def stage_down(i):
            return pltpu.make_async_copy(dt_hbm.at[i // 2, ds((i % 2) * ROWS2, ROWS2)], sdt, st_sem.at[1])

        for cp in loads[:3]:
            cp.start()
        stage_up(0).start()
        stage_down(0).start()
        loads[3].start()
        sq[...] = jnp.zeros_like(sq)
        for cp in loads[:3]:
            cp.wait()
        for b in PAIR:
            v = suo[b]
            sq[b] = fold_sq(v)
            wuo[b] = v.astype(BF16)
            v = sdo[b]
            sq[2 + b] = fold_sq(v)
            wdo[b] = v.astype(BF16)

        def stage_one(t, carry):
            xf[...] = xb[ds(t * ROWS2, ROWS2), :].astype(F32)
            r = jnp.concatenate([xf[pl.ds(j, TILE, stride=4), :] for j in QUADS], axis=0)
            rows = ds(t * ROWS2, ROWS2)
            for b in PAIR:
                xhat, rstd = ln_parts(r)
                n = xhat.astype(BF16)
                n1[b, rows, :] = n
                if b == 1:
                    rst1[rows, :] = rstd
                a = gelu_only(nn(n, wuo[b])).astype(BF16)
                rb = (r + nn(a, wdo[b])).astype(BF16)
                r = rb.astype(F32)
            for j in QUADS:
                merged[ds(t * TILE, TILE), D1 * j:D1 * (j + 1)] = rb[TILE * j:TILE * (j + 1), :]
            layer = t // 2
            stage_up(t).wait()

            def cast_up(i, acc):
                v = sut[ds(i * 32, 32), :]
                wut[layer, ds((t % 2) * TILE + i * 32, 32), :] = v.astype(BF16)
                return acc + fold_sq(v)

            sq[4 + layer] += lax.fori_loop(0, SUB, cast_up, jnp.zeros((SUB, D1), F32))
            stage_down(t).wait()

            def cast_down(i, acc):
                v = sdt[ds(i * D1, D1), :]
                wdt[layer, ds((t % 2) * ROWS2 + i * D1, D1), :] = v.astype(BF16)
                return acc + fold_sq(v)

            sq[6 + layer] += lax.fori_loop(0, SUB, cast_down, jnp.zeros((SUB, D1), F32))

            @pl.when(t < 3)
            def _():
                stage_up(t + 1).start()
                stage_down(t + 1).start()

            return carry

        lax.fori_loop(0, NTILE, stage_one, 0)

        loads[4].start()
        loads[3].wait()

        def cast_m(i, acc):
            v = sm[ds(i * MT, MT), :]
            wm[ds(i * MT, MT), :] = v.astype(BF16)
            return acc + fold_sq(v)

        sq[SUB] = lax.fori_loop(0, SUB, cast_m, jnp.zeros((SUB, D1), F32))

        def merge_tile(t, carry):
            rows = ds(t * WIDE, WIDE)
            r2[rows, :] = nn(merged[rows, :], wm[...]).astype(BF16)
            return carry

        lax.fori_loop(0, ROWS2 // WIDE, merge_tile, 0)
        asum[...] = jnp.zeros_like(asum)
        pooled[...] = jnp.zeros_like(pooled)

        for layer in PAIR:
            def stage_two(t, carry):
                rows = ds(t * WIDE, WIDE)
                r = r2[rows, :].astype(F32)
                xhat, rstd = ln_parts(r)
                n = xhat.astype(BF16)
                n2[layer, rows, :] = n
                rst2[layer, rows, :] = rstd
                for q in QUADS:
                    cols = slice(D2 * q, D2 * (q + 1))
                    acts, slope = gelu_pair(nn(n, wut[layer, :, cols]))
                    if layer == 0:
                        a2[rows, cols] = acts.astype(BF16)
                    else:
                        abuf[:, cols] = acts.astype(BF16)
                    sl2[layer, rows, cols] = slope.astype(BF16)
                if layer == 0:
                    r2[rows, :] = (r + nn(a2[rows, :], wdt[layer])).astype(BF16)
                else:
                    rb = (r + nn(abuf[...], wdt[layer])).astype(BF16)
                    pick = onehot_rows(t)
                    asum[...] += nn(pick, abuf[...])
                    pooled[...] += nn(pick, rb)
                return carry

            lax.fori_loop(0, ROWS2 // WIDE, stage_two, 0)
        wh[CLASSES:, :] = jnp.zeros((CPAD - CLASSES, D2), BF16)
        loads[4].wait()
        for k in QUADS:
            rows = slice(TILE * k, min(TILE * (k + 1), CLASSES))
            v = sdt[rows, :]
            wh[rows, :] = v.astype(BF16)
            sq[9] += fold_sq(v)

    pl.run_scoped(
        forward,
        pltpu.VMEM((ROWS1, D1), BF16),
        pltpu.VMEM((ROWS2, D1), F32),
        pltpu.VMEM((2, D1, H1), F32),
        pltpu.VMEM((2, H1, D1), F32),
        pltpu.VMEM((D2, D2), F32),
        pltpu.VMEM((TILE, H2), F32),
        pltpu.VMEM((ROWS2, D2), F32),
        pltpu.VMEM((WIDE, H2), BF16),
    )

    xhat, rstd = ln_parts(pooled[...] * (1.0 / MT))
    hb = xhat.astype(BF16)
    logits = nt(hb, wh[...])
    col = lax.broadcasted_iota(jnp.int32, (IMAGES, CPAD), 1)
    row = lax.broadcasted_iota(jnp.int32, (IMAGES, CPAD), 0)
    logits = jnp.where(col < CLASSES, logits, -jnp.inf)
    ex = jnp.exp(logits - jnp.max(logits, axis=-1, keepdims=True))
    prob = ex / jnp.sum(ex, axis=-1, keepdims=True)
    lab_row = jnp.zeros((IMAGES, CPAD), jnp.int32)
    for i in range(IMAGES):
        lab_row = jnp.where(row == i, lab[i], lab_row)
    gl = ((prob - jnp.where(col == lab_row, 1.0, 0.0)) * (1.0 / (IMAGES * NDEV))).astype(BF16)
    g16 = (ln_back(nn(gl, wh[...]), xhat, rstd) * (1.0 / MT)).astype(BF16)
    hi = asum[...].astype(BF16)
    lo = (asum[...] - hi.astype(F32)).astype(BF16)
    me = pos['me']
    lr[me, 0:IMAGES, 0:H2] = hi
    lr[me, IMAGES:32, 0:H2] = lo
    lr[me, 0:IMAGES, H2:LRG] = g16
    lr[me, IMAGES:32, H2:LRG] = hb
    lr[me, 0:IMAGES, LRG:LRW] = gl[:, 0:D2]
    lr[me, IMAGES:32, LRG:LRW] = gl[:, D2:CPAD]
    pl.semaphore_wait(barrier, 3)
    share.send()

    asum[...] = nt(g16, wdt[1])
    pooled[...] = g16.astype(F32)

    def slope_one(i, carry):
        rows = ds(i * MT, MT)
        grad[rows, :] = jnp.broadcast_to(pooled[pl.ds(i, 1), :], (MT, D2)).astype(BF16)
        for q in QUADS:
            cols = slice(D2 * q, D2 * (q + 1))
            sl2[1, rows, cols] = (asum[pl.ds(i, 1), cols] * sl2[1, rows, cols].astype(F32)).astype(BF16)
        return carry

    lax.fori_loop(0, IMAGES, slope_one, 0)

    def up_grad(layer, first):
        def body(q):
            g_all[first + q // 2, ds((q % 2) * D2, D2), :] = tn(n2[layer], sl2[layer, :, ds(q * D2, D2)]).astype(BF16)

        return body

    def down_grad(q):
        g_all[2 + q // 2, ds((q % 2) * D2, D2), :] = tn(a2[:, ds(q * D2, D2)], grad[...]).astype(BF16)

    def input_grad(layer):
        def body(t):
            rows = ds(t * TILE, TILE)
            dy = nt(sl2[layer, rows, :], wut[layer])
            dx = ln_back(dy, n2[layer, rows, :].astype(F32), rst2[layer, rows, :])
            grad[rows, :] = (dx + grad[rows, :].astype(F32)).astype(BF16)

        return body

    def pre_grad(t):
        rows = ds(t * TILE, TILE)
        for q in QUADS:
            cols = slice(D2 * q, D2 * (q + 1))
            ga = nt(grad[rows, :], wdt[0, cols, :])
            sl2[0, rows, cols] = (ga * sl2[0, rows, cols].astype(F32)).astype(BF16)

    gsm = g_all.at[CH - 1]

    def merge_grad(t):
        gsm[D2:ROWS2, :] = tn(merged[...], grad[...]).astype(BF16)

    def stage_one_back(t):
        gm = nt(grad[ds(t * TILE, TILE), :], wm[...]).astype(BF16)
        rows = ds(t * ROWS2, ROWS2)
        g = jnp.concatenate([gm[:, D1 * j:D1 * (j + 1)] for j in QUADS], axis=0)
        for b in (1, 0):
            n = n1[b, rows, :]
            acts, slope = gelu_pair(nn(n, wuo[b]))
            accv[b] += tn(acts.astype(BF16), g)
            gp = (nt(g, wdo[b]) * slope).astype(BF16)
            accu[b] += tn(n, gp)
            if b == 1:
                dx = ln_back(nt(gp, wuo[b]), n.astype(F32), rst1[rows, :])
                g = (dx + g.astype(F32)).astype(BF16)

        @pl.when(t == 3)
        def _():
            for b in PAIR:
                gsm[D1 * b:D1 * (b + 1), :] = accu[b].astype(BF16)
                for q in PAIR:
                    gsm[TILE:D2, TILE * b + D1 * q:TILE * b + D1 * (q + 1)] = accv[b, TILE * q:TILE * (q + 1), :].astype(BF16)

    run('up1', up_grad(1, 0))
    run('in1', input_grad(1))
    run('dn0', down_grad)
    run('pre0', pre_grad)
    run('up0', up_grad(0, 4))
    run('in0', input_grad(0))
    accv[...] = jnp.zeros_like(accv)
    accu[...] = jnp.zeros_like(accu)
    gsq[...] = jnp.zeros_like(gsq)
    run('mrg', merge_grad)
    run('back', stage_one_back)

    def v1_rows(i):
        cols = ds(i * D2, D2)
        out = jnp.zeros((D2, D2), F32)
        for d in range(NDEV):
            out = out + tn(lr[d, :, cols], gdup[d]).astype(BF16).astype(F32)
        ob = out.astype(BF16)
        gv1[cols, :] = ob
        gsq[7] += fold_sq(ob.astype(F32))

    def head_rows(i):
        rows = ds(i * TILE, TILE)
        out = jnp.zeros((TILE, D2), F32)
        for d in range(NDEV):
            gl_d = lr[d, ds((i // 2) * IMAGES, IMAGES), ds(LRG + (i % 2) * TILE, TILE)]
            out = out + tn(gl_d, lr[d, IMAGES:32, H2:LRG]).astype(BF16).astype(F32)
        ob = out.astype(BF16)
        gh[rows, :] = ob
        gsq[9] += fold_sq(ob.astype(F32))

    gv1_cp = pltpu.make_async_copy(gv1, gv1_out, out_sem.at[CH + 1])
    gh_cp = pltpu.make_async_copy(gh, gh_out, out_sem.at[CH + 2])
    for d in range(NDEV):
        gdup[d, 0:IMAGES, :] = lr[d, 0:IMAGES, H2:LRG]
        gdup[d, IMAGES:32, :] = lr[d, 0:IMAGES, H2:LRG]
    run('rank', v1_rows)
    gv1_cp.start()
    run('rankh', head_rows)
    gh_cp.start()
    for word in PLAN['tail']:
        act(word)
    for b in PAIR:
        gsq[b] = fold_sq(gsm[D1 * b:D1 * (b + 1), :].astype(F32))
        gsq[2 + b] = fold_sq(gsm[TILE:D2, TILE * b:TILE * (b + 1)].astype(F32))
    gsq[SUB] = fold_sq(gsm[D2:ROWS2, :].astype(F32))
    for i in range(10):
        ratio = jnp.sqrt(total(sq[i])) / jnp.sqrt(total(gsq[i]))
        scal[i:i + 1, :] = jnp.broadcast_to(TRUST * ratio, (1, D1))
    scal[10:IMAGES, :] = jnp.zeros((6, D1), F32)
    for letter in LETTERS:
        outs[letter].wait()
    gv1_cp.wait()
    gh_cp.wait()


def step_kernel(x_hbm, uo_hbm, do_hbm, m_hbm, ut_hbm, dt_hbm, h_hbm, vuo_hbm, vdo_hbm, vm_hbm, vut_hbm, vdt_hbm, vh_hbm,
                g_hbm, gv1_hbm, gh_hbm, scal,
                logits_out, uo_out, do_out, m_out, ut_out, dt_out, h_out, vuo_out, vdo_out, vm_out, vut_out, vdt_out, vh_out,
                xb, xf, g_all, gv1, gh, suo, sdo, sm, sh, sut, sdt, tuo, tdo, tm, th, tut, tdt,
                wuo, wdo, wm, wut, wdt, wh, r2, pooled,
                s_in, s_out, q_in, q_out, g_sem):
    small = [(uo_hbm, suo, uo_out), (vuo_hbm, tuo, vuo_out), (do_hbm, sdo, do_out), (vdo_hbm, tdo, vdo_out), (m_hbm, sm, m_out), (vm_hbm, tm, vm_out), (h_hbm, sh, h_out), (vh_hbm, th, vh_out)]
    ins = [pltpu.make_async_copy(src, buf, s_in.at[i]) for i, (src, buf, _) in enumerate(small)]
    louts = [pltpu.make_async_copy(buf, dst, s_out.at[i]) for i, (_, buf, dst) in enumerate(small)]
    up_big = [(ut_hbm, sut, ut_out), (vut_hbm, tut, vut_out)]
    down_big = [(dt_hbm, sdt, dt_out), (vdt_hbm, tdt, vdt_out)]
    gsm = g_all.at[CH - 1]

    def copies(layer, t, into, which=QUADS):
        out = []
        for k in which:
            src, buf, dst = (up_big + down_big)[k]
            n = D1 if k in PAIR else D2
            rows = ds(t * n, n)
            here = buf.at[rows] if k in PAIR else buf.at[layer, rows]
            if into:
                out.append(pltpu.make_async_copy(src.at[layer, rows], here, q_in.at[layer, k, t]))
            else:
                out.append(pltpu.make_async_copy(here, dst.at[layer, rows], q_out.at[layer, k, t]))
        return out

    def start(cps):
        for cp in cps:
            cp.start()

    def wait(cps):
        for cp in cps:
            cp.wait()

    x_cp = pltpu.make_async_copy(x_hbm, xb, g_sem.at[CH])
    g_cps = [pltpu.make_async_copy(g_hbm.at[i], g_all.at[i], g_sem.at[i]) for i in range(CH)]
    gv1_cp = pltpu.make_async_copy(gv1_hbm, gv1, g_sem.at[CH + 1])
    gh_cp = pltpu.make_async_copy(gh_hbm, gh, g_sem.at[CH + 2])

    def up_part(layer, t):
        scale = scal[4 + layer:5 + layer, 0:1]
        rows = ds(t * D1, D1)
        for q in QUADS:
            cols = slice(D2 * q, D2 * (q + 1))
            g = g_all[4 - 4 * layer + q // 2, ds((q % 2) * D2 + t * D1, D1), :]
            nw, nv = update(sut[rows, cols], tut[rows, cols], g, scale)
            sut[rows, cols] = nw
            tut[rows, cols] = nv
            wut[layer, rows, cols] = nw.astype(BF16)

    def down_part(layer, t):
        rows = ds(t * D2, D2)
        g = g_all[2 + t // 2, ds((t % 2) * D2, D2), :] if layer == 0 else gv1[rows, :]
        nw, nv = update(sdt[layer, rows, :], tdt[layer, rows, :], g, scal[6 + layer:7 + layer, 0:1])
        sdt[layer, rows, :] = nw
        tdt[layer, rows, :] = nv
        wdt[layer, rows, :] = nw.astype(BF16)

    def stage_two(layer, r):
        xhat, _ = ln_parts(r)
        n = xhat.astype(BF16)
        acc = r
        for q in QUADS:
            cols = slice(D2 * q, D2 * (q + 1))
            a = gelu_only(nn(n, wut[layer, :, cols])).astype(BF16)
            acc = acc + nn(a, wdt[layer, cols, :])
        return acc.astype(BF16)

    first_in = [x_cp, g_cps[CH - 1]] + ins[:4]
    early = [g_cps[i] for i in (4, 5, 2)]
    later = [g_cps[0], g_cps[1], gv1_cp]
    start(first_in)
    start(early)
    start(copies(0, 0, True))
    wait(first_in)
    for b in PAIR:
        nw, tuo[b] = update(suo[b], tuo[b], gsm[D1 * b:D1 * (b + 1), :], scal[b:b + 1, 0:1])
        suo[b] = nw
        wuo[b] = nw.astype(BF16)
        for q in PAIR:
            rows = slice(TILE * q, TILE * (q + 1))
            nw, tdo[b, rows, :] = update(sdo[b, rows, :], tdo[b, rows, :], gsm[TILE:D2, TILE * b + D1 * q:TILE * b + D1 * (q + 1)], scal[2 + b:3 + b, 0:1])
            sdo[b, rows, :] = nw
            wdo[b, rows, :] = nw.astype(BF16)
    wait(early)

    def stage_one_update(t, carry):
        wait(copies(0, t, True))

        @pl.when(t < 3)
        def _():
            start(copies(0, t + 1, True))

        @pl.when(t == 0)
        def _():
            start([g_cps[3]])

        @pl.when(t == 1)
        def _():
            start(ins[4:6])

        @pl.when(t == 2)
        def _():
            wait([g_cps[3]])
            start(later)

        @pl.when(t == 3)
        def _():
            start(copies(1, 0, True, DOWNS))
            start(copies(1, 1, True, DOWNS))
            start([gh_cp] + ins[6:])

        stage_one_tile(t, xb, xf, wuo, wdo, r2)
        up_part(0, t)
        down_part(0, t)
        start(copies(0, t, False, PAIR))
        return carry

    lax.fori_loop(0, NTILE, stage_one_update, 0)
    start(copies(1, 2, True, DOWNS))
    start(copies(1, 3, True, DOWNS))
    wait(ins[4:6])
    nw, tm[...] = update(sm[...], tm[...], gsm[D2:ROWS2, :], scal[SUB:9, 0:1])
    sm[...] = nw
    wm[...] = nw.astype(BF16)

    def merge_tile(t, carry):
        rows = ds(t * WIDE, WIDE)
        r2[rows, :] = nn(r2[rows, :], wm[...]).astype(BF16)
        return carry

    lax.fori_loop(0, ROWS2 // WIDE, merge_tile, 0)
    wait(later)
    pooled[...] = jnp.zeros_like(pooled)

    def first(t, carry):
        rows = ds(t * WIDE, WIDE)
        for i in PAIR:
            wait(copies(0, 2 * t + i, False, PAIR))
            start(copies(1, 2 * t + i, True, PAIR))
        for i in PAIR:
            wait(copies(1, 2 * t + i, True, DOWNS))
            start(copies(0, 2 * t + i, False, DOWNS))
        r2[rows, :] = stage_two(0, r2[rows, :].astype(F32))
        for i in PAIR:
            down_part(1, 2 * t + i)
        return carry

    lax.fori_loop(0, ROWS2 // WIDE, first, 0)
    def second_up(t, carry):
        wait(copies(1, t, True, PAIR))
        up_part(1, t)
        start(copies(1, t, False))
        return carry

    lax.fori_loop(0, NTILE, second_up, 0)
    start(louts[:6])
    wh[CLASSES:, :] = jnp.zeros((CPAD - CLASSES, D2), BF16)
    wait(ins[6:] + [gh_cp])

    def head_update(rows):
        nw, th[rows, :] = update(sh[rows, :], th[rows, :], gh[rows, :], scal[9:10, 0:1])
        sh[rows, :] = nw
        wh[rows, :] = nw.astype(BF16)

    def head_part(i, carry):
        head_update(ds(i * HEAD_STEP, HEAD_STEP))
        return carry

    lax.fori_loop(0, CLASSES // HEAD_STEP, head_part, 0)
    head_update(slice(CLASSES - CLASSES % HEAD_STEP, CLASSES))
    start(louts[6:])

    def second(t, carry):
        rows = ds(t * WIDE, WIDE)
        rb = stage_two(1, r2[rows, :].astype(F32))
        pooled[...] += nn(onehot_rows(t), rb)
        return carry

    lax.fori_loop(0, ROWS2 // WIDE, second, 0)
    xhat, _ = ln_parts(pooled[...] * (1.0 / MT))
    logits = nt(xhat.astype(BF16), wh[...])
    logits_out[...] = logits[:, 0:CLASSES]
    wait(louts)
    for t in QUADS:
        wait(copies(0, t, False, DOWNS))
        wait(copies(1, t, False))


def weight_scratch():
    return [pltpu.VMEM((2, D1, H1), BF16), pltpu.VMEM((2, H1, D1), BF16), pltpu.VMEM((D2, D2), BF16), pltpu.VMEM((2, D2, H2), BF16), pltpu.VMEM((2, H2, D2), BF16), pltpu.VMEM((CPAD, D2), BF16)]


def master_scratch():
    return [pltpu.VMEM((2, D1, H1), F32), pltpu.VMEM((2, H1, D1), F32), pltpu.VMEM((D2, D2), F32), pltpu.VMEM((CLASSES, D2), F32), pltpu.VMEM((D2, H2), F32), pltpu.VMEM((2, H2, D2), F32)]


def solution(mesh):
    hbm = pl.BlockSpec(memory_space=pl.ANY)
    vmem = pl.BlockSpec(memory_space=pltpu.VMEM)
    smem = pl.BlockSpec(memory_space=pltpu.SMEM)
    shape = jax.ShapeDtypeStruct
    dma = pltpu.SemaphoreType.DMA
    wide_g = [shape((CH, ROWS2, D2), BF16), shape((H2, D2), BF16), shape((CPAD, D2), BF16)]
    masters = [shape((2, D1, H1), F32), shape((2, H1, D1), F32), shape((D2, D2), F32), shape((2, D2, H2), F32), shape((2, H2, D2), F32), shape((CLASSES, D2), F32)]

    grads_call = pl.pallas_call(
        grad_kernel,
        out_shape=wide_g + [shape((IMAGES, D1), F32)],
        in_specs=[hbm, smem] + [hbm] * 6,
        out_specs=[hbm] * 3 + [vmem],
        scratch_shapes=[pltpu.VMEM((CH, ROWS2 // k, D2), BF16) for k in (1, 2, 4, NDEV)]
        + [pltpu.VMEM((NDEV, 32, LRW), BF16), pltpu.VMEM((NDEV, 32, D2), BF16)]
        + weight_scratch()
        + [pltpu.VMEM((ROWS2, D2), BF16), pltpu.VMEM((2, ROWS1, D1), BF16), pltpu.VMEM((ROWS1, 1), F32), pltpu.VMEM((ROWS2, D2), BF16), pltpu.VMEM((2, ROWS2, D2), BF16), pltpu.VMEM((2, ROWS2, 1), F32), pltpu.VMEM((ROWS2, H2), BF16), pltpu.VMEM((2, ROWS2, H2), BF16), pltpu.VMEM((IMAGES, D2), F32), pltpu.VMEM((IMAGES, H2), F32), pltpu.VMEM((2, H1, D1), F32), pltpu.VMEM((2, D1, H1), F32), pltpu.VMEM((10, SUB, D1), F32), pltpu.VMEM((10, SUB, D1), F32)]
        + [dma((5,)), dma((2,)), dma((CH + 3,)), dma((CH + 1, 10)), dma((CH + 1, 10)), pltpu.SemaphoreType.REGULAR((CH + 1, 3)), dma((CH,)), dma((CH,))],
        compiler_params=pltpu.CompilerParams(collective_id=0, has_side_effects=True, vmem_limit_bytes=VMEM_LIMIT),
        name="grads",
    )

    step_call = pl.pallas_call(
        step_kernel,
        out_shape=[shape((IMAGES, CLASSES), F32)] + masters * 2,
        in_specs=[hbm] * 16 + [vmem],
        out_specs=[vmem] + [hbm] * 12,
        scratch_shapes=[pltpu.VMEM((ROWS1, D1), BF16), pltpu.VMEM((ROWS2, D1), F32)]
        + [pltpu.VMEM(g.shape, BF16) for g in wide_g]
        + master_scratch() * 2
        + weight_scratch()
        + [pltpu.VMEM((ROWS2, D2), BF16), pltpu.VMEM((IMAGES, D2), F32)]
        + [dma((SUB,)), dma((SUB,)), dma((2, 4, 4)), dma((2, 4, 4)), dma((CH + 3,))],
        compiler_params=pltpu.CompilerParams(vmem_limit_bytes=VMEM_LIMIT),
        name="step",
    )

    def local_step(x_now, labels_now, x_next, up_one, down_one, merge_proj, up_two, down_two, head_proj, vel_up_one, vel_down_one, vel_merge_proj, vel_up_two, vel_down_two, vel_head_proj):
        params = (up_one, down_one, merge_proj, up_two, down_two, head_proj.T)
        vels = (vel_up_one, vel_down_one, vel_merge_proj, vel_up_two, vel_down_two, vel_head_proj.T)
        got = grads_call(x_now.reshape(ROWS1, D1), labels_now, *params)
        outs = list(step_call(x_next.reshape(ROWS1, D1), *params, *vels, *got))
        outs[6], outs[12] = outs[6].T, outs[12].T
        return tuple(outs)

    replicated = P()
    batch_split = P('data')
    in_specs = (batch_split, batch_split, batch_split) + (replicated,) * 12
    out_specs = (batch_split,) + (replicated,) * 12
    return jax.shard_map(local_step, mesh=mesh, in_specs=in_specs, out_specs=out_specs, check_vma=False)
```

```python
import jax
import jax.numpy as jnp
from jax import lax
from jax.experimental import pallas as pl
from jax.experimental.pallas import tpu as pltpu
from jax.sharding import PartitionSpec as P

MOMENTUM = 0.9
TRUST = 0.1
LN_EPS = 1e-6
GELU_C = 0.7978845608028654
GELU_K = 0.044715
MESH = pl.DeviceIdType.MESH
F32 = jnp.float32
BF16 = jnp.bfloat16
SCOPED_LIMIT = 59600000

IMAGES = 16
TOKENS = 256
D1 = 128
H1 = 512
D2 = 512
H2 = 2048
ROWS1 = IMAGES * TOKENS
ROWS2 = ROWS1 // 4
CLASSES = 1000
CPAD = 1024
TILE = 256
NTILE = ROWS2 // TILE
WIDE = 512
HEAD_STEP = 192
CH = 7
LETTERS = 'abcdefgh'
NORM_ROW = dict(a=5, b=5, c=6, d=6, e=4, f=4)
LRW = 3072
LRG = 2560
NDEV = 8
MT = 64
SUB = 8
PAIR = range(2)
QUADS = range(4)
DOWNS = (2, 3)
CHUNK = 32768


def nn(a, b):
    return lax.dot_general(a, b, (((1,), (0,)), ((), ())), preferred_element_type=F32)


def nt(a, b):
    return lax.dot_general(a, b, (((1,), (1,)), ((), ())), preferred_element_type=F32)


def tn(a, b):
    return lax.dot_general(a, b, (((0,), (0,)), ((), ())), preferred_element_type=F32)


def gelu_only(x):
    inner = x * (GELU_C + (GELU_C * GELU_K) * (x * x))
    half = 0.5 + 0.5 * jnp.tanh(inner)
    return x * half


def gelu_pair(x):
    x2 = x * x
    t = jnp.tanh(x * (GELU_C + (GELU_C * GELU_K) * x2))
    half = 0.5 + 0.5 * t
    act = x * half
    slope = half + act * ((1.0 - t) * (GELU_C + (3.0 * GELU_C * GELU_K) * x2))
    return act, slope


def ln_parts(r):
    mean = jnp.mean(r, axis=-1, keepdims=True)
    cen = r - mean
    var = jnp.mean(cen * cen, axis=-1, keepdims=True)
    rstd = lax.rsqrt(var + LN_EPS)
    return cen * rstd, rstd


def ln_back(dy, xhat, rstd):
    m1 = jnp.mean(dy, axis=-1, keepdims=True)
    m2 = jnp.mean(dy * xhat, axis=-1, keepdims=True)
    return rstd * (dy - m1 - xhat * m2)


def fold_sq(v):
    rows, cols = v.shape
    s = jnp.sum((v * v).reshape(rows // SUB, SUB, cols), axis=0)
    out = s[:, 0:D1]
    for q in range(1, cols // D1):
        out = out + s[:, D1 * q:D1 * (q + 1)]
    return out


def total(acc):
    return jnp.sum(jnp.sum(acc, axis=1, keepdims=True), axis=0, keepdims=True)


def ds(start, size, mult=None):
    if isinstance(start, int):
        return pl.ds(start, size)
    return pl.ds(pl.multiple_of(start, mult or size), size)


def onehot_rows(t):
    row = lax.broadcasted_iota(jnp.int32, (IMAGES, WIDE), 0)
    col = lax.broadcasted_iota(jnp.int32, (IMAGES, WIDE), 1)
    return jnp.where(row == t * (WIDE // MT) + col // MT, 1.0, 0.0).astype(BF16)


def stage_one_tile(t, xb, xf, wuo, wdo, dst):
    xf[...] = xb[ds(t * ROWS2, ROWS2), :].astype(F32)
    r = jnp.concatenate([xf[pl.ds(j, TILE, stride=4), :] for j in QUADS], axis=0)
    for b in PAIR:
        xhat, _ = ln_parts(r)
        a = gelu_only(nn(xhat.astype(BF16), wuo[b])).astype(BF16)
        rb = (r + nn(a, wdo[b])).astype(BF16)
        r = rb.astype(F32)
    for j in QUADS:
        dst[ds(t * TILE, TILE), D1 * j:D1 * (j + 1)] = rb[TILE * j:TILE * (j + 1), :]


def update(w, v, g, scale):
    nv = MOMENTUM * v + scale * g.astype(F32)
    nw = w - nv
    return nw, nv


def chunk_of(num, ref):
    if num < CH - 1:
        return ref.at[num]
    half = ref.shape[1] // 2
    return ref.at[CH - 1, pl.ds((num - CH + 1) * half, half)]


class Ring:
    def __init__(self, num, stacks, ssem, rsem, csem, pos):
        self.num = num
        self.g, self.r1, self.r2, self.r3 = (chunk_of(num, ref) for ref in stacks)
        g = self.g
        self.ssem, self.rsem, self.csem = ssem, rsem, csem
        self.pos = pos
        self.rb = g.shape[0] // NDEV
        c, f, s = pos['c'], pos['f'], pos['s']
        self.f, self.s, self.nf, self.ns = f, s, 1 - f, 1 - s
        self.mine, self.other = 4 * c, 4 - 4 * c
        self.keep = self.mine + 2 * f
        self.give = self.mine + 2 * self.nf
        self.own_b, self.s_b = self.keep + s, self.keep + self.ns
        self.f_b, self.d_b = self.give + s, self.give + self.ns

    def blk(self, b, n=1):
        return self.g.at[ds(b * self.rb, n * self.rb, self.rb)]

    def rc(self, k, src, dst, dev):
        return pltpu.make_async_remote_copy(src_ref=src, dst_ref=dst, send_sem=self.ssem.at[self.num, k], recv_sem=self.rsem.at[self.num, k], device_id=(self.pos[dev],), device_id_type=MESH)

    def add(self, b, recv, i, n):
        rows, width = n * self.rb, self.g.shape[1]
        step = min(rows, CHUNK // width)
        b0, i0 = b * self.rb, i * self.rb

        def body(j, carry):
            dst = ds(b0 + j * step, step)
            src = ds(i0 + j * step, step)
            self.g[dst, :] = (self.g[dst, :].astype(F32) + recv[src, :].astype(F32)).astype(BF16)
            return carry

        lax.fori_loop(0, rows // step, body, 0)

    def to_core(self):
        return self.rc(0, self.blk(self.other, 4), self.r1, 'core')

    def to_f(self):
        return self.rc(1, self.blk(self.give, 2), self.r2, 'fn')

    def to_s(self):
        return self.rc(2, self.blk(self.s_b), self.r3, 'sn')

    def back(self, k, b, dev):
        return self.rc(k, self.blk(b), self.blk(b), dev)

    def own_to_s(self):
        return self.back(3, self.own_b, 'sn')

    def own_to_f(self):
        return self.back(4, self.own_b, 'fn')

    def own_to_core(self):
        return self.back(5, self.own_b, 'core')

    def s_to_f(self):
        return self.back(6, self.s_b, 'fn')

    def s_to_core(self):
        return self.back(7, self.s_b, 'core')

    def f_to_core(self):
        return self.back(8, self.f_b, 'core')

    def d_to_core(self):
        return self.back(9, self.d_b, 'core')

    def half(self):
        self.to_core().start()

    def link_f(self):
        self.to_core().wait_recv()
        self.add(self.give, self.r1, 2 * self.nf, 2)
        self.to_f().start()
        self.add(self.keep, self.r1, 2 * self.f, 2)

    def link_s(self):
        self.to_f().wait_recv()
        self.add(self.s_b, self.r2, self.ns, 1)
        self.to_s().start()
        self.add(self.own_b, self.r2, self.s, 1)
        self.to_core().wait_send()
        self.free(0, 'core')
        self.to_f().wait_send()
        self.free(1, 'fn')

    def own(self):
        self.to_s().wait_recv()
        self.to_s().wait_send()
        self.free(2, 'sn')
        self.add(self.own_b, self.r3, 0, 1)
        self.held(1)
        self.own_to_f().start()
        self.held(0)
        self.own_to_core().start()

    def own_s(self):
        self.held(2)
        self.own_to_s().start()

    def pass_s(self):
        self.own_to_s().wait_recv()
        self.s_to_f().start()
        self.s_to_core().start()

    def pass_f(self):
        self.own_to_f().wait_recv()
        self.f_to_core().start()

    def pass_d(self):
        self.s_to_f().wait_recv()
        self.d_to_core().start()

    def done(self):
        for cp in (self.own_to_core(), self.s_to_core(), self.f_to_core(), self.d_to_core()):
            cp.wait()
        for cp in (self.own_to_s(), self.own_to_f(), self.s_to_f()):
            cp.wait_send()

    def free(self, i, who):
        pl.semaphore_signal(self.csem.at[self.num, i], inc=1, device_id=(self.pos[who],), device_id_type=MESH)

    def held(self, i):
        pl.semaphore_wait(self.csem.at[self.num, i], 1)


class Share:
    def __init__(self, buf, ssem, rsem, pos):
        self.buf, self.ssem, self.rsem, self.pos = buf, ssem, rsem, pos

    def rc(self, k):
        p = self.pos
        own, fblk, sblk, dblk = p['me'], p['fn'], p['sn'], p['diag']
        b, dev = {0: (own, 'fn'), 1: (own, 'sn'), 2: (own, 'core'), 3: (fblk, 'sn'), 4: (fblk, 'core'), 5: (sblk, 'core'), 6: (dblk, 'core')}[k]
        return pltpu.make_async_remote_copy(src_ref=self.buf.at[b], dst_ref=self.buf.at[b], send_sem=self.ssem.at[k], recv_sem=self.rsem.at[k], device_id=(p[dev],), device_id_type=MESH)


    def send(self):
        for k in (0, 1, 2):
            self.rc(k).start()

    def relay(self):
        self.rc(0).wait_recv()
        self.rc(3).start()
        self.rc(4).start()
        self.rc(1).wait_recv()
        self.rc(5).start()

    def done(self):
        self.rc(3).wait_recv()
        self.rc(6).start()
        for k in (2, 4, 5, 6):
            self.rc(k).wait_recv()
        for k in range(7):
            self.rc(k).wait_send()


def position():
    me = lax.axis_index('data')
    c = lax.rem(me, 2)
    x = lax.rem(me // 2, 2)
    y = me // 4
    f = c * y + (1 - c) * x
    s = c * x + (1 - c) * y
    xn = me + 2 - 4 * x
    yn = me + 4 - SUB * y
    fn = c * yn + (1 - c) * xn
    sn = c * xn + (1 - c) * yn
    diag = xn + yn - me
    core = me + 1 - 2 * c
    return dict(me=me, c=c, f=f, s=s, fn=fn, sn=sn, diag=diag, core=core)


STEPS = ('half', 'link_f', 'link_s', 'own', 'own_s', 'pass_s', 'pass_f', 'pass_d', 'done')
SHARE_STEPS = ('send', 'relay', 'done')
PLAN = dict(
    up1=((), ('a0',), (), ('b0',),),
    in1=((), ('a1',), ('s1', 'b1',), (),),
    dn0=((), ('c0',), (), ('d0',),),
    pre0=((), ('c1', 'a2',), ('s2', 'd1',), (),),
    up0=((), ('b2', 'e0',), (), ('f0',),),
    in0=(('a3', 'e1',), ('a4', 'c2', 'f1',), ('b3',), (),),
    mrg=(('b4', 'h0',),),
    back=(('a5', 'a6', 'd2', 'h1',), ('b5', 'c3',), ('c4', 'd3', 'e2', 'f2',), ('a7', 'b6', 'd4', 'g0',),),
    rank=(('c5', 'h2',), ('a8', 'g1',), ('b7', 'e3',), ('e4',),),
    rankh=(('b8', 'c6', 'f3',), (), ('f4',), ('d5',),),
    tail=('d6', 'h3', 'h4', 'c7', 'e5', 'c8', 'g2', 'f5', 'h5', 'e6', 'g3', 'f6', 'g4', 'd7', 'h6', 'd8', 'e7', 'g5', 'f7', 'e8', 'h7', 'g6', 'f8', 'g7', 'h8', 'g8', ),
)


def grad_kernel(x_hbm, lab, uo_hbm, do_hbm, m_hbm, ut_hbm, dt_hbm, h_hbm,
                g_all, gv1_out, gh_out, scal,
                r1_all, r2_all, r3_all, lr, gdup,
                wuo, wdo, wm, wut, wdt, wh,
                merged, n1, rst1, r2, n2, rst2, a2, sl2, pooled, asum, accv, accu, sq, gsq,
                in_sem, st_sem, out_sem, ssem, rsem, csem, lssem, lrsem):
    pos = position()
    barrier = pltpu.get_barrier_semaphore()
    for who in ('core', 'fn', 'sn'):
        pl.semaphore_signal(barrier, inc=1, device_id=(pos[who],), device_id_type=MESH)

    gv1, gh, grad = wdt.at[1], wh, r2

    share = Share(lr, lssem, lrsem, pos)
    rings = {letter: Ring(i, (g_all, r1_all, r2_all, r3_all), ssem, rsem, csem, pos) for i, letter in enumerate(LETTERS)}

    def norm_of(letter):
        ref = g_all.at[LETTERS.index(letter)]

        def body(i, acc):
            return acc + fold_sq(ref[ds(i * MT, MT), :].astype(F32))

        gsq[NORM_ROW[letter]] += lax.fori_loop(0, ROWS2 // MT, body, jnp.zeros((SUB, D1), F32))

    def act(word):
        letter, num = word[0], int(word[1])
        if letter == 's':
            getattr(share, SHARE_STEPS[num])()
        else:
            getattr(rings[letter], STEPS[num])()
            if STEPS[num] == 'done':
                if letter in NORM_ROW:
                    norm_of(letter)

    def run(name, body):
        plan = PLAN[name]

        def wrapped(t, carry):
            body(t)
            for i, words in enumerate(plan):
                if words:
                    @pl.when(t == i)
                    def _():
                        for word in words:
                            act(word)
            return carry

        lax.fori_loop(0, len(plan), wrapped, 0)

    def forward(xb, xf, suo, sdo, sm, sut, sdt, abuf):
        loads = [pltpu.make_async_copy(src, dst, in_sem.at[i]) for i, (src, dst) in enumerate(((x_hbm, xb), (uo_hbm, suo), (do_hbm, sdo), (m_hbm, sm), (h_hbm, sdt.at[0:CLASSES])))]

        def stage_up(i):
            return pltpu.make_async_copy(ut_hbm.at[i // 2, ds((i % 2) * TILE, TILE)], sut, st_sem.at[0])

        def stage_down(i):
            return pltpu.make_async_copy(dt_hbm.at[i // 2, ds((i % 2) * ROWS2, ROWS2)], sdt, st_sem.at[1])

        for cp in loads[:3]:
            cp.start()
        stage_up(0).start()
        stage_down(0).start()
        loads[3].start()
        sq[...] = jnp.zeros_like(sq)
        for cp in loads[:3]:
            cp.wait()
        for b in PAIR:
            v = suo[b]
            sq[b] = fold_sq(v)
            wuo[b] = v.astype(BF16)
            v = sdo[b]
            sq[2 + b] = fold_sq(v)
            wdo[b] = v.astype(BF16)

        def stage_one(t, carry):
            xf[...] = xb[ds(t * ROWS2, ROWS2), :].astype(F32)
            r = jnp.concatenate([xf[pl.ds(j, TILE, stride=4), :] for j in QUADS], axis=0)
            rows = ds(t * ROWS2, ROWS2)
            for b in PAIR:
                xhat, rstd = ln_parts(r)
                n = xhat.astype(BF16)
                n1[b, rows, :] = n
                if b == 1:
                    rst1[rows, :] = rstd
                a = gelu_only(nn(n, wuo[b])).astype(BF16)
                rb = (r + nn(a, wdo[b])).astype(BF16)
                r = rb.astype(F32)
            for j in QUADS:
                merged[ds(t * TILE, TILE), D1 * j:D1 * (j + 1)] = rb[TILE * j:TILE * (j + 1), :]
            layer = t // 2
            stage_up(t).wait()

            def cast_up(i, acc):
                v = sut[ds(i * 32, 32), :]
                wut[layer, ds((t % 2) * TILE + i * 32, 32), :] = v.astype(BF16)
                return acc + fold_sq(v)

            sq[4 + layer] += lax.fori_loop(0, SUB, cast_up, jnp.zeros((SUB, D1), F32))
            stage_down(t).wait()

            def cast_down(i, acc):
                v = sdt[ds(i * D1, D1), :]
                wdt[layer, ds((t % 2) * ROWS2 + i * D1, D1), :] = v.astype(BF16)
                return acc + fold_sq(v)

            sq[6 + layer] += lax.fori_loop(0, SUB, cast_down, jnp.zeros((SUB, D1), F32))

            @pl.when(t < 3)
            def _():
                stage_up(t + 1).start()
                stage_down(t + 1).start()

            return carry

        lax.fori_loop(0, NTILE, stage_one, 0)

        loads[4].start()
        loads[3].wait()

        def cast_m(i, acc):
            v = sm[ds(i * MT, MT), :]
            wm[ds(i * MT, MT), :] = v.astype(BF16)
            return acc + fold_sq(v)

        sq[SUB] = lax.fori_loop(0, SUB, cast_m, jnp.zeros((SUB, D1), F32))

        def merge_tile(t, carry):
            rows = ds(t * WIDE, WIDE)
            r2[rows, :] = nn(merged[rows, :], wm[...]).astype(BF16)
            return carry

        lax.fori_loop(0, ROWS2 // WIDE, merge_tile, 0)
        asum[...] = jnp.zeros_like(asum)
        pooled[...] = jnp.zeros_like(pooled)

        for layer in PAIR:
            def stage_two(t, carry):
                rows = ds(t * WIDE, WIDE)
                r = r2[rows, :].astype(F32)
                xhat, rstd = ln_parts(r)
                n = xhat.astype(BF16)
                n2[layer, rows, :] = n
                rst2[layer, rows, :] = rstd
                for q in QUADS:
                    cols = slice(D2 * q, D2 * (q + 1))
                    acts, slope = gelu_pair(nn(n, wut[layer, :, cols]))
                    if layer == 0:
                        a2[rows, cols] = acts.astype(BF16)
                    else:
                        abuf[:, cols] = acts.astype(BF16)
                    sl2[layer, rows, cols] = slope.astype(BF16)
                if layer == 0:
                    r2[rows, :] = (r + nn(a2[rows, :], wdt[layer])).astype(BF16)
                else:
                    rb = (r + nn(abuf[...], wdt[layer])).astype(BF16)
                    pick = onehot_rows(t)
                    asum[...] += nn(pick, abuf[...])
                    pooled[...] += nn(pick, rb)
                return carry

            lax.fori_loop(0, ROWS2 // WIDE, stage_two, 0)
        wh[CLASSES:, :] = jnp.zeros((CPAD - CLASSES, D2), BF16)
        loads[4].wait()
        for k in QUADS:
            rows = slice(TILE * k, min(TILE * (k + 1), CLASSES))
            v = sdt[rows, :]
            wh[rows, :] = v.astype(BF16)
            sq[9] += fold_sq(v)

    pl.run_scoped(
        forward,
        pltpu.VMEM((ROWS1, D1), BF16),
        pltpu.VMEM((ROWS2, D1), F32),
        pltpu.VMEM((2, D1, H1), F32),
        pltpu.VMEM((2, H1, D1), F32),
        pltpu.VMEM((D2, D2), F32),
        pltpu.VMEM((TILE, H2), F32),
        pltpu.VMEM((ROWS2, D2), F32),
        pltpu.VMEM((WIDE, H2), BF16),
    )

    xhat, rstd = ln_parts(pooled[...] * (1.0 / MT))
    hb = xhat.astype(BF16)
    logits = nt(hb, wh[...])
    col = lax.broadcasted_iota(jnp.int32, (IMAGES, CPAD), 1)
    row = lax.broadcasted_iota(jnp.int32, (IMAGES, CPAD), 0)
    logits = jnp.where(col < CLASSES, logits, -jnp.inf)
    ex = jnp.exp(logits - jnp.max(logits, axis=-1, keepdims=True))
    prob = ex / jnp.sum(ex, axis=-1, keepdims=True)
    lab_row = jnp.zeros((IMAGES, CPAD), jnp.int32)
    for i in range(IMAGES):
        lab_row = jnp.where(row == i, lab[i], lab_row)
    gl = ((prob - jnp.where(col == lab_row, 1.0, 0.0)) * (1.0 / (IMAGES * NDEV))).astype(BF16)
    g16 = (ln_back(nn(gl, wh[...]), xhat, rstd) * (1.0 / MT)).astype(BF16)
    hi = asum[...].astype(BF16)
    lo = (asum[...] - hi.astype(F32)).astype(BF16)
    me = pos['me']
    lr[me, 0:IMAGES, 0:H2] = hi
    lr[me, IMAGES:32, 0:H2] = lo
    lr[me, 0:IMAGES, H2:LRG] = g16
    lr[me, IMAGES:32, H2:LRG] = hb
    lr[me, 0:IMAGES, LRG:LRW] = gl[:, 0:D2]
    lr[me, IMAGES:32, LRG:LRW] = gl[:, D2:CPAD]
    pl.semaphore_wait(barrier, 3)
    share.send()

    asum[...] = nt(g16, wdt[1])
    pooled[...] = g16.astype(F32)

    def slope_one(i, carry):
        rows = ds(i * MT, MT)
        grad[rows, :] = jnp.broadcast_to(pooled[pl.ds(i, 1), :], (MT, D2)).astype(BF16)
        for q in QUADS:
            cols = slice(D2 * q, D2 * (q + 1))
            sl2[1, rows, cols] = (asum[pl.ds(i, 1), cols] * sl2[1, rows, cols].astype(F32)).astype(BF16)
        return carry

    lax.fori_loop(0, IMAGES, slope_one, 0)

    def up_grad(layer, first):
        def body(q):
            g_all[first + q // 2, ds((q % 2) * D2, D2), :] = tn(n2[layer], sl2[layer, :, ds(q * D2, D2)]).astype(BF16)

        return body

    def down_grad(q):
        g_all[2 + q // 2, ds((q % 2) * D2, D2), :] = tn(a2[:, ds(q * D2, D2)], grad[...]).astype(BF16)

    def input_grad(layer):
        def body(t):
            rows = ds(t * TILE, TILE)
            dy = nt(sl2[layer, rows, :], wut[layer])
            dx = ln_back(dy, n2[layer, rows, :].astype(F32), rst2[layer, rows, :])
            grad[rows, :] = (dx + grad[rows, :].astype(F32)).astype(BF16)

        return body

    def pre_grad(t):
        rows = ds(t * TILE, TILE)
        for q in QUADS:
            cols = slice(D2 * q, D2 * (q + 1))
            ga = nt(grad[rows, :], wdt[0, cols, :])
            sl2[0, rows, cols] = (ga * sl2[0, rows, cols].astype(F32)).astype(BF16)

    gsm = g_all.at[CH - 1]

    def merge_grad(t):
        gsm[D2:ROWS2, :] = tn(merged[...], grad[...]).astype(BF16)

    def stage_one_back(t):
        gm = nt(grad[ds(t * TILE, TILE), :], wm[...]).astype(BF16)
        rows = ds(t * ROWS2, ROWS2)
        g = jnp.concatenate([gm[:, D1 * j:D1 * (j + 1)] for j in QUADS], axis=0)
        for b in (1, 0):
            n = n1[b, rows, :]
            acts, slope = gelu_pair(nn(n, wuo[b]))
            accv[b] += tn(acts.astype(BF16), g)
            gp = (nt(g, wdo[b]) * slope).astype(BF16)
            accu[b] += tn(n, gp)
            if b == 1:
                dx = ln_back(nt(gp, wuo[b]), n.astype(F32), rst1[rows, :])
                g = (dx + g.astype(F32)).astype(BF16)

        @pl.when(t == 3)
        def _():
            for b in PAIR:
                gsm[D1 * b:D1 * (b + 1), :] = accu[b].astype(BF16)
                for q in PAIR:
                    gsm[TILE:D2, TILE * b + D1 * q:TILE * b + D1 * (q + 1)] = accv[b, TILE * q:TILE * (q + 1), :].astype(BF16)

    run('up1', up_grad(1, 0))
    run('in1', input_grad(1))
    run('dn0', down_grad)
    run('pre0', pre_grad)
    run('up0', up_grad(0, 4))
    run('in0', input_grad(0))
    accv[...] = jnp.zeros_like(accv)
    accu[...] = jnp.zeros_like(accu)
    gsq[...] = jnp.zeros_like(gsq)
    run('mrg', merge_grad)
    run('back', stage_one_back)

    def v1_rows(i):
        cols = ds(i * D2, D2)
        out = jnp.zeros((D2, D2), F32)
        for d in range(NDEV):
            out = out + tn(lr[d, :, cols], gdup[d]).astype(BF16).astype(F32)
        ob = out.astype(BF16)
        gv1[cols, :] = ob
        gsq[7] += fold_sq(ob.astype(F32))

    def head_rows(i):
        rows = ds(i * TILE, TILE)
        out = jnp.zeros((TILE, D2), F32)
        for d in range(NDEV):
            gl_d = lr[d, ds((i // 2) * IMAGES, IMAGES), ds(LRG + (i % 2) * TILE, TILE)]
            out = out + tn(gl_d, lr[d, IMAGES:32, H2:LRG]).astype(BF16).astype(F32)
        ob = out.astype(BF16)
        gh[rows, :] = ob
        gsq[9] += fold_sq(ob.astype(F32))

    gv1_cp = pltpu.make_async_copy(gv1, gv1_out, out_sem.at[0])
    gh_cp = pltpu.make_async_copy(gh, gh_out, out_sem.at[1])
    for d in range(NDEV):
        gdup[d, 0:IMAGES, :] = lr[d, 0:IMAGES, H2:LRG]
        gdup[d, IMAGES:32, :] = lr[d, 0:IMAGES, H2:LRG]
    run('rank', v1_rows)
    gv1_cp.start()
    run('rankh', head_rows)
    gh_cp.start()
    for word in PLAN['tail']:
        act(word)
    for b in PAIR:
        gsq[b] = fold_sq(gsm[D1 * b:D1 * (b + 1), :].astype(F32))
        gsq[2 + b] = fold_sq(gsm[TILE:D2, TILE * b:TILE * (b + 1)].astype(F32))
    gsq[SUB] = fold_sq(gsm[D2:ROWS2, :].astype(F32))
    for i in range(10):
        ratio = jnp.sqrt(total(sq[i])) / jnp.sqrt(total(gsq[i]))
        scal[i:i + 1, :] = jnp.broadcast_to(TRUST * ratio, (1, D1))
    scal[10:IMAGES, :] = jnp.zeros((6, D1), F32)
    gv1_cp.wait()
    gh_cp.wait()


def step_kernel(x_hbm, uo_hbm, do_hbm, m_hbm, ut_hbm, dt_hbm, h_hbm, vuo_hbm, vdo_hbm, vm_hbm, vut_hbm, vdt_hbm, vh_hbm,
                g_all, gv1_hbm, gh_hbm, scal,
                logits_out, uo_out, do_out, m_out, ut_out, dt_out, h_out, vuo_out, vdo_out, vm_out, vut_out, vdt_out, vh_out,
                xb, xf, gv1, gh, suo, sdo, sm, sh, sut, sdt, tuo, tdo, tm, th, tut, tdt,
                wuo, wdo, wm, wut, wdt, wh, r2, pooled,
                s_in, s_out, q_in, q_out, g_sem):
    small = [(uo_hbm, suo, uo_out), (vuo_hbm, tuo, vuo_out), (do_hbm, sdo, do_out), (vdo_hbm, tdo, vdo_out), (m_hbm, sm, m_out), (vm_hbm, tm, vm_out), (h_hbm, sh, h_out), (vh_hbm, th, vh_out)]
    ins = [pltpu.make_async_copy(src, buf, s_in.at[i]) for i, (src, buf, _) in enumerate(small)]
    louts = [pltpu.make_async_copy(buf, dst, s_out.at[i]) for i, (_, buf, dst) in enumerate(small)]
    up_big = [(ut_hbm, sut, ut_out), (vut_hbm, tut, vut_out)]
    down_big = [(dt_hbm, sdt, dt_out), (vdt_hbm, tdt, vdt_out)]
    gsm = g_all.at[CH - 1]

    def copies(layer, t, into, which=QUADS):
        out = []
        for k in which:
            src, buf, dst = (up_big + down_big)[k]
            n = D1 if k in PAIR else D2
            rows = ds(t * n, n)
            here = buf.at[rows] if k in PAIR else buf.at[layer, rows]
            if into:
                out.append(pltpu.make_async_copy(src.at[layer, rows], here, q_in.at[layer, k, t]))
            else:
                out.append(pltpu.make_async_copy(here, dst.at[layer, rows], q_out.at[layer, k, t]))
        return out

    def start(cps):
        for cp in cps:
            cp.start()

    def wait(cps):
        for cp in cps:
            cp.wait()

    x_cp = pltpu.make_async_copy(x_hbm, xb, g_sem.at[CH])
    gv1_cp = pltpu.make_async_copy(gv1_hbm, gv1, g_sem.at[CH + 1])
    gh_cp = pltpu.make_async_copy(gh_hbm, gh, g_sem.at[CH + 2])

    def up_part(layer, t):
        scale = scal[4 + layer:5 + layer, 0:1]
        rows = ds(t * D1, D1)
        for q in QUADS:
            cols = slice(D2 * q, D2 * (q + 1))
            g = g_all[4 - 4 * layer + q // 2, ds((q % 2) * D2 + t * D1, D1), :]
            nw, nv = update(sut[rows, cols], tut[rows, cols], g, scale)
            sut[rows, cols] = nw
            tut[rows, cols] = nv
            wut[layer, rows, cols] = nw.astype(BF16)

    def down_part(layer, t):
        rows = ds(t * D2, D2)
        g = g_all[2 + t // 2, ds((t % 2) * D2, D2), :] if layer == 0 else gv1[rows, :]
        nw, nv = update(sdt[layer, rows, :], tdt[layer, rows, :], g, scal[6 + layer:7 + layer, 0:1])
        sdt[layer, rows, :] = nw
        tdt[layer, rows, :] = nv
        wdt[layer, rows, :] = nw.astype(BF16)

    def stage_two(layer, r):
        xhat, _ = ln_parts(r)
        n = xhat.astype(BF16)
        acc = r
        for q in QUADS:
            cols = slice(D2 * q, D2 * (q + 1))
            a = gelu_only(nn(n, wut[layer, :, cols])).astype(BF16)
            acc = acc + nn(a, wdt[layer, cols, :])
        return acc.astype(BF16)

    first_in = [x_cp] + ins[:4]
    later = [gv1_cp]
    start(first_in)
    start(copies(0, 0, True))
    wait(first_in)
    for b in PAIR:
        nw, tuo[b] = update(suo[b], tuo[b], gsm[D1 * b:D1 * (b + 1), :], scal[b:b + 1, 0:1])
        suo[b] = nw
        wuo[b] = nw.astype(BF16)
        for q in PAIR:
            rows = slice(TILE * q, TILE * (q + 1))
            nw, tdo[b, rows, :] = update(sdo[b, rows, :], tdo[b, rows, :], gsm[TILE:D2, TILE * b + D1 * q:TILE * b + D1 * (q + 1)], scal[2 + b:3 + b, 0:1])
            sdo[b, rows, :] = nw
            wdo[b, rows, :] = nw.astype(BF16)

    def stage_one_update(t, carry):
        wait(copies(0, t, True))

        @pl.when(t < 3)
        def _():
            start(copies(0, t + 1, True))

        @pl.when(t == 1)
        def _():
            start(ins[4:6])

        @pl.when(t == 2)
        def _():
            start(later)

        @pl.when(t == 3)
        def _():
            start(copies(1, 0, True, DOWNS))
            start(copies(1, 1, True, DOWNS))
            start([gh_cp] + ins[6:])

        stage_one_tile(t, xb, xf, wuo, wdo, r2)
        up_part(0, t)
        down_part(0, t)
        start(copies(0, t, False, PAIR))
        return carry

    lax.fori_loop(0, NTILE, stage_one_update, 0)
    start(copies(1, 2, True, DOWNS))
    start(copies(1, 3, True, DOWNS))
    wait(ins[4:6])
    nw, tm[...] = update(sm[...], tm[...], gsm[D2:ROWS2, :], scal[SUB:9, 0:1])
    sm[...] = nw
    wm[...] = nw.astype(BF16)

    def merge_tile(t, carry):
        rows = ds(t * WIDE, WIDE)
        r2[rows, :] = nn(r2[rows, :], wm[...]).astype(BF16)
        return carry

    lax.fori_loop(0, ROWS2 // WIDE, merge_tile, 0)
    wait(later)
    pooled[...] = jnp.zeros_like(pooled)

    def first(t, carry):
        rows = ds(t * WIDE, WIDE)
        for i in PAIR:
            wait(copies(0, 2 * t + i, False, PAIR))
            start(copies(1, 2 * t + i, True, PAIR))
        for i in PAIR:
            wait(copies(1, 2 * t + i, True, DOWNS))
            start(copies(0, 2 * t + i, False, DOWNS))
        r2[rows, :] = stage_two(0, r2[rows, :].astype(F32))
        for i in PAIR:
            down_part(1, 2 * t + i)
        return carry

    lax.fori_loop(0, ROWS2 // WIDE, first, 0)
    def second_up(t, carry):
        wait(copies(1, t, True, PAIR))
        up_part(1, t)
        start(copies(1, t, False))
        return carry

    lax.fori_loop(0, NTILE, second_up, 0)
    start(louts[:6])
    wh[CLASSES:, :] = jnp.zeros((CPAD - CLASSES, D2), BF16)
    wait(ins[6:] + [gh_cp])

    def head_update(rows):
        nw, th[rows, :] = update(sh[rows, :], th[rows, :], gh[rows, :], scal[9:10, 0:1])
        sh[rows, :] = nw
        wh[rows, :] = nw.astype(BF16)

    def head_part(i, carry):
        head_update(ds(i * HEAD_STEP, HEAD_STEP))
        return carry

    lax.fori_loop(0, CLASSES // HEAD_STEP, head_part, 0)
    head_update(slice(CLASSES - CLASSES % HEAD_STEP, CLASSES))
    start(louts[6:])

    def second(t, carry):
        rows = ds(t * WIDE, WIDE)
        rb = stage_two(1, r2[rows, :].astype(F32))
        pooled[...] += nn(onehot_rows(t), rb)
        return carry

    lax.fori_loop(0, ROWS2 // WIDE, second, 0)
    xhat, _ = ln_parts(pooled[...] * (1.0 / MT))
    logits = nt(xhat.astype(BF16), wh[...])
    logits_out[...] = logits[:, 0:CLASSES]
    wait(louts)
    for t in QUADS:
        wait(copies(0, t, False, DOWNS))
        wait(copies(1, t, False))


def weight_scratch():
    return [pltpu.VMEM((2, D1, H1), BF16), pltpu.VMEM((2, H1, D1), BF16), pltpu.VMEM((D2, D2), BF16), pltpu.VMEM((2, D2, H2), BF16), pltpu.VMEM((2, H2, D2), BF16), pltpu.VMEM((CPAD, D2), BF16)]


def master_scratch():
    return [pltpu.VMEM((2, D1, H1), F32), pltpu.VMEM((2, H1, D1), F32), pltpu.VMEM((D2, D2), F32), pltpu.VMEM((CLASSES, D2), F32), pltpu.VMEM((D2, H2), F32), pltpu.VMEM((2, H2, D2), F32)]


def solution(mesh):
    hbm = pl.BlockSpec(memory_space=pl.ANY)
    vmem = pl.BlockSpec(memory_space=pltpu.VMEM)
    smem = pl.BlockSpec(memory_space=pltpu.SMEM)
    shape = jax.ShapeDtypeStruct
    dma = pltpu.SemaphoreType.DMA
    wide_g = [shape((CH, ROWS2, D2), BF16), shape((H2, D2), BF16), shape((CPAD, D2), BF16)]
    masters = [shape((2, D1, H1), F32), shape((2, H1, D1), F32), shape((D2, D2), F32), shape((2, D2, H2), F32), shape((2, H2, D2), F32), shape((CLASSES, D2), F32)]

    grads_call = pl.pallas_call(
        grad_kernel,
        out_shape=[pltpu.VMEM(wide_g[0].shape, BF16)] + wide_g[1:] + [shape((IMAGES, D1), F32)],
        in_specs=[hbm, smem] + [hbm] * 6,
        out_specs=[vmem] + [hbm] * 2 + [vmem],
        scratch_shapes=[pltpu.VMEM((CH, ROWS2 // k, D2), BF16) for k in (2, 4, NDEV)]
        + [pltpu.VMEM((NDEV, 32, LRW), BF16), pltpu.VMEM((NDEV, 32, D2), BF16)]
        + weight_scratch()
        + [pltpu.VMEM((ROWS2, D2), BF16), pltpu.VMEM((2, ROWS1, D1), BF16), pltpu.VMEM((ROWS1, 1), F32), pltpu.VMEM((ROWS2, D2), BF16), pltpu.VMEM((2, ROWS2, D2), BF16), pltpu.VMEM((2, ROWS2, 1), F32), pltpu.VMEM((ROWS2, H2), BF16), pltpu.VMEM((2, ROWS2, H2), BF16), pltpu.VMEM((IMAGES, D2), F32), pltpu.VMEM((IMAGES, H2), F32), pltpu.VMEM((2, H1, D1), F32), pltpu.VMEM((2, D1, H1), F32), pltpu.VMEM((10, SUB, D1), F32), pltpu.VMEM((10, SUB, D1), F32)]
        + [dma((5,)), dma((2,)), dma((2,)), dma((CH + 1, 10)), dma((CH + 1, 10)), pltpu.SemaphoreType.REGULAR((CH + 1, 3)), dma((CH,)), dma((CH,))],
        compiler_params=pltpu.CompilerParams(collective_id=0, has_side_effects=True, vmem_limit_bytes=SCOPED_LIMIT),
        name="grads",
    )

    step_call = pl.pallas_call(
        step_kernel,
        out_shape=[shape((IMAGES, CLASSES), F32)] + masters * 2,
        in_specs=[hbm] * 13 + [vmem] + [hbm] * 2 + [vmem],
        out_specs=[vmem] + [hbm] * 12,
        scratch_shapes=[pltpu.VMEM((ROWS1, D1), BF16), pltpu.VMEM((ROWS2, D1), F32)]
        + [pltpu.VMEM(g.shape, BF16) for g in wide_g[1:]]
        + master_scratch() * 2
        + weight_scratch()
        + [pltpu.VMEM((ROWS2, D2), BF16), pltpu.VMEM((IMAGES, D2), F32)]
        + [dma((SUB,)), dma((SUB,)), dma((2, 4, 4)), dma((2, 4, 4)), dma((CH + 3,))],
        compiler_params=pltpu.CompilerParams(vmem_limit_bytes=SCOPED_LIMIT),
        name="step",
    )

    def local_step(x_now, labels_now, x_next, up_one, down_one, merge_proj, up_two, down_two, head_proj, vel_up_one, vel_down_one, vel_merge_proj, vel_up_two, vel_down_two, vel_head_proj):
        params = (up_one, down_one, merge_proj, up_two, down_two, head_proj.T)
        vels = (vel_up_one, vel_down_one, vel_merge_proj, vel_up_two, vel_down_two, vel_head_proj.T)
        got = grads_call(x_now.reshape(ROWS1, D1), labels_now, *params)
        stack = pltpu.with_memory_space_constraint(got[0], pltpu.VMEM)
        outs = list(step_call(x_next.reshape(ROWS1, D1), *params, *vels, stack, *got[1:]))
        outs[6], outs[12] = outs[6].T, outs[12].T
        return tuple(outs)

    replicated = P()
    batch_split = P('data')
    in_specs = (batch_split, batch_split, batch_split) + (replicated,) * 12
    out_specs = (batch_split,) + (replicated,) * 12
    return jax.shard_map(local_step, mesh=mesh, in_specs=in_specs, out_specs=out_specs, check_vma=False)
```

```python
import jax
import jax.numpy as jnp
from jax import lax
from jax.experimental import pallas as pl
from jax.experimental.pallas import tpu as pltpu
from jax.sharding import PartitionSpec as P

MOMENTUM = 0.9
TRUST = 0.1
LN_EPS = 1e-6
GELU_C = 0.7978845608028654
GELU_K = 0.044715
MESH = pl.DeviceIdType.MESH
F32 = jnp.float32
BF16 = jnp.bfloat16
SCOPED_LIMIT = 59600000

IMAGES = 16
TOKENS = 256
D1 = 128
H1 = 512
D2 = 512
H2 = 2048
ROWS1 = IMAGES * TOKENS
ROWS2 = ROWS1 // 4
CLASSES = 1000
CPAD = 1024
TILE = 256
NTILE = ROWS2 // TILE
WIDE = 512
HEAD_STEP = 192
CH = 7
LETTERS = 'abcdefgh'
NORM_ROW = dict(a=5, b=5, c=6, d=6, e=4, f=4)
LRW = 3072
LRG = 2560
NDEV = 8
MT = 64
SUB = 8
PAIR = range(2)
QUADS = range(4)
DOWNS = (2, 3)
CHUNK = 32768


def nn(a, b):
    return lax.dot_general(a, b, (((1,), (0,)), ((), ())), preferred_element_type=F32)


def nt(a, b):
    return lax.dot_general(a, b, (((1,), (1,)), ((), ())), preferred_element_type=F32)


def tn(a, b):
    return lax.dot_general(a, b, (((0,), (0,)), ((), ())), preferred_element_type=F32)


def gelu_only(x):
    inner = x * (GELU_C + (GELU_C * GELU_K) * (x * x))
    half = 0.5 + 0.5 * jnp.tanh(inner)
    return x * half


def gelu_pair(x):
    x2 = x * x
    t = jnp.tanh(x * (GELU_C + (GELU_C * GELU_K) * x2))
    half = 0.5 + 0.5 * t
    act = x * half
    slope = half + act * ((1.0 - t) * (GELU_C + (3.0 * GELU_C * GELU_K) * x2))
    return act, slope


def ln_parts(r):
    mean = jnp.mean(r, axis=-1, keepdims=True)
    cen = r - mean
    var = jnp.mean(cen * cen, axis=-1, keepdims=True)
    rstd = lax.rsqrt(var + LN_EPS)
    return cen * rstd, rstd


def ln_back(dy, xhat, rstd):
    m1 = jnp.mean(dy, axis=-1, keepdims=True)
    m2 = jnp.mean(dy * xhat, axis=-1, keepdims=True)
    return rstd * (dy - m1 - xhat * m2)


def fold_sq(v):
    rows, cols = v.shape
    s = jnp.sum((v * v).reshape(rows // SUB, SUB, cols), axis=0)
    out = s[:, 0:D1]
    for q in range(1, cols // D1):
        out = out + s[:, D1 * q:D1 * (q + 1)]
    return out


def total(acc):
    return jnp.sum(jnp.sum(acc, axis=1, keepdims=True), axis=0, keepdims=True)


def ds(start, size, mult=None):
    if isinstance(start, int):
        return pl.ds(start, size)
    return pl.ds(pl.multiple_of(start, mult or size), size)


def onehot_rows(t):
    row = lax.broadcasted_iota(jnp.int32, (IMAGES, WIDE), 0)
    col = lax.broadcasted_iota(jnp.int32, (IMAGES, WIDE), 1)
    return jnp.where(row == t * (WIDE // MT) + col // MT, 1.0, 0.0).astype(BF16)


def stage_one_tile(t, xb, xf, wuo, wdo, dst):
    xf[...] = xb[ds(t * ROWS2, ROWS2), :].astype(F32)
    r = jnp.concatenate([xf[pl.ds(j, TILE, stride=4), :] for j in QUADS], axis=0)
    for b in PAIR:
        xhat, _ = ln_parts(r)
        a = gelu_only(nn(xhat.astype(BF16), wuo[b])).astype(BF16)
        rb = (r + nn(a, wdo[b])).astype(BF16)
        r = rb.astype(F32)
    for j in QUADS:
        dst[ds(t * TILE, TILE), D1 * j:D1 * (j + 1)] = rb[TILE * j:TILE * (j + 1), :]


def update(w, v, g, scale):
    nv = MOMENTUM * v + scale * g.astype(F32)
    nw = w - nv
    return nw, nv


def chunk_of(num, ref):
    if num < CH - 1:
        return ref.at[num]
    half = ref.shape[1] // 2
    return ref.at[CH - 1, pl.ds((num - CH + 1) * half, half)]


class Ring:
    def __init__(self, num, stacks, ssem, rsem, csem, pos):
        self.num = num
        self.g, self.r1, self.r2, self.r3 = (chunk_of(num, ref) for ref in stacks)
        g = self.g
        self.ssem, self.rsem, self.csem = ssem, rsem, csem
        self.pos = pos
        self.rb = g.shape[0] // NDEV
        c, f, s = pos['c'], pos['f'], pos['s']
        self.f, self.s, self.nf, self.ns = f, s, 1 - f, 1 - s
        self.mine, self.other = 4 * c, 4 - 4 * c
        self.keep = self.mine + 2 * f
        self.give = self.mine + 2 * self.nf
        self.own_b, self.s_b = self.keep + s, self.keep + self.ns
        self.f_b, self.d_b = self.give + s, self.give + self.ns

    def blk(self, b, n=1):
        return self.g.at[ds(b * self.rb, n * self.rb, self.rb)]

    def rc(self, k, src, dst, dev):
        return pltpu.make_async_remote_copy(src_ref=src, dst_ref=dst, send_sem=self.ssem.at[self.num, k], recv_sem=self.rsem.at[self.num, k], device_id=(self.pos[dev],), device_id_type=MESH)

    def add(self, b, recv, i, n):
        rows, width = n * self.rb, self.g.shape[1]
        step = min(rows, CHUNK // width)
        b0, i0 = b * self.rb, i * self.rb

        def body(j, carry):
            dst = ds(b0 + j * step, step)
            src = ds(i0 + j * step, step)
            self.g[dst, :] = (self.g[dst, :].astype(F32) + recv[src, :].astype(F32)).astype(BF16)
            return carry

        lax.fori_loop(0, rows // step, body, 0)

    def to_core(self):
        return self.rc(0, self.blk(self.other, 4), self.r1, 'core')

    def to_f(self):
        return self.rc(1, self.blk(self.give, 2), self.r2, 'fn')

    def to_s(self):
        return self.rc(2, self.blk(self.s_b), self.r3, 'sn')

    def back(self, k, b, dev):
        return self.rc(k, self.blk(b), self.blk(b), dev)

    def own_to_s(self):
        return self.back(3, self.own_b, 'sn')

    def own_to_f(self):
        return self.back(4, self.own_b, 'fn')

    def own_to_core(self):
        return self.back(5, self.own_b, 'core')

    def s_to_f(self):
        return self.back(6, self.s_b, 'fn')

    def s_to_core(self):
        return self.back(7, self.s_b, 'core')

    def f_to_core(self):
        return self.back(8, self.f_b, 'core')

    def d_to_core(self):
        return self.back(9, self.d_b, 'core')

    def half(self):
        self.to_core().start()

    def link_f(self):
        self.to_core().wait_recv()
        self.add(self.give, self.r1, 2 * self.nf, 2)
        self.to_f().start()
        self.add(self.keep, self.r1, 2 * self.f, 2)

    def link_s(self):
        self.to_f().wait_recv()
        self.add(self.s_b, self.r2, self.ns, 1)
        self.to_s().start()
        self.add(self.own_b, self.r2, self.s, 1)
        self.to_core().wait_send()
        self.free(0, 'core')
        self.to_f().wait_send()
        self.free(1, 'fn')

    def own(self):
        self.to_s().wait_recv()
        self.to_s().wait_send()
        self.free(2, 'sn')
        self.add(self.own_b, self.r3, 0, 1)
        self.held(1)
        self.own_to_f().start()
        self.held(0)
        self.own_to_core().start()

    def own_s(self):
        self.held(2)
        self.own_to_s().start()

    def pass_s(self):
        self.own_to_s().wait_recv()
        self.s_to_f().start()
        self.s_to_core().start()

    def pass_f(self):
        self.own_to_f().wait_recv()
        self.f_to_core().start()

    def pass_d(self):
        self.s_to_f().wait_recv()
        self.d_to_core().start()

    def done(self):
        for cp in (self.own_to_core(), self.s_to_core(), self.f_to_core(), self.d_to_core()):
            cp.wait()
        for cp in (self.own_to_s(), self.own_to_f(), self.s_to_f()):
            cp.wait_send()

    def free(self, i, who):
        pl.semaphore_signal(self.csem.at[self.num, i], inc=1, device_id=(self.pos[who],), device_id_type=MESH)

    def held(self, i):
        pl.semaphore_wait(self.csem.at[self.num, i], 1)


class Share:
    def __init__(self, buf, ssem, rsem, pos):
        self.buf, self.ssem, self.rsem, self.pos = buf, ssem, rsem, pos

    def rc(self, k):
        p = self.pos
        own, fblk, sblk, dblk = p['me'], p['fn'], p['sn'], p['diag']
        b, dev = {0: (own, 'fn'), 1: (own, 'sn'), 2: (own, 'core'), 3: (fblk, 'sn'), 4: (fblk, 'core'), 5: (sblk, 'core'), 6: (dblk, 'core')}[k]
        return pltpu.make_async_remote_copy(src_ref=self.buf.at[b], dst_ref=self.buf.at[b], send_sem=self.ssem.at[k], recv_sem=self.rsem.at[k], device_id=(p[dev],), device_id_type=MESH)


    def send(self):
        for k in (0, 1, 2):
            self.rc(k).start()

    def relay(self):
        self.rc(0).wait_recv()
        self.rc(3).start()
        self.rc(4).start()
        self.rc(1).wait_recv()
        self.rc(5).start()

    def done(self):
        self.rc(3).wait_recv()
        self.rc(6).start()
        for k in (2, 4, 5, 6):
            self.rc(k).wait_recv()
        for k in range(7):
            self.rc(k).wait_send()


def position():
    me = lax.axis_index('data')
    c = lax.rem(me, 2)
    x = lax.rem(me // 2, 2)
    y = me // 4
    f = c * y + (1 - c) * x
    s = c * x + (1 - c) * y
    xn = me + 2 - 4 * x
    yn = me + 4 - SUB * y
    fn = c * yn + (1 - c) * xn
    sn = c * xn + (1 - c) * yn
    diag = xn + yn - me
    core = me + 1 - 2 * c
    return dict(me=me, c=c, f=f, s=s, fn=fn, sn=sn, diag=diag, core=core)


STEPS = ('half', 'link_f', 'link_s', 'own', 'own_s', 'pass_s', 'pass_f', 'pass_d', 'done')
SHARE_STEPS = ('send', 'relay', 'done')
PLAN = dict(
    up1=((), ('a0',), (), ('b0',),),
    in1=((), ('a1',), ('s1', 'b1',), (),),
    dn0=((), ('c0',), (), ('d0',),),
    pre0=((), ('c1', 'a2',), ('s2', 'd1',), (),),
    up0=((), ('b2', 'e0',), (), ('f0',),),
    in0=(('a3', 'e1',), ('a4', 'c2', 'f1',), ('b3',), (),),
    mrg=(('b4', 'h0',),),
    back=(('a5', 'a6', 'd2', 'h1',), ('b5', 'c3',), ('c4', 'd3', 'e2', 'f2',), ('a7', 'b6', 'd4', 'g0',),),
    rank=(('c5', 'h2',), ('a8', 'g1',), ('b7', 'e3',), ('e4',),),
    rankh=(('b8', 'c6', 'f3',), (), ('f4',), ('d5',),),
    tail=('d6', 'h3', 'h4', 'c7', 'e5', 'c8', 'g2', 'f5', 'h5', 'e6', 'g3', 'f6', 'g4', 'd7', 'h6', 'd8', 'e7', 'g5', 'f7', 'e8', 'h7', 'g6', 'f8', 'g7', 'h8', 'g8', ),
)


def grad_kernel(x_hbm, lab, uo_hbm, do_hbm, m_hbm, ut_hbm, dt_hbm, h_hbm,
                g_all, gv1_out, gh_out, scal,
                r1_all, r2_all, r3_all, lr, gdup,
                wuo, wdo, wm, wut, wdt, wh,
                merged, n1, rst1, r2, n2, rst2, a2, sl2, pooled, asum, accv, accu, sq, gsq,
                in_sem, st_sem, out_sem, ssem, rsem, csem, lssem, lrsem):
    pos = position()
    barrier = pltpu.get_barrier_semaphore()
    for who in ('core', 'fn', 'sn'):
        pl.semaphore_signal(barrier, inc=1, device_id=(pos[who],), device_id_type=MESH)

    gv1, gh, grad = wdt.at[1], wh, r2

    share = Share(lr, lssem, lrsem, pos)
    rings = {letter: Ring(i, (g_all, r1_all, r2_all, r3_all), ssem, rsem, csem, pos) for i, letter in enumerate(LETTERS)}

    def norm_of(letter):
        ref = g_all.at[LETTERS.index(letter)]

        def body(i, acc):
            return acc + fold_sq(ref[ds(i * MT, MT), :].astype(F32))

        gsq[NORM_ROW[letter]] += lax.fori_loop(0, ROWS2 // MT, body, jnp.zeros((SUB, D1), F32))

    def act(word):
        letter, num = word[0], int(word[1])
        if letter == 's':
            getattr(share, SHARE_STEPS[num])()
        else:
            getattr(rings[letter], STEPS[num])()
            if STEPS[num] == 'done':
                if letter in NORM_ROW:
                    norm_of(letter)

    def run(name, body):
        plan = PLAN[name]

        def wrapped(t, carry):
            body(t)
            for i, words in enumerate(plan):
                if words:
                    @pl.when(t == i)
                    def _():
                        for word in words:
                            act(word)
            return carry

        lax.fori_loop(0, len(plan), wrapped, 0)

    def forward(xb, xf, suo, sdo, sm, sut, sdt, abuf):
        loads = [pltpu.make_async_copy(src, dst, in_sem.at[i]) for i, (src, dst) in enumerate(((x_hbm, xb), (uo_hbm, suo), (do_hbm, sdo), (m_hbm, sm), (h_hbm, sdt.at[0:CLASSES])))]

        def stage_up(i):
            return pltpu.make_async_copy(ut_hbm.at[i // 2, ds((i % 2) * TILE, TILE)], sut, st_sem.at[0])

        def stage_down(i):
            return pltpu.make_async_copy(dt_hbm.at[i // 2, ds((i % 2) * ROWS2, ROWS2)], sdt, st_sem.at[1])

        for cp in loads[:3]:
            cp.start()
        stage_up(0).start()
        stage_down(0).start()
        loads[3].start()
        sq[...] = jnp.zeros_like(sq)
        for cp in loads[:3]:
            cp.wait()
        for b in PAIR:
            v = suo[b]
            sq[b] = fold_sq(v)
            wuo[b] = v.astype(BF16)
            v = sdo[b]
            sq[2 + b] = fold_sq(v)
            wdo[b] = v.astype(BF16)

        def stage_one(t, carry):
            xf[...] = xb[ds(t * ROWS2, ROWS2), :].astype(F32)
            r = jnp.concatenate([xf[pl.ds(j, TILE, stride=4), :] for j in QUADS], axis=0)
            rows = ds(t * ROWS2, ROWS2)
            for b in PAIR:
                xhat, rstd = ln_parts(r)
                n = xhat.astype(BF16)
                n1[b, rows, :] = n
                if b == 1:
                    rst1[rows, :] = rstd
                a = gelu_only(nn(n, wuo[b])).astype(BF16)
                rb = (r + nn(a, wdo[b])).astype(BF16)
                r = rb.astype(F32)
            for j in QUADS:
                merged[ds(t * TILE, TILE), D1 * j:D1 * (j + 1)] = rb[TILE * j:TILE * (j + 1), :]
            layer = t // 2
            stage_up(t).wait()

            def cast_up(i, acc):
                v = sut[ds(i * 32, 32), :]
                wut[layer, ds((t % 2) * TILE + i * 32, 32), :] = v.astype(BF16)
                return acc + fold_sq(v)

            sq[4 + layer] += lax.fori_loop(0, SUB, cast_up, jnp.zeros((SUB, D1), F32))
            stage_down(t).wait()

            def cast_down(i, acc):
                v = sdt[ds(i * D1, D1), :]
                wdt[layer, ds((t % 2) * ROWS2 + i * D1, D1), :] = v.astype(BF16)
                return acc + fold_sq(v)

            sq[6 + layer] += lax.fori_loop(0, SUB, cast_down, jnp.zeros((SUB, D1), F32))

            @pl.when(t < 3)
            def _():
                stage_up(t + 1).start()
                stage_down(t + 1).start()

            return carry

        lax.fori_loop(0, NTILE, stage_one, 0)

        loads[4].start()
        loads[3].wait()

        def cast_m(i, acc):
            v = sm[ds(i * MT, MT), :]
            wm[ds(i * MT, MT), :] = v.astype(BF16)
            return acc + fold_sq(v)

        sq[SUB] = lax.fori_loop(0, SUB, cast_m, jnp.zeros((SUB, D1), F32))

        def merge_tile(t, carry):
            rows = ds(t * WIDE, WIDE)
            r2[rows, :] = nn(merged[rows, :], wm[...]).astype(BF16)
            return carry

        lax.fori_loop(0, ROWS2 // WIDE, merge_tile, 0)
        asum[...] = jnp.zeros_like(asum)
        pooled[...] = jnp.zeros_like(pooled)

        for layer in PAIR:
            def stage_two(t, carry):
                rows = ds(t * WIDE, WIDE)
                r = r2[rows, :].astype(F32)
                xhat, rstd = ln_parts(r)
                n = xhat.astype(BF16)
                n2[layer, rows, :] = n
                rst2[layer, rows, :] = rstd
                for q in QUADS:
                    cols = slice(D2 * q, D2 * (q + 1))
                    acts, slope = gelu_pair(nn(n, wut[layer, :, cols]))
                    if layer == 0:
                        a2[rows, cols] = acts.astype(BF16)
                    else:
                        abuf[:, cols] = acts.astype(BF16)
                    sl2[layer, rows, cols] = slope.astype(BF16)
                if layer == 0:
                    r2[rows, :] = (r + nn(a2[rows, :], wdt[layer])).astype(BF16)
                else:
                    rb = (r + nn(abuf[...], wdt[layer])).astype(BF16)
                    pick = onehot_rows(t)
                    asum[...] += nn(pick, abuf[...])
                    pooled[...] += nn(pick, rb)
                return carry

            lax.fori_loop(0, ROWS2 // WIDE, stage_two, 0)
        wh[CLASSES:, :] = jnp.zeros((CPAD - CLASSES, D2), BF16)
        loads[4].wait()
        for k in QUADS:
            rows = slice(TILE * k, min(TILE * (k + 1), CLASSES))
            v = sdt[rows, :]
            wh[rows, :] = v.astype(BF16)
            sq[9] += fold_sq(v)

    pl.run_scoped(
        forward,
        pltpu.VMEM((ROWS1, D1), BF16),
        pltpu.VMEM((ROWS2, D1), F32),
        pltpu.VMEM((2, D1, H1), F32),
        pltpu.VMEM((2, H1, D1), F32),
        pltpu.VMEM((D2, D2), F32),
        pltpu.VMEM((TILE, H2), F32),
        pltpu.VMEM((ROWS2, D2), F32),
        pltpu.VMEM((WIDE, H2), BF16),
    )

    xhat, rstd = ln_parts(pooled[...] * (1.0 / MT))
    hb = xhat.astype(BF16)
    logits = nt(hb, wh[...])
    col = lax.broadcasted_iota(jnp.int32, (IMAGES, CPAD), 1)
    row = lax.broadcasted_iota(jnp.int32, (IMAGES, CPAD), 0)
    logits = jnp.where(col < CLASSES, logits, -jnp.inf)
    ex = jnp.exp(logits - jnp.max(logits, axis=-1, keepdims=True))
    prob = ex / jnp.sum(ex, axis=-1, keepdims=True)
    lab_row = jnp.zeros((IMAGES, CPAD), jnp.int32)
    for i in range(IMAGES):
        lab_row = jnp.where(row == i, lab[i], lab_row)
    gl = ((prob - jnp.where(col == lab_row, 1.0, 0.0)) * (1.0 / (IMAGES * NDEV))).astype(BF16)
    g16 = (ln_back(nn(gl, wh[...]), xhat, rstd) * (1.0 / MT)).astype(BF16)
    hi = asum[...].astype(BF16)
    lo = (asum[...] - hi.astype(F32)).astype(BF16)
    me = pos['me']
    lr[me, 0:IMAGES, 0:H2] = hi
    lr[me, IMAGES:32, 0:H2] = lo
    lr[me, 0:IMAGES, H2:LRG] = g16
    lr[me, IMAGES:32, H2:LRG] = hb
    lr[me, 0:IMAGES, LRG:LRW] = gl[:, 0:D2]
    lr[me, IMAGES:32, LRG:LRW] = gl[:, D2:CPAD]
    pl.semaphore_wait(barrier, 3)
    share.send()

    asum[...] = nt(g16, wdt[1])
    pooled[...] = g16.astype(F32)

    def slope_one(i, carry):
        rows = ds(i * MT, MT)
        grad[rows, :] = jnp.broadcast_to(pooled[pl.ds(i, 1), :], (MT, D2)).astype(BF16)
        for q in QUADS:
            cols = slice(D2 * q, D2 * (q + 1))
            sl2[1, rows, cols] = (asum[pl.ds(i, 1), cols] * sl2[1, rows, cols].astype(F32)).astype(BF16)
        return carry

    lax.fori_loop(0, IMAGES, slope_one, 0)

    def up_grad(layer, first):
        def body(q):
            g_all[first + q // 2, ds((q % 2) * D2, D2), :] = tn(n2[layer], sl2[layer, :, ds(q * D2, D2)]).astype(BF16)

        return body

    def down_grad(q):
        g_all[2 + q // 2, ds((q % 2) * D2, D2), :] = tn(a2[:, ds(q * D2, D2)], grad[...]).astype(BF16)

    def input_grad(layer):
        def body(t):
            rows = ds(t * TILE, TILE)
            dy = nt(sl2[layer, rows, :], wut[layer])
            dx = ln_back(dy, n2[layer, rows, :].astype(F32), rst2[layer, rows, :])
            grad[rows, :] = (dx + grad[rows, :].astype(F32)).astype(BF16)

        return body

    def pre_grad(t):
        rows = ds(t * TILE, TILE)
        for q in QUADS:
            cols = slice(D2 * q, D2 * (q + 1))
            ga = nt(grad[rows, :], wdt[0, cols, :])
            sl2[0, rows, cols] = (ga * sl2[0, rows, cols].astype(F32)).astype(BF16)

    gsm = g_all.at[CH - 1]

    def merge_grad(t):
        gsm[D2:ROWS2, :] = tn(merged[...], grad[...]).astype(BF16)

    def stage_one_back(t):
        gm = nt(grad[ds(t * TILE, TILE), :], wm[...]).astype(BF16)
        rows = ds(t * ROWS2, ROWS2)
        g = jnp.concatenate([gm[:, D1 * j:D1 * (j + 1)] for j in QUADS], axis=0)
        for b in (1, 0):
            n = n1[b, rows, :]
            acts, slope = gelu_pair(nn(n, wuo[b]))
            accv[b] += tn(acts.astype(BF16), g)
            gp = (nt(g, wdo[b]) * slope).astype(BF16)
            accu[b] += tn(n, gp)
            if b == 1:
                dx = ln_back(nt(gp, wuo[b]), n.astype(F32), rst1[rows, :])
                g = (dx + g.astype(F32)).astype(BF16)

        @pl.when(t == 3)
        def _():
            for b in PAIR:
                gsm[D1 * b:D1 * (b + 1), :] = accu[b].astype(BF16)
                for q in PAIR:
                    gsm[TILE:D2, TILE * b + D1 * q:TILE * b + D1 * (q + 1)] = accv[b, TILE * q:TILE * (q + 1), :].astype(BF16)

    run('up1', up_grad(1, 0))
    run('in1', input_grad(1))
    run('dn0', down_grad)
    run('pre0', pre_grad)
    run('up0', up_grad(0, 4))
    run('in0', input_grad(0))
    accv[...] = jnp.zeros_like(accv)
    accu[...] = jnp.zeros_like(accu)
    gsq[...] = jnp.zeros_like(gsq)
    run('mrg', merge_grad)
    run('back', stage_one_back)

    def v1_rows(i):
        cols = ds(i * D2, D2)
        out = jnp.zeros((D2, D2), F32)
        for d in range(NDEV):
            out = out + tn(lr[d, :, cols], gdup[d]).astype(BF16).astype(F32)
        ob = out.astype(BF16)
        gv1[cols, :] = ob
        gsq[7] += fold_sq(ob.astype(F32))

    def head_rows(i):
        rows = ds(i * TILE, TILE)
        out = jnp.zeros((TILE, D2), F32)
        for d in range(NDEV):
            gl_d = lr[d, ds((i // 2) * IMAGES, IMAGES), ds(LRG + (i % 2) * TILE, TILE)]
            out = out + tn(gl_d, lr[d, IMAGES:32, H2:LRG]).astype(BF16).astype(F32)
        ob = out.astype(BF16)
        gh[rows, :] = ob
        gsq[9] += fold_sq(ob.astype(F32))

    gv1_cp = pltpu.make_async_copy(gv1, gv1_out, out_sem.at[0])
    gh_cp = pltpu.make_async_copy(gh, gh_out, out_sem.at[1])
    for d in range(NDEV):
        gdup[d, 0:IMAGES, :] = lr[d, 0:IMAGES, H2:LRG]
        gdup[d, IMAGES:32, :] = lr[d, 0:IMAGES, H2:LRG]
    run('rank', v1_rows)
    gv1_cp.start()
    run('rankh', head_rows)
    gh_cp.start()
    for word in PLAN['tail']:
        act(word)
    for b in PAIR:
        gsq[b] = fold_sq(gsm[D1 * b:D1 * (b + 1), :].astype(F32))
        gsq[2 + b] = fold_sq(gsm[TILE:D2, TILE * b:TILE * (b + 1)].astype(F32))
    gsq[SUB] = fold_sq(gsm[D2:ROWS2, :].astype(F32))
    for i in range(10):
        ratio = jnp.sqrt(total(sq[i])) / jnp.sqrt(total(gsq[i]))
        scal[i:i + 1, :] = jnp.broadcast_to(TRUST * ratio, (1, D1))
    scal[10:IMAGES, :] = jnp.zeros((6, D1), F32)
    gv1_cp.wait()
    gh_cp.wait()


def step_kernel(x_hbm, uo_hbm, do_hbm, m_hbm, ut_hbm, dt_hbm, h_hbm, vuo_hbm, vdo_hbm, vm_hbm, vut_hbm, vdt_hbm, vh_hbm,
                g_all, gv1_hbm, gh_hbm, scal,
                logits_out, uo_out, do_out, m_out, ut_out, dt_out, h_out, vuo_out, vdo_out, vm_out, vut_out, vdt_out, vh_out,
                xb, xf, gv1, gh, suo, sdo, sm, sh, sut, sdt, tuo, tdo, tm, th, tut, tdt,
                wuo, wdo, wm, wut, wdt, wh, r2, pooled,
                s_in, s_out, q_in, q_out, g_sem):
    small = [(uo_hbm, suo, uo_out), (vuo_hbm, tuo, vuo_out), (do_hbm, sdo, do_out), (vdo_hbm, tdo, vdo_out), (m_hbm, sm, m_out), (vm_hbm, tm, vm_out), (h_hbm, sh, h_out), (vh_hbm, th, vh_out)]
    ins = [pltpu.make_async_copy(src, buf, s_in.at[i]) for i, (src, buf, _) in enumerate(small)]
    louts = [pltpu.make_async_copy(buf, dst, s_out.at[i]) for i, (_, buf, dst) in enumerate(small)]
    up_big = [(ut_hbm, sut, ut_out), (vut_hbm, tut, vut_out)]
    down_big = [(dt_hbm, sdt, dt_out), (vdt_hbm, tdt, vdt_out)]
    gsm = g_all.at[CH - 1]

    def copies(layer, t, into, which=QUADS):
        out = []
        for k in which:
            src, buf, dst = (up_big + down_big)[k]
            n = D1 if k in PAIR else D2
            rows = ds(t * n, n)
            here = buf.at[rows] if k in PAIR else buf.at[layer, rows]
            if into:
                out.append(pltpu.make_async_copy(src.at[layer, rows], here, q_in.at[layer, k, t]))
            else:
                out.append(pltpu.make_async_copy(here, dst.at[layer, rows], q_out.at[layer, k, t]))
        return out

    def start(cps):
        for cp in cps:
            cp.start()

    def wait(cps):
        for cp in cps:
            cp.wait()

    x_cp = pltpu.make_async_copy(x_hbm, xb, g_sem.at[CH])
    gv1_cp = pltpu.make_async_copy(gv1_hbm, gv1, g_sem.at[CH + 1])
    gh_cp = pltpu.make_async_copy(gh_hbm, gh, g_sem.at[CH + 2])

    def up_part(layer, t):
        scale = scal[4 + layer:5 + layer, 0:1]
        rows = ds(t * D1, D1)
        for q in QUADS:
            cols = slice(D2 * q, D2 * (q + 1))
            g = g_all[4 - 4 * layer + q // 2, ds((q % 2) * D2 + t * D1, D1), :]
            nw, nv = update(sut[rows, cols], tut[rows, cols], g, scale)
            sut[rows, cols] = nw
            tut[rows, cols] = nv
            wut[layer, rows, cols] = nw.astype(BF16)

    def down_part(layer, t):
        rows = ds(t * D2, D2)
        g = g_all[2 + t // 2, ds((t % 2) * D2, D2), :] if layer == 0 else gv1[rows, :]
        nw, nv = update(sdt[layer, rows, :], tdt[layer, rows, :], g, scal[6 + layer:7 + layer, 0:1])
        sdt[layer, rows, :] = nw
        tdt[layer, rows, :] = nv
        wdt[layer, rows, :] = nw.astype(BF16)

    def stage_two(layer, r):
        xhat, _ = ln_parts(r)
        n = xhat.astype(BF16)
        acc = r
        for q in QUADS:
            cols = slice(D2 * q, D2 * (q + 1))
            a = gelu_only(nn(n, wut[layer, :, cols])).astype(BF16)
            acc = acc + nn(a, wdt[layer, cols, :])
        return acc.astype(BF16)

    first_in = [x_cp] + ins[:4]
    later = [gv1_cp]
    start(first_in)
    start(copies(0, 0, True))
    wait(first_in)
    for b in PAIR:
        nw, tuo[b] = update(suo[b], tuo[b], gsm[D1 * b:D1 * (b + 1), :], scal[b:b + 1, 0:1])
        suo[b] = nw
        wuo[b] = nw.astype(BF16)
        for q in PAIR:
            rows = slice(TILE * q, TILE * (q + 1))
            nw, tdo[b, rows, :] = update(sdo[b, rows, :], tdo[b, rows, :], gsm[TILE:D2, TILE * b + D1 * q:TILE * b + D1 * (q + 1)], scal[2 + b:3 + b, 0:1])
            sdo[b, rows, :] = nw
            wdo[b, rows, :] = nw.astype(BF16)

    def stage_one_update(t, carry):
        wait(copies(0, t, True))

        @pl.when(t < 3)
        def _():
            start(copies(0, t + 1, True))

        @pl.when(t == 1)
        def _():
            start(ins[4:6])
            start(copies(1, 0, True, DOWNS))

        @pl.when(t == 2)
        def _():
            start(later)
            start(copies(1, 1, True, DOWNS))

        @pl.when(t == 3)
        def _():
            start(copies(1, 2, True, DOWNS))
            start([gh_cp] + ins[6:])

        stage_one_tile(t, xb, xf, wuo, wdo, r2)
        up_part(0, t)
        down_part(0, t)
        start(copies(0, t, False, PAIR))
        return carry

    lax.fori_loop(0, NTILE, stage_one_update, 0)
    start(copies(1, 3, True, DOWNS))
    wait(ins[4:6])
    nw, tm[...] = update(sm[...], tm[...], gsm[D2:ROWS2, :], scal[SUB:9, 0:1])
    sm[...] = nw
    wm[...] = nw.astype(BF16)

    def merge_tile(t, carry):
        rows = ds(t * WIDE, WIDE)
        r2[rows, :] = nn(r2[rows, :], wm[...]).astype(BF16)
        return carry

    lax.fori_loop(0, ROWS2 // WIDE, merge_tile, 0)
    wait(later)
    pooled[...] = jnp.zeros_like(pooled)

    def first(t, carry):
        rows = ds(t * WIDE, WIDE)
        for i in PAIR:
            wait(copies(0, 2 * t + i, False, PAIR))
            start(copies(1, 2 * t + i, True, PAIR))
        for i in PAIR:
            wait(copies(1, 2 * t + i, True, DOWNS))
            start(copies(0, 2 * t + i, False, DOWNS))
        r2[rows, :] = stage_two(0, r2[rows, :].astype(F32))
        for i in PAIR:
            down_part(1, 2 * t + i)
        return carry

    lax.fori_loop(0, ROWS2 // WIDE, first, 0)
    def second_up(t, carry):
        wait(copies(1, t, True, PAIR))
        up_part(1, t)
        start(copies(1, t, False))
        return carry

    lax.fori_loop(0, NTILE, second_up, 0)
    start(louts[:6])
    wh[CLASSES:, :] = jnp.zeros((CPAD - CLASSES, D2), BF16)
    wait(ins[6:] + [gh_cp])

    def head_update(rows):
        nw, th[rows, :] = update(sh[rows, :], th[rows, :], gh[rows, :], scal[9:10, 0:1])
        sh[rows, :] = nw
        wh[rows, :] = nw.astype(BF16)

    def head_part(i, carry):
        head_update(ds(i * HEAD_STEP, HEAD_STEP))
        return carry

    lax.fori_loop(0, CLASSES // HEAD_STEP, head_part, 0)
    head_update(slice(CLASSES - CLASSES % HEAD_STEP, CLASSES))
    start(louts[6:])

    def second(t, carry):
        rows = ds(t * WIDE, WIDE)
        rb = stage_two(1, r2[rows, :].astype(F32))
        pooled[...] += nn(onehot_rows(t), rb)
        return carry

    lax.fori_loop(0, ROWS2 // WIDE, second, 0)
    xhat, _ = ln_parts(pooled[...] * (1.0 / MT))
    logits = nt(xhat.astype(BF16), wh[...])
    logits_out[...] = logits[:, 0:CLASSES]
    wait(louts)
    for t in QUADS:
        wait(copies(0, t, False, DOWNS))
        wait(copies(1, t, False))


def weight_scratch():
    return [pltpu.VMEM((2, D1, H1), BF16), pltpu.VMEM((2, H1, D1), BF16), pltpu.VMEM((D2, D2), BF16), pltpu.VMEM((2, D2, H2), BF16), pltpu.VMEM((2, H2, D2), BF16), pltpu.VMEM((CPAD, D2), BF16)]


def master_scratch():
    return [pltpu.VMEM((2, D1, H1), F32), pltpu.VMEM((2, H1, D1), F32), pltpu.VMEM((D2, D2), F32), pltpu.VMEM((CLASSES, D2), F32), pltpu.VMEM((D2, H2), F32), pltpu.VMEM((2, H2, D2), F32)]


def solution(mesh):
    hbm = pl.BlockSpec(memory_space=pl.ANY)
    vmem = pl.BlockSpec(memory_space=pltpu.VMEM)
    smem = pl.BlockSpec(memory_space=pltpu.SMEM)
    shape = jax.ShapeDtypeStruct
    dma = pltpu.SemaphoreType.DMA
    wide_g = [shape((CH, ROWS2, D2), BF16), shape((H2, D2), BF16), shape((CPAD, D2), BF16)]
    masters = [shape((2, D1, H1), F32), shape((2, H1, D1), F32), shape((D2, D2), F32), shape((2, D2, H2), F32), shape((2, H2, D2), F32), shape((CLASSES, D2), F32)]

    grads_call = pl.pallas_call(
        grad_kernel,
        out_shape=[pltpu.VMEM(wide_g[0].shape, BF16)] + wide_g[1:] + [shape((IMAGES, D1), F32)],
        in_specs=[hbm, smem] + [hbm] * 6,
        out_specs=[vmem] + [hbm] * 2 + [vmem],
        scratch_shapes=[pltpu.VMEM((CH, ROWS2 // k, D2), BF16) for k in (2, 4, NDEV)]
        + [pltpu.VMEM((NDEV, 32, LRW), BF16), pltpu.VMEM((NDEV, 32, D2), BF16)]
        + weight_scratch()
        + [pltpu.VMEM((ROWS2, D2), BF16), pltpu.VMEM((2, ROWS1, D1), BF16), pltpu.VMEM((ROWS1, 1), F32), pltpu.VMEM((ROWS2, D2), BF16), pltpu.VMEM((2, ROWS2, D2), BF16), pltpu.VMEM((2, ROWS2, 1), F32), pltpu.VMEM((ROWS2, H2), BF16), pltpu.VMEM((2, ROWS2, H2), BF16), pltpu.VMEM((IMAGES, D2), F32), pltpu.VMEM((IMAGES, H2), F32), pltpu.VMEM((2, H1, D1), F32), pltpu.VMEM((2, D1, H1), F32), pltpu.VMEM((10, SUB, D1), F32), pltpu.VMEM((10, SUB, D1), F32)]
        + [dma((5,)), dma((2,)), dma((2,)), dma((CH + 1, 10)), dma((CH + 1, 10)), pltpu.SemaphoreType.REGULAR((CH + 1, 3)), dma((CH,)), dma((CH,))],
        compiler_params=pltpu.CompilerParams(collective_id=0, has_side_effects=True, vmem_limit_bytes=SCOPED_LIMIT),
        name="grads",
    )

    step_call = pl.pallas_call(
        step_kernel,
        out_shape=[shape((IMAGES, CLASSES), F32)] + masters * 2,
        in_specs=[hbm] * 13 + [vmem] + [hbm] * 2 + [vmem],
        out_specs=[vmem] + [hbm] * 12,
        scratch_shapes=[pltpu.VMEM((ROWS1, D1), BF16), pltpu.VMEM((ROWS2, D1), F32)]
        + [pltpu.VMEM(g.shape, BF16) for g in wide_g[1:]]
        + master_scratch() * 2
        + weight_scratch()
        + [pltpu.VMEM((ROWS2, D2), BF16), pltpu.VMEM((IMAGES, D2), F32)]
        + [dma((SUB,)), dma((SUB,)), dma((2, 4, 4)), dma((2, 4, 4)), dma((CH + 3,))],
        compiler_params=pltpu.CompilerParams(vmem_limit_bytes=SCOPED_LIMIT),
        name="step",
    )

    def local_step(x_now, labels_now, x_next, up_one, down_one, merge_proj, up_two, down_two, head_proj, vel_up_one, vel_down_one, vel_merge_proj, vel_up_two, vel_down_two, vel_head_proj):
        params = (up_one, down_one, merge_proj, up_two, down_two, head_proj.T)
        vels = (vel_up_one, vel_down_one, vel_merge_proj, vel_up_two, vel_down_two, vel_head_proj.T)
        got = grads_call(x_now.reshape(ROWS1, D1), labels_now, *params)
        stack = pltpu.with_memory_space_constraint(got[0], pltpu.VMEM)
        outs = list(step_call(x_next.reshape(ROWS1, D1), *params, *vels, stack, *got[1:]))
        outs[6], outs[12] = outs[6].T, outs[12].T
        return tuple(outs)

    replicated = P()
    batch_split = P('data')
    in_specs = (batch_split, batch_split, batch_split) + (replicated,) * 12
    out_specs = (batch_split,) + (replicated,) * 12
    return jax.shard_map(local_step, mesh=mesh, in_specs=in_specs, out_specs=out_specs, check_vma=False)
```
